32 devices in a mesh: seq: 8 (over z, x), tp: 4 (over y, core).
Axes of the slice: x: 2, y: 2, z: 4, core: 2. Of those that a mesh axis runs over, the one named last changes fastest.
Arguments:
- packed_input: int32 [512, 5120], P('seq', 'tp'), may hold values from -2147483648 to 2147483646
- block_exponent: int32 [40, 4096], P('tp', 'seq'), may hold values from -5 to -1
- gate_input: bfloat16 [4096, 5120], P('seq', 'tp'), may hold values from -80 to 80
- state_write: bfloat16 [4096, 128], P('seq'), may hold values from -6 to 6
- state_read: bfloat16 [4096, 128], P('seq'), may hold values from -6 to 6
- log_decay: float32 [80, 4096], P('tp', 'seq'), may hold values from -1.6 to 0
- skip_weight: float32 [80], P('tp'), may hold values from 0.3 to 3
- norm_gain: float32 [5120], P('tp'), may hold values from 0.5 to 1.5
- out_weight: bfloat16 [5120, 2560], P('tp'), may hold values from -0.078125 to 0.078125
- out_cotangent: bfloat16 [4096, 2560], P('seq', 'tp'), may hold values from -6 to 6
Outputs:
- grad_input: bfloat16 [4096, 5120], P('seq', 'tp')
- grad_gate: bfloat16 [4096, 5120], P('seq', 'tp')
- grad_write: float32 [4096, 128], P('seq')
- grad_read: float32 [4096, 128], P('seq')
- grad_decay: float32 [80, 4096], P('tp', 'seq')
- grad_skip: float32 [80], P('tp')
- grad_gain: float32 [5120], P('tp')
- grad_out_weight: float32 [5120, 2560], P('tp', 'seq')
The draws below stay inside these ranges and needn't reach their ends.
All inputs are finite; a program needn't handle non-finite values.
Results may differ from the reference program's by a relative error of at most 0.0049.
Values may be sent and summed in bfloat16 or wider, within the bound.
No kernel may reach another device: no remote copies, remote signals or barrier semaphores. Data moves between devices by JAX's collectives and lax.ppermute only.
A program may use at most 128 MiB of HBM per device.

```python
import math
import jax
import jax.numpy as jnp
from jax import lax

D = 2560
HEAD_NUMBER = 80
N = 128
QBLOCK = 128
TOK_DEV = 512
TOKEN_NUMBER = 4096
HP = 5120


def draw_gate_input(key, part):
    first_key, second_key = jax.random.split(jax.random.fold_in(key, 11))
    column_pos = jnp.arange(HP, dtype=jnp.float32) / (HP - 1)
    base = jax.random.truncated_normal(first_key, -4.0, 4.0, (TOKEN_NUMBER, HP), jnp.float32)
    column_scale = 3.0 ** column_pos
    row_scale = jnp.exp(jax.random.uniform(second_key, (TOKEN_NUMBER, 1), jnp.float32, math.log(0.3), math.log(3.0)))
    return (base * column_scale[None, :] * row_scale).astype(jnp.bfloat16)


def draw_log_decay(key, part):
    random_keys = jax.random.split(jax.random.fold_in(key, 23), 7)
    slow_share = 0.5
    is_slow = jax.random.uniform(random_keys[0], (HEAD_NUMBER, 1), jnp.float32) < slow_share
    slow_rate = jax.random.uniform(random_keys[1], (HEAD_NUMBER, 1), jnp.float32, 0.15, 0.6) / TOKEN_NUMBER
    fast_rate = jnp.exp(jax.random.uniform(random_keys[2], (HEAD_NUMBER, 1), jnp.float32, math.log(1.0 / 50.0), math.log(1.0 / 30.0)))
    baseline_rate = jnp.where(is_slow, slow_rate, fast_rate)
    coarse_values = jnp.exp(jax.random.uniform(random_keys[3], (HEAD_NUMBER, TOKEN_NUMBER), jnp.float32, math.log(0.5), math.log(2.0)))
    block_multiplier = jnp.exp(jax.random.uniform(random_keys[4], (HEAD_NUMBER, TOKEN_NUMBER // TOK_DEV), jnp.float32, math.log(0.5), math.log(2.0)))
    block_multiplier = jnp.repeat(block_multiplier, TOK_DEV, axis=1)
    spike_position = jax.random.randint(random_keys[5], (HEAD_NUMBER, 2), 0, TOKEN_NUMBER)
    spike_magnitude = jax.random.uniform(random_keys[6], (HEAD_NUMBER, 2), jnp.float32, 0.22, 0.69)
    token_places = jnp.arange(TOKEN_NUMBER)[None, :]
    spike_list = jnp.where(token_places == spike_position[:, 0:1], spike_magnitude[:, 0:1], 0.0) + jnp.where(token_places == spike_position[:, 1:2], spike_magnitude[:, 1:2], 0.0)
    return -(baseline_rate * coarse_values * block_multiplier + spike_list)


def set_ends(entries, rng, least, high):
    longest = entries.shape.index(max(entries.shape))
    spots = []
    for shift in (0, 1):
        where = [jax.random.randint(jax.random.fold_in(rng, axis), (), 0, length) for axis, length in enumerate(entries.shape)]
        where[longest] = (where[longest] + shift) % entries.shape[longest]
        spots.append(tuple(where))
    return entries.at[spots[0]].set(least).at[spots[1]].set(high)


def levels(rng, shape, cuts, low, high):
    gain = 1.0
    for axis_at, parts in cuts:
        steps = jax.random.uniform(jax.random.fold_in(jax.random.fold_in(rng, 6), axis_at), (parts,), jnp.float32, low / len(cuts), high / len(cuts))
        gain = gain * jnp.repeat(jnp.exp(steps), shape[axis_at] // parts).reshape((-1,) + (1,) * (len(shape) - 1 - axis_at))
    return gain


def bell_draw(stream_key, extent, scale, limit, pieces=(), kind=jnp.bfloat16):
    drawn = jax.random.normal(stream_key, extent, jnp.float32) * scale
    if len(pieces) > 0:
        drawn = levels(stream_key, extent, pieces, -0.22, 0.18) * drawn
    return jnp.clip(drawn, min=-limit, max=limit).astype(kind)


def setup_inputs(seed: int = 0) -> dict:
    splits = jax.random.split(jax.random.key(seed), 11)
    return {
        "packed_input": set_ends(jax.random.randint(splits[0], (TOKEN_NUMBER // 8, HP), -2147483648, 2147483647), jax.random.fold_in(splits[0], 1), -2147483648, 2147483646).astype(jnp.int32),
        "block_exponent": set_ends(jax.random.randint(splits[1], (HP // QBLOCK, TOKEN_NUMBER), -5, 0), jax.random.fold_in(splits[1], 1), -5, -1).astype(jnp.int32),
        "gate_input": draw_gate_input(jax.random.fold_in(splits[10], 71), 0),
        "state_write": bell_draw(splits[3], (TOKEN_NUMBER, N), 1.0, 6.0, ((0, 8),)),
        "state_read": bell_draw(splits[4], (TOKEN_NUMBER, N), 1.0, 6.0, ((0, 8),)),
        "log_decay": draw_log_decay(jax.random.fold_in(splits[10], 71), 0),
        "skip_weight": jnp.clip(jnp.exp(math.log(3.0) - 2.3025851 * jax.random.uniform(splits[6], (HEAD_NUMBER,), jnp.float32) ** levels(splits[6], (HEAD_NUMBER,), ((0, 4),), -0.2, 0.2)), 0.3, 3.0),
        "norm_gain": jnp.clip(1.0 + 0.1 * jax.random.normal(splits[7], (HP,), jnp.float32), 0.5, 1.5),
        "out_weight": bell_draw(splits[8], (HP, D), HP ** -0.5, 0.078125, ((0, 4),)),
        "out_cotangent": bell_draw(splits[9], (TOKEN_NUMBER, D), 1.0, 6.0, ((0, 8), (1, 4))),
    }


PRECISE = lax.Precision.HIGHEST

def dequantize(packed_words, exponents):
    shifts = 4 * jnp.arange(8, dtype=jnp.int32)
    fields = jnp.bitwise_and(jnp.right_shift(packed_words[:, None, :], shifts[None, :, None]), 15) - 8
    fields = fields.reshape(packed_words.shape[0] * 8, packed_words.shape[1])
    factors = jnp.exp2(exponents.astype(jnp.float32))
    group_width = fields.shape[1] // exponents.shape[0]
    factors = jnp.repeat(factors.T, group_width, axis=1)
    return (fields.astype(jnp.float32) * factors).astype(jnp.bfloat16)

def lower_decays(seg_sum):
    length = seg_sum.shape[1]
    is_lower = (jnp.arange(length)[:, None] >= jnp.arange(length)[None, :])[None]
    spread = seg_sum[:, :, None] - seg_sum[:, None, :]
    return jnp.where(is_lower, jnp.exp(jnp.where(is_lower, spread, 0.0)), 0.0)

def block_step(state_now, inputs):
    x_part, decay_part, write_part, read_part = inputs
    seg_sum = jnp.cumsum(decay_part, axis=1)
    mixing = lower_decays(seg_sum) * jnp.dot(read_part, write_part.T, precision=PRECISE)[None]
    carried_in = jnp.einsum('in,hpn->ihp', read_part, state_now, precision=PRECISE)
    result = jnp.einsum('hij,jhp->ihp', mixing, x_part, precision=PRECISE) + jnp.exp(seg_sum).T[:, :, None] * carried_in
    end_weight = jnp.exp(seg_sum[:, -1:] - seg_sum)
    state_next = jnp.exp(seg_sum[:, -1])[:, None, None] * state_now + jnp.einsum('jhp,jn->hpn', x_part * end_weight.T[:, :, None], write_part, precision=PRECISE)
    return (state_next, result)

def scan_states(x_heads, log_decay, write_rows, read_rows):
    total, head_count, head_width = x_heads.shape
    block_len = min(256, TOK_DEV)
    blocks = total // block_len
    x_blocks = x_heads.reshape(blocks, block_len, head_count, head_width)
    decay_blocks = log_decay.reshape(head_count, blocks, block_len).transpose(1, 0, 2)
    write_blocks = write_rows.reshape(blocks, block_len, -1)
    read_blocks = read_rows.reshape(blocks, block_len, -1)
    initial = jnp.zeros((head_count, head_width, write_rows.shape[1]), jnp.float32)
    _, outputs = lax.scan(jax.checkpoint(block_step), initial, (x_blocks, decay_blocks, write_blocks, read_blocks))
    return outputs.reshape(total, head_count, head_width)

def add_block(running, pair):
    part_sum = jnp.dot(pair[0].T, pair[1], preferred_element_type=jnp.float32)
    rounded = lax.optimization_barrier(part_sum.astype(jnp.bfloat16))
    return (running + rounded.astype(jnp.float32), None)

def reference(packed_input, block_exponent, gate_input, state_write, state_read, log_decay, skip_weight, norm_gain, out_weight, out_cotangent):
    x_values = dequantize(packed_input, block_exponent)
    total, width = x_values.shape
    head_count = log_decay.shape[0]
    x_heads = x_values.astype(jnp.float32).reshape(total, head_count, width // head_count)
    write_rows = state_write.astype(jnp.float32)
    read_rows = state_read.astype(jnp.float32)
    core, pullback = jax.vjp(scan_states, x_heads, log_decay, write_rows, read_rows)
    y_full = (core + skip_weight[None, :, None] * x_heads).reshape(total, width)
    gate = gate_input.astype(jnp.float32)
    sigma = jax.nn.sigmoid(gate)
    active = gate * sigma
    mixed = y_full * active
    scale_row = lax.rsqrt(lax.optimization_barrier(jnp.mean(mixed * mixed, axis=1, keepdims=True)) + 1e-05)
    normed = (mixed * scale_row * norm_gain).astype(jnp.bfloat16)
    grad_v = jnp.dot(out_cotangent, out_weight.T, preferred_element_type=jnp.float32)
    model_width = out_weight.shape[1]
    normed_blocks = normed.reshape(-1, TOK_DEV, width)
    cot_blocks = out_cotangent.reshape(-1, TOK_DEV, model_width)
    grad_out_weight, _ = lax.scan(add_block, jnp.zeros((width, model_width), jnp.float32), (normed_blocks, cot_blocks))
    scaled = grad_v * norm_gain
    grad_gain = lax.optimization_barrier(jnp.sum(grad_v * mixed * scale_row, axis=0))
    inner = lax.optimization_barrier(jnp.sum(scaled * mixed, axis=1, keepdims=True))
    grad_mixed = scale_row * scaled - mixed * (scale_row * scale_row * scale_row) * inner / width
    grad_gate = (grad_mixed * y_full * sigma * (1.0 + gate * (1.0 - sigma))).astype(jnp.bfloat16)
    grad_y = (grad_mixed * active).reshape(total, head_count, width // head_count)
    grad_skip = lax.optimization_barrier(jnp.sum(grad_y * x_heads, axis=(0, 2)))
    grad_core, grad_decay, grad_write, grad_read = pullback(grad_y)
    grad_input = (grad_core + skip_weight[None, :, None] * grad_y).reshape(total, width).astype(jnp.bfloat16)
    return (grad_input, grad_gate, grad_write, grad_read, grad_decay, grad_skip, grad_gain, grad_out_weight)
```

```python
import functools
import jax
import jax.numpy as jnp
from jax import lax
from jax.experimental import pallas as pl
from jax.experimental.pallas import tpu as pltpu
from jax.sharding import PartitionSpec as P

F32 = jnp.float32
BF16 = jnp.bfloat16
LANES = 128
EXTRA = 16
EPSILON = 1e-05
NORMED_PARTS = 2


def mm(a, b):
    return jnp.dot(a, b, preferred_element_type=F32)


def mm_t(a, b):
    return lax.dot_general(a, b, (((1,), (1,)), ((), ())), preferred_element_type=F32)


def split2(v):
    high = v.astype(BF16)
    return high, (v - high.astype(F32)).astype(BF16)


def split3(v):
    high = v.astype(BF16)
    rest = v - high.astype(F32)
    middle = rest.astype(BF16)
    return high, middle, (rest - middle.astype(F32)).astype(BF16)


def iota(shape, axis):
    return lax.broadcasted_iota(jnp.int32, shape, axis)


def spread(values, spread2):
    return mm(jnp.concatenate(split2(values), axis=1), spread2)


def params(limit=48 << 20):
    return pltpu.CompilerParams(vmem_limit_bytes=limit)


def cost(flops, nbytes, special=0):
    return pl.CostEstimate(flops=int(flops), bytes_accessed=int(nbytes), transcendentals=int(special))


def prepare_kernel(
    heads, packed, expo_t, decay, skip, write, read,
    x_out, pay_out, seg_t_out, seg_out, spread_out, skip_out, read_t_out, pad, pad16,
):
    length, width = x_out.shape
    head_width = width // heads
    rows8 = packed.shape[0]
    pad[...] = jnp.zeros_like(pad)
    pad[0:heads, :] = decay[...]
    decay_t = pad[...].T
    lower = (iota((length, length), 0) >= iota((length, length), 1)).astype(BF16)
    seg_t = sum(mm(lower, part) for part in split3(decay_t))
    seg_t_out[...] = seg_t
    seg_out[...] = seg_t.T
    of_head = (iota((LANES, width), 1) // head_width == iota((LANES, width), 0)).astype(BF16)
    spread2 = jnp.concatenate([of_head, of_head], axis=0)
    spread_out[...] = spread2
    pad16[...] = jnp.zeros_like(pad16)
    pad16[0:heads, :] = jnp.broadcast_to(skip[...], (heads, LANES))
    skip_row = pad16[...].T[0:8, :]
    skip_out[...] = sum(mm(part, of_head) for part in split3(skip_row))
    total = seg_t[length - 1 : length, :]
    to_end = spread(jnp.exp(total - seg_t), spread2)
    groups = expo_t.shape[1]
    factor = jnp.left_shift(1, expo_t[...] + 8).astype(F32) * (2.0**-8)
    of_group = (
        iota((groups, width), 1) // (width // groups) == iota((groups, width), 0)
    ).astype(BF16)
    factors = mm(factor.astype(BF16), of_group)
    words = jnp.broadcast_to(packed[...][:, None, :], (rows8, 8, width))
    words = jnp.right_shift(words, 4 * iota((rows8, 8, width), 1))
    fields = (jnp.bitwise_and(words, 15) - 8).astype(F32).reshape(length, width)
    x = fields * factors
    x_out[...] = x.astype(BF16)
    states = mm(write[...].T, (x * to_end).astype(BF16))
    read_t_out[...] = read[...].T
    pay_out[0:LANES, :] = states.astype(BF16)
    total8 = jnp.broadcast_to(total, (8, LANES))
    high, middle, low = (mm(part, of_head) for part in split3(total8))
    row = iota((EXTRA, width), 0)
    tail = jnp.where(row == 0, high[0:1, :], jnp.where(row == 1, middle[0:1, :], low[0:1, :]))
    pay_out[LANES:, :] = jnp.where(row < 3, tail, 0.0).astype(BF16)


def prepare(packed, expo_t, decay, skip, write, read):
    heads, length = decay.shape
    width = packed.shape[1]
    shapes = (
        jax.ShapeDtypeStruct((length, width), BF16),
        jax.ShapeDtypeStruct((LANES + EXTRA, width), BF16),
        jax.ShapeDtypeStruct((length, LANES), F32),
        jax.ShapeDtypeStruct((LANES, length), F32),
        jax.ShapeDtypeStruct((2 * LANES, width), BF16),
        jax.ShapeDtypeStruct((8, width), F32),
        jax.ShapeDtypeStruct((LANES, length), BF16),
    )
    return pl.pallas_call(
        functools.partial(prepare_kernel, heads),
        name="prepare",
        out_shape=shapes,
        scratch_shapes=[pltpu.VMEM((LANES, length), F32), pltpu.VMEM((LANES, LANES), F32)],
        compiler_params=params(),
        cost_estimate=cost(3e9, 8e6),
    )(packed, expo_t, decay, skip, write, read)


def pair_columns(seg_t, seg, step):
    rolled = pltpu.roll(seg_t[...], lax.rem(LANES - 2 * step, LANES), 1)
    for side in (0, 1):
        yield side, rolled[:, side : side + 1], seg[pl.ds(2 * step + side, 1), :]


def inside_kernel(head_width, seg_t, seg, write, read, x, skip, out, cross):
    step = pl.program_id(0)
    length = x.shape[0]
    half = length // 2

    @pl.when(step == 0)
    def _():
        cross[...] = mm_t(read[...], write[...])

    diagonal = iota((half, half), 0) >= iota((half, half), 1)
    parts = []
    for side, column, row in pair_columns(seg_t, seg, step):
        rows = []
        for block in (0, 1):
            low = block * half
            square = slice(low, low + half)
            gap = column[square] - row[:, square]
            decayed = jnp.where(diagonal, jnp.exp(jnp.minimum(gap, 0.0)), 0.0)
            mixing = decayed * cross[square, square]
            if block == 1:
                left = jnp.exp(column[square] - row[:, 0:half]) * cross[square, 0:half]
                mixing = jnp.concatenate([left, mixing], axis=1)
            high, rest = split2(mixing)
            values = x[0 : low + half, :]
            rows.append(mm(high, values) + mm(rest, values))
        parts.append(jnp.concatenate(rows, axis=0))
    first = iota((length, LANES), 1) < head_width
    out[...] = jnp.where(first, parts[0], parts[1]) + skip[0:1, :] * x[...].astype(F32)


def whole(shape):
    return pl.BlockSpec(shape, lambda *_: (0,) * len(shape))


def inside(heads, seg_t, seg, write, read, x, skip):
    length, width = x.shape
    column = pl.BlockSpec((length, LANES), lambda j: (0, j))
    return pl.pallas_call(
        functools.partial(inside_kernel, width // heads),
        name="inside",
        grid=(width // LANES,),
        in_specs=[
            whole((length, LANES)), whole((LANES, length)), whole(write.shape), whole(read.shape),
            column, pl.BlockSpec((8, LANES), lambda j: (0, j)),
        ],
        out_specs=column,
        out_shape=jax.ShapeDtypeStruct((length, width), F32),
        scratch_shapes=[pltpu.VMEM((length, length), F32)],
        compiler_params=params(),
        cost_estimate=cost(20e9, 5e6),
    )(seg_t, seg, write, read, x, skip)


def gathered_total(pays, k):
    tail = pays[k][LANES : LANES + 8, :].astype(F32)
    return tail[0:1, :] + tail[1:2, :] + tail[2:3, :]


def boundary(totals, pays, sources, position, later, count):
    width = totals.shape[1]
    column = jnp.zeros((count, 1), jnp.int32)
    for k in range(count):
        column = jnp.where(iota((count, 1), 0) == k, sources[k], column)
    powers = jnp.zeros((count, width), F32)
    for j in range(count):
        if later:
            between = jnp.logical_and(column > sources[j], sources[j] > position)
        else:
            between = jnp.logical_and(column < sources[j], sources[j] < position)
        powers = powers + jnp.where(between, totals[j : j + 1, :], 0.0)
    wanted = column > position if later else column < position
    weights = jnp.where(wanted, jnp.exp(powers), 0.0)
    result = jnp.zeros((LANES, width), F32)
    for k in range(count):
        result = result + weights[k : k + 1, :] * pays[k][0:LANES, :].astype(F32)
    return result


def enter_kernel(
    count, sources, y_local, gate, grad_v, gain, read, seg_t, spread2, *rest,
):
    pays = rest[:count]
    y_out, scaled_t_out, stats_out, state_out, totals_out, state2 = rest[count:]
    width = y_out.shape[1]

    @pl.when(pl.program_id(0) == 0)
    def _():
        for k in range(count):
            totals_out[k : k + 1, :] = gathered_total(pays, k)
        state = boundary(totals_out[...], pays, sources, sources[count], False, count)
        state_out[...] = state
        state2[0:LANES, :], state2[LANES:, :] = split2(state)

    from_start = spread(jnp.exp(seg_t[...]), spread2[...])
    read_part = read[...]
    carried = mm(jnp.concatenate([read_part, read_part], axis=1), state2[...])
    y = y_local[...] + from_start * carried
    y_out[...] = y
    z = gate[...].astype(F32)
    mixed = y * z / (1.0 + jnp.exp(-z))
    with_gain = mixed * gain[...]
    scaled_t_out[...] = with_gain.T
    squares = jnp.sum(mixed * mixed, axis=1, keepdims=True)
    inner = jnp.sum(grad_v[...] * with_gain, axis=1, keepdims=True)
    lane = iota((squares.shape[0], LANES), 1)
    stats = jnp.where(lane == 0, squares, jnp.where(lane == 1, inner, 0.0))
    stats_out[...] = stats.T[0:8, :]


def enter(sources, y_local, gate, grad_v, gain, read, seg_t, spread2, pays):
    length, width = y_local.shape
    count = len(pays)
    block = LANES
    token = pl.BlockSpec((block, width), lambda i, *_: (i, 0))
    narrow = pl.BlockSpec((block, LANES), lambda i, *_: (i, 0))
    shapes = (
        jax.ShapeDtypeStruct((length, width), F32),
        jax.ShapeDtypeStruct((width, length), F32),
        jax.ShapeDtypeStruct((8, length), F32),
        jax.ShapeDtypeStruct((LANES, width), F32),
        jax.ShapeDtypeStruct((count, width), F32),
    )
    return pl.pallas_call(
        functools.partial(enter_kernel, count),
        name="enter",
        grid_spec=pltpu.PrefetchScalarGridSpec(
            num_scalar_prefetch=1,
            grid=(length // block,),
            in_specs=[
                token, token, token, whole((1, width)), narrow, narrow, whole(spread2.shape),
            ] + [whole(pays[0].shape)] * count,
            out_specs=[
                token,
                pl.BlockSpec((width, block), lambda i, *_: (0, i)),
                pl.BlockSpec((8, block), lambda i, *_: (0, i)),
                whole((LANES, width)),
                whole((count, width)),
            ],
            scratch_shapes=[pltpu.VMEM((2 * LANES, width), BF16)],
        ),
        out_shape=shapes,
        compiler_params=params(),
        cost_estimate=cost(3e9, 15e6),
    )(sources, y_local, gate, grad_v, gain, read, seg_t, spread2, *pays)


def gate_kernel(
    total_width, y_ref, gate, grad_v, gain, stats, x, seg_t, spread2, read_t,
    gate_out, grad_y_out, pay_out, columns, cot, sums,
):
    step = pl.program_id(0)
    row = iota((LANES, LANES), 0)
    squares, inner = stats[0:1, :], stats[1:2, :]
    scale_row = lax.rsqrt(squares * (1.0 / total_width) + EPSILON)
    back_row = scale_row * scale_row * scale_row * inner * (1.0 / total_width)
    columns[...] = jnp.where(row == 0, scale_row, jnp.where(row == 1, back_row, 0.0)).T
    scale, back = columns[:, 0:1], columns[:, 1:2]
    y = y_ref[...]
    z = gate[...].astype(F32)
    sigma = 1.0 / (1.0 + jnp.exp(-z))
    active = z * sigma
    mixed = y * active
    scaled_v = scale * grad_v[...]
    grad_mixed = scaled_v * gain[...] - mixed * back
    gate_out[...] = (grad_mixed * y * sigma * (1.0 + z * (1.0 - sigma))).astype(BF16)
    grad_y = grad_mixed * active
    grad_y_out[...] = grad_y
    gain_part = jnp.sum(scaled_v * mixed, axis=0, keepdims=True)
    skip_part = jnp.sum(grad_y * x[...].astype(F32), axis=0, keepdims=True)
    from_start = spread(jnp.exp(seg_t[...]), spread2[...])
    cot_part = mm(read_t[...], (grad_y * from_start).astype(BF16))
    wide = iota((8, grad_y.shape[1]), 0)
    sum_part = jnp.where(wide == 0, gain_part, jnp.where(wide == 1, skip_part, 0.0))

    @pl.when(step == 0)
    def _():
        cot[...] = cot_part
        sums[...] = sum_part

    @pl.when(step > 0)
    def _():
        cot[...] += cot_part
        sums[...] += sum_part

    @pl.when(step == pl.num_programs(0) - 1)
    def _():
        pay_out[0:LANES, :] = cot[...].astype(BF16)
        high, low = split2(sums[...])
        pay_out[LANES:, :] = jnp.concatenate([high, low], axis=0)


def gate_grads(total_width, y, gate, grad_v, gain, stats, x, seg_t, spread2, read_t):
    length, width = y.shape
    block = LANES
    token = pl.BlockSpec((block, width), lambda i: (i, 0))
    narrow = pl.BlockSpec((block, LANES), lambda i: (i, 0))
    shapes = (
        jax.ShapeDtypeStruct((length, width), BF16),
        jax.ShapeDtypeStruct((length, width), F32),
        jax.ShapeDtypeStruct((LANES + EXTRA, width), BF16),
    )
    return pl.pallas_call(
        functools.partial(gate_kernel, total_width),
        name="gate_grads",
        grid=(length // block,),
        in_specs=[
            token, token, token, whole((1, width)), pl.BlockSpec((8, block), lambda i: (0, i)),
            token, narrow, whole(spread2.shape), pl.BlockSpec((LANES, block), lambda i: (0, i)),
        ],
        out_specs=[token, token, whole((LANES + EXTRA, width))],
        out_shape=shapes,
        scratch_shapes=[
            pltpu.VMEM((LANES, LANES), F32), pltpu.VMEM((LANES, width), F32), pltpu.VMEM((8, width), F32),
        ],
        compiler_params=params(),
        cost_estimate=cost(3e9, 15e6),
    )(y, gate, grad_v, gain, stats, x, seg_t, spread2, read_t)


def inside_back_kernel(
    head_width, seg_t, seg, write, read, x, grad_y, out, grad_write, grad_read, cross, grad_cross,
):
    step = pl.program_id(0)
    length = x.shape[0]
    half = length // 2

    @pl.when(step == 0)
    def _():
        cross[...] = mm_t(write[...], read[...])
        grad_cross[...] = jnp.zeros_like(grad_cross)

    diagonal = iota((half, half), 0) <= iota((half, half), 1)
    first = iota((length, LANES), 1) < head_width
    grads = grad_y[...].astype(BF16)
    values = x[...]
    parts = []
    for side, column, row in pair_columns(seg_t, seg, step):
        mine = first if side == 0 else jnp.logical_not(first)
        own = jnp.where(mine, values, jnp.zeros_like(values))
        rows = []
        for block in (0, 1):
            low = block * half
            square = slice(low, low + half)
            gap = row[:, square] - column[square]
            decayed = jnp.where(diagonal, jnp.exp(jnp.minimum(gap, 0.0)), 0.0)
            mixing = decayed * cross[square, square]
            grad_cross[square, square] += mm_t(own[square], grads[square]) * decayed
            if block == 0:
                decayed = jnp.exp(row[:, half:] - column[square])
                mixing = jnp.concatenate([mixing, decayed * cross[square, half:]], axis=1)
                grad_cross[square, half:] += mm_t(own[square], grads[half:]) * decayed
            rows.append(mm(mixing.astype(BF16), grads[low:]))
        parts.append(jnp.concatenate(rows, axis=0))
    out[...] = jnp.where(first, parts[0], parts[1])

    @pl.when(step == pl.num_programs(0) - 1)
    def _():
        high, low = split2(grad_cross[...])
        grad_write[...] = mm(high, read[...]) + mm(low, read[...])
        turned = grad_cross[...].T
        high, low = split2(turned)
        grad_read[...] = mm(high, write[...]) + mm(low, write[...])


def inside_back(heads, seg_t, seg, write, read, x, grad_y):
    length, width = x.shape
    column = pl.BlockSpec((length, LANES), lambda j: (0, j))
    shapes = (
        jax.ShapeDtypeStruct((length, width), F32),
        jax.ShapeDtypeStruct((length, LANES), F32),
        jax.ShapeDtypeStruct((length, LANES), F32),
    )
    return pl.pallas_call(
        functools.partial(inside_back_kernel, width // heads),
        name="inside_back",
        grid=(width // LANES,),
        in_specs=[
            whole((length, LANES)), whole((LANES, length)), whole(write.shape), whole(read.shape),
            column, column,
        ],
        out_specs=[column, whole((length, LANES)), whole((length, LANES))],
        out_shape=shapes,
        scratch_shapes=[pltpu.VMEM((length, length), F32), pltpu.VMEM((length, length), F32)],
        compiler_params=params(),
        cost_estimate=cost(20e9, 8e6),
    )(seg_t, seg, write, read, x, grad_y)


def leave_kernel(
    count, heads, sources, y_ref, x_ref, grad_y_ref, inner_ref, write, seg_t, last, spread2,
    skip, state, totals, write_part, read_part, *rest,
):
    pays = rest[:count]
    (input_out, maps_out, decay_out, gain_out, skip_out, cot2, state16, from_head, per_head, sums) = rest[count:]
    step = pl.program_id(0)
    steps = pl.num_programs(0)
    block, width = y_ref.shape
    length = per_head.shape[0]

    @pl.when(step == 0)
    def _():
        cot = boundary(totals[...], pays, sources, sources[count], True, count)
        cot2[0:LANES, :], cot2[LANES:, :] = split2(cot)
        state16[...] = state[...].astype(BF16)
        from_head[...] = spread2[0:LANES, :].T
        ended = spread(jnp.exp(last[...]), spread2[...])
        through = jnp.sum(cot * state[...], axis=0, keepdims=True) * ended[0:1, :]
        sums[...] = jnp.where(iota((8, width), 0) == 0, through, 0.0)
        collected = jnp.zeros((8, width), F32)
        for k in range(count):
            tail = pays[k][LANES:, :].astype(F32)
            collected = collected + tail[0:8, :] + tail[8:16, :]
        gain_out[...] = collected
        skip_out[...] = sum(mm(part, from_head[...]) for part in split3(collected))

    seg_part = seg_t[...]
    decays = jnp.exp(seg_part)
    to_end = spread(jnp.exp(last[0:1, :] - seg_part), spread2[...])
    from_start = spread(decays, spread2[...])
    x = x_ref[...].astype(F32)
    grad_y = grad_y_ref[...]
    write_rows = write[...]
    from_later = to_end * mm(jnp.concatenate([write_rows, write_rows], axis=1), cot2[...])
    core_grad = inner_ref[...] + from_later
    skip_row = skip[0:1, :]
    input_out[...] = (skip_row * grad_y + core_grad).astype(BF16)
    leaving = jnp.sum(x * from_later, axis=0, keepdims=True)
    sums[...] += jnp.where(iota((8, width), 0) == 0, leaving, 0.0)
    terms = grad_y * (y_ref[...] - skip_row * x) - x * core_grad
    high, low = split2(terms)
    start = pl.multiple_of(step * block, block)
    per_head[pl.ds(start, block), :] = mm(high, from_head[...]) + mm(low, from_head[...])
    maps_out[:, 0:LANES] = write_part[...] + mm_t((x * to_end).astype(BF16), cot2[0:LANES, :])
    maps_out[:, LANES:] = read_part[...] + mm_t((grad_y * from_start).astype(BF16), state16[...])

    @pl.when(step == steps - 1)
    def _():
        final = sum(mm(part, from_head[...]) for part in split3(sums[...]))
        upper = (iota((length, length), 0) <= iota((length, length), 1)).astype(BF16)
        tail = sum(mm(upper, part) for part in split3(per_head[...]))
        decay_out[...] = (tail + final[0:1, :]).T[0:heads, :]


def leave(
    heads, sources, y, x, grad_y, inner, write, seg_t, spread2, skip, state, totals,
    write_part, read_part, pays,
):
    length, width = y.shape
    count = len(pays)
    block = LANES
    token = pl.BlockSpec((block, width), lambda i, *_: (i, 0))
    narrow = pl.BlockSpec((block, LANES), lambda i, *_: (i, 0))
    shapes = (
        jax.ShapeDtypeStruct((length, width), BF16),
        jax.ShapeDtypeStruct((length, 2 * LANES), F32),
        jax.ShapeDtypeStruct((heads, length), F32),
        jax.ShapeDtypeStruct((8, width), F32),
        jax.ShapeDtypeStruct((8, LANES), F32),
    )
    last = jnp.broadcast_to(seg_t[length - 1 :, :], (8, LANES))
    return pl.pallas_call(
        functools.partial(leave_kernel, count, heads),
        name="leave",
        grid_spec=pltpu.PrefetchScalarGridSpec(
            num_scalar_prefetch=1,
            grid=(length // block,),
            in_specs=[
                token, token, token, token, narrow, narrow, whole((8, LANES)),
                whole(spread2.shape), whole((8, width)), whole((LANES, width)),
                whole((count, width)), narrow, narrow,
            ] + [whole(pays[0].shape)] * count,
            out_specs=[
                token,
                pl.BlockSpec((block, 2 * LANES), lambda i, *_: (i, 0)),
                whole((heads, length)),
                whole((8, width)),
                whole((8, LANES)),
            ],
            scratch_shapes=[
                pltpu.VMEM((2 * LANES, width), BF16),
                pltpu.VMEM((LANES, width), BF16),
                pltpu.VMEM((width, LANES), BF16),
                pltpu.VMEM((length, LANES), F32),
                pltpu.VMEM((8, width), F32),
            ],
        ),
        out_shape=shapes,
        compiler_params=params(),
        cost_estimate=cost(5e9, 20e6),
    )(
        sources, y, x, grad_y, inner, write, seg_t, last, spread2, skip, state, totals,
        write_part, read_part, *pays,
    )


def product_kernel(final, index, mine, theirs, cot_mine, cot_theirs, out):
    first = mm(mine[...], cot_mine[0]).astype(BF16).astype(F32)
    second = mm(theirs[...], cot_theirs[0]).astype(BF16).astype(F32)
    out[...] = (first + second).astype(out.dtype)


def product(final, index, mine, theirs, cot_mine, cot_theirs):
    rows, length = mine.shape
    columns = cot_mine.shape[2]
    block = rows // 2 if (rows // 2) % 16 == 0 else rows
    side = pl.BlockSpec((block, length), lambda i, index: (i, 0))
    piece = pl.BlockSpec((1, length, columns), lambda i, index: (index[0], 0, 0))
    return pl.pallas_call(
        functools.partial(product_kernel, final),
        name="product",
        grid_spec=pltpu.PrefetchScalarGridSpec(
            num_scalar_prefetch=1,
            grid=(rows // block,),
            in_specs=[side, side, piece, piece],
            out_specs=pl.BlockSpec((block, columns), lambda i, index: (i, 0)),
        ),
        out_shape=jax.ShapeDtypeStruct((rows, columns), F32 if final else BF16),
        compiler_params=params(),
        cost_estimate=cost(4.0 * rows * length * columns, 2e6),
    )(index, mine, theirs, cot_mine, cot_theirs)


def ring_gather(value, size):
    half = size // 2
    order = [2 * q for q in range(half)] + [2 * (size - 1 - q) + 1 for q in range(half, size)]
    ahead = [(order[i], order[(i + 1) % size]) for i in range(size)]
    behind = [(b, a) for a, b in ahead]
    held = [(value, 0)]
    forward = backward = value
    for hop in range(1, half + 1):
        forward = lax.ppermute(forward, "seq", ahead)
        held.append((forward, -hop))
        if hop < half:
            backward = lax.ppermute(backward, "seq", behind)
            held.append((backward, hop))
    return [v for v, _ in held], [shift for _, shift in held]


def ring_sources(shifts, size):
    position = lax.axis_index("seq")
    half = size // 2
    place = jnp.where(position % 2 == 0, position // 2, size - 1 - position // 2)
    places = (place + jnp.array(shifts, jnp.int32) + size) % size
    found = jnp.where(places < half, 2 * places, 2 * (size - 1 - places) + 1)
    return jnp.concatenate([found, position[None]]).astype(jnp.int32)


def butterfly_sum(value, size):
    stride = 1
    while stride < size:
        value = value + lax.ppermute(value, "tp", [(i, i ^ stride) for i in range(size)])
        stride *= 2
    return value


def gather_columns(value, size):
    place = lax.axis_index("tp")
    stride = size // 2
    held = value
    while stride >= 1:
        other = lax.ppermute(held, "tp", [(i, i ^ stride) for i in range(size)])
        low = (place // stride) % 2 == 0
        held = jnp.stack([jnp.where(low, held, other), jnp.where(low, other, held)])
        stride //= 2
    levels = held.ndim - 2
    held = held.transpose((levels,) + tuple(range(levels - 1, -1, -1)) + (levels + 1,))
    return held.reshape(value.shape[0], size * value.shape[1])


def on_device(
    packed_input, block_exponent, gate_input, state_write, state_read, log_decay,
    skip_weight, norm_gain, out_weight, out_cotangent,
):
    heads, length = log_decay.shape
    width = packed_input.shape[1]
    seq_size = lax.axis_size("seq")
    tp_size = lax.axis_size("tp")
    total_width = width * tp_size
    model_width = out_weight.shape[1]
    columns = model_width // seq_size
    groups = seq_size // 2
    position = lax.axis_index("seq")
    parity = position % 2
    partner = [(i, i ^ 1) for i in range(seq_size)]

    per_shard = out_cotangent.shape[1] // (2 * columns)
    halves = out_cotangent.reshape(length, per_shard, 2, columns)
    other_half = jnp.where(parity == 0, halves[:, :, 1], halves[:, :, 0])
    shard_theirs = lax.ppermute(other_half, "seq", partner).reshape(length, per_shard * columns)
    cot_full = gather_columns(out_cotangent, tp_size)

    gain = norm_gain[None, :]
    x, pay, seg_t, seg, spread2, skip, read_t = prepare(
        packed_input, block_exponent.T, log_decay, skip_weight[:, None], state_write, state_read
    )
    pays, shifts = ring_gather(pay, seq_size)
    sources = ring_sources(shifts, seq_size)
    y_local = inside(heads, seg_t, seg, state_write, state_read, x, skip)
    grad_v = lax.dot_general(
        cot_full, out_weight, (((1,), (1,)), ((), ())), preferred_element_type=F32
    )
    cot_halves = cot_full.reshape(length, groups, 2, columns)
    cot_mine = jnp.where(parity == 0, cot_halves[:, :, 0], cot_halves[:, :, 1]).transpose(1, 0, 2)
    cot_theirs = (
        gather_columns(shard_theirs, tp_size).reshape(length, groups, columns).transpose(1, 0, 2)
    )

    y, scaled_t, stats, state, totals = enter(
        sources, y_local, gate_input, grad_v, gain, state_read, seg_t, spread2, pays
    )
    stats = butterfly_sum(stats, tp_size)
    scale = lax.rsqrt(stats[0:1, :] / total_width + EPSILON)
    part_rows = width // NORMED_PARTS
    normed, normed_theirs = [], []
    for part in range(NORMED_PARTS):
        rows = scaled_t[part * part_rows : (part + 1) * part_rows]
        normed.append((rows * scale).astype(BF16))
        normed_theirs.append(lax.ppermute(normed[part], "seq", partner))

    grad_gate, grad_y, pay_back = gate_grads(
        total_width, y, gate_input, grad_v, gain, stats, x, seg_t, spread2, read_t
    )
    pays_back, _ = ring_gather(pay_back, seq_size)
    inner, write_part, read_part = inside_back(heads, seg_t, seg, state_write, state_read, x, grad_y)

    group = position // 2
    weight_parts = []
    for part in range(NORMED_PARTS):
        received = []
        for shift in range(groups - 1, -1, -1):
            index = ((group + shift) % groups)[None].astype(jnp.int32)
            piece = product(
                shift == 0, index, normed[part], normed_theirs[part], cot_mine, cot_theirs
            )
            if shift > 0:
                moves = [(i, (i + 2 * shift) % seq_size) for i in range(seq_size)]
                piece = lax.ppermute(piece, "seq", moves)
            received.append(piece)
        weight_parts.append(sum(piece.astype(F32) for piece in received))
    grad_out_weight = jnp.concatenate(weight_parts, axis=0)

    grad_input, maps, grad_decay, gain_rows, skip_rows = leave(
        heads, sources, y, x, grad_y, inner, state_write, seg_t, spread2, skip, state, totals,
        write_part, read_part, pays_back,
    )
    maps = butterfly_sum(maps, tp_size)
    return (
        grad_input,
        grad_gate,
        maps[:, 0:LANES],
        maps[:, LANES:],
        grad_decay,
        skip_rows[1, 0:heads],
        gain_rows[0],
        grad_out_weight,
    )


def solution(mesh):
    placed = (
        P("seq", "tp"), P("tp", "seq"), P("seq", "tp"), P("seq", None), P("seq", None),
        P("tp", "seq"), P("tp"), P("tp"), P("tp", None), P("seq", "tp"),
    )
    return jax.shard_map(
        on_device,
        mesh=mesh,
        in_specs=placed,
        out_specs=(
            P("seq", "tp"), P("seq", "tp"), P("seq", None), P("seq", None), P("tp", "seq"),
            P("tp"), P("tp"), P("tp", "seq"),
        ),
        check_vma=False,
    )
```

```python
import functools
import jax
import jax.numpy as jnp
from jax import lax
from jax.experimental import pallas as pl
from jax.experimental.pallas import tpu as pltpu
from jax.sharding import PartitionSpec as P

F32 = jnp.float32
BF16 = jnp.bfloat16
LANES = 128
EXTRA = 16
EPSILON = 1e-05
NORMED_PARTS = 2
HALF = LANES // 2


def mm(a, b):
    return jnp.dot(a, b, preferred_element_type=F32)


def mm_t(a, b):
    return lax.dot_general(a, b, (((1,), (1,)), ((), ())), preferred_element_type=F32)


def split2(v):
    high = v.astype(BF16)
    return high, (v - high.astype(F32)).astype(BF16)


def split3(v):
    high = v.astype(BF16)
    rest = v - high.astype(F32)
    middle = rest.astype(BF16)
    return high, middle, (rest - middle.astype(F32)).astype(BF16)


def iota(shape, axis):
    return lax.broadcasted_iota(jnp.int32, shape, axis)


def spread(values, spread2):
    return mm(jnp.concatenate(split2(values), axis=1), spread2)


def params(limit=24 << 20):
    return pltpu.CompilerParams(vmem_limit_bytes=limit)


def cost(flops, nbytes, special=0):
    return pl.CostEstimate(flops=int(flops), bytes_accessed=int(nbytes), transcendentals=int(special))


def skipping(kernel, first, extra):
    return lambda *refs: kernel(*refs[:first], *refs[first + extra :])


WAIT = pl.BlockSpec(memory_space=pl.ANY)


def prepare_kernel(
    heads, packed, expo, decay, skip, write, read,
    x_out, near_out, far_out, seg_t_out, seg_out, spread_out, skip_out, read_t_out, pad, pad8,
):
    length, width = x_out.shape
    head_width = width // heads
    rows8 = packed.shape[0]
    groups = expo.shape[0]
    pad[...] = jnp.zeros_like(pad)
    pad[0:heads, :] = decay[...]
    decay_t = pad[...].T
    lower = (iota((length, length), 0) >= iota((length, length), 1)).astype(BF16)
    seg_t = sum(mm(lower, part) for part in split3(decay_t))
    seg_t_out[...] = seg_t
    seg_out[...] = seg_t.T
    of_head = (iota((LANES, width), 1) // head_width == iota((LANES, width), 0)).astype(BF16)
    spread2 = jnp.concatenate([of_head, of_head], axis=0)
    spread_out[...] = spread2
    pad8[...] = jnp.zeros_like(pad8)
    pad8[0:1, 0:heads] = skip[...]
    skip_out[...] = sum(mm(part, of_head) for part in split3(pad8[...]))
    total = seg_t[length - 1 : length, :]
    to_end = spread(jnp.exp(total - seg_t), spread2)
    pad[...] = jnp.zeros_like(pad)
    pad[0:groups, :] = jnp.left_shift(1, expo[...] + 8).astype(F32) * (2.0**-8)
    of_group = (
        iota((LANES, width), 1) // (width // groups) == iota((LANES, width), 0)
    ).astype(BF16)
    factors = mm(pad[...].T.astype(BF16), of_group)
    words = jnp.broadcast_to(packed[...][:, None, :], (rows8, 8, width))
    words = jnp.right_shift(words, 4 * iota((rows8, 8, width), 1))
    fields = (jnp.bitwise_and(words, 15) - 8).astype(F32).reshape(length, width)
    x = fields * factors
    x_out[...] = x.astype(BF16)
    states = mm(write[...].T, (x * to_end).astype(BF16)).astype(BF16)
    read_t_out[...] = read[...].T
    near_out[0:HALF, :] = states[0:HALF, :]
    far_out[...] = states[HALF:, :]
    total8 = jnp.broadcast_to(total, (8, LANES))
    high, middle, low = (mm(part, of_head) for part in split3(total8))
    row = iota((EXTRA, width), 0)
    tail = jnp.where(row == 0, high[0:1, :], jnp.where(row == 1, middle[0:1, :], low[0:1, :]))
    near_out[HALF:, :] = jnp.where(row < 3, tail, 0.0).astype(BF16)


def prepare(packed, expo, decay, skip, write, read):
    heads, length = decay.shape
    width = packed.shape[1]
    shapes = (
        jax.ShapeDtypeStruct((length, width), BF16),
        jax.ShapeDtypeStruct((HALF + EXTRA, width), BF16),
        jax.ShapeDtypeStruct((HALF, width), BF16),
        jax.ShapeDtypeStruct((length, LANES), F32),
        jax.ShapeDtypeStruct((LANES, length), F32),
        jax.ShapeDtypeStruct((2 * LANES, width), BF16),
        jax.ShapeDtypeStruct((8, width), F32),
        jax.ShapeDtypeStruct((LANES, length), BF16),
    )
    return pl.pallas_call(
        functools.partial(prepare_kernel, heads),
        name="prepare",
        out_shape=shapes,
        scratch_shapes=[pltpu.VMEM((LANES, length), F32), pltpu.VMEM((8, LANES), F32)],
        compiler_params=params(),
        cost_estimate=cost(3e9, 8e6),
    )(packed, expo, decay, skip, write, read)


def pick_kernel(per_half, columns, parity, shard, out):
    odd_wanted = parity[0] == 0
    for sub in range(per_half):
        even_part = shard[:, 2 * sub * columns : (2 * sub + 1) * columns]
        odd_part = shard[:, (2 * sub + 1) * columns : (2 * sub + 2) * columns]
        out[:, sub * columns : (sub + 1) * columns] = jnp.where(odd_wanted, odd_part, even_part)


def pick(parity, shard, columns):
    length, shard_width = shard.shape
    out = (length, shard_width // 2)
    return pl.pallas_call(
        functools.partial(pick_kernel, shard_width // (2 * columns), columns),
        name="pick",
        grid_spec=pltpu.PrefetchScalarGridSpec(
            num_scalar_prefetch=1, grid=(1,), in_specs=[whole(shard.shape)], out_specs=whole(out)
        ),
        out_shape=jax.ShapeDtypeStruct(out, BF16),
        compiler_params=params(),
        cost_estimate=cost(1e8, 2e6),
    )(parity, shard)


def cotangent_kernel(shards, per_half, owners, weight, *rest):
    mine = rest[:shards]
    theirs = rest[shards : 2 * shards]
    grad_v, cot_mine, cot_theirs, full = rest[2 * shards :]
    shard_width = mine[0].shape[1]
    columns = cot_mine.shape[1]

    @pl.when(pl.program_id(0) == 0)
    def _():
        odd = owners[shards] == 1
        for m in range(shards):
            for q in range(shards):
                @pl.when(owners[m] == q)
                def _():
                    full[:, q * shard_width : (q + 1) * shard_width] = mine[m][...]
            for sub in range(per_half):
                even_part = mine[m][:, 2 * sub * columns : (2 * sub + 1) * columns]
                odd_part = mine[m][:, (2 * sub + 1) * columns : (2 * sub + 2) * columns]
                spot = owners[m] * per_half + sub
                cot_mine[spot] = jnp.where(odd, odd_part, even_part).T
                cot_theirs[spot] = theirs[m][:, sub * columns : (sub + 1) * columns].T

    grad_v[...] = mm_t(full[...], weight[...])


def cotangent(owners, weight, mine, theirs, columns, waits):
    shards = len(mine)
    length, shard_width = mine[0].shape
    width, model_width = weight.shape
    per_half = shard_width // (2 * columns)
    groups = shards * per_half
    block = 2 * LANES if width % (2 * LANES) == 0 else LANES
    stacked = (groups, columns, length)
    return pl.pallas_call(
        skipping(
            functools.partial(cotangent_kernel, shards, per_half), 2 + 2 * shards, len(waits)
        ),
        name="cotangent",
        grid_spec=pltpu.PrefetchScalarGridSpec(
            num_scalar_prefetch=1,
            grid=(width // block,),
            in_specs=[pl.BlockSpec((block, model_width), lambda i, *_: (i, 0))]
            + [whole(mine[0].shape)] * shards
            + [whole(theirs[0].shape)] * shards
            + [WAIT] * len(waits),
            out_specs=[
                pl.BlockSpec((length, block), lambda i, *_: (0, i)), whole(stacked), whole(stacked),
            ],
            scratch_shapes=[pltpu.VMEM((length, model_width), BF16)],
        ),
        out_shape=(
            jax.ShapeDtypeStruct((length, width), F32),
            jax.ShapeDtypeStruct(stacked, BF16),
            jax.ShapeDtypeStruct(stacked, BF16),
        ),
        compiler_params=params(),
        cost_estimate=cost(2.0 * length * width * model_width, 20e6),
    )(owners, weight, *mine, *theirs, *waits)


def pair_columns(seg_t, seg, step):
    rolled = pltpu.roll(seg_t[...], lax.rem(LANES - 2 * step, LANES), 1)
    for side in (0, 1):
        yield side, rolled[:, side : side + 1], seg[pl.ds(2 * step + side, 1), :]


def inside_kernel(head_width, start, seg_t, seg, write, read, x, skip, *rest):
    out, cross = rest[-2:]
    step = pl.program_id(0) + start
    length = x.shape[0]
    half = length // 2

    @pl.when(pl.program_id(0) == 0)
    def _():
        cross[...] = mm_t(read[...], write[...])

    diagonal = iota((half, half), 0) >= iota((half, half), 1)
    parts = []
    for side, column, row in pair_columns(seg_t, seg, step):
        rows = []
        for block in (0, 1):
            low = block * half
            square = slice(low, low + half)
            gap = column[square] - row[:, square]
            decayed = jnp.where(diagonal, jnp.exp(jnp.minimum(gap, 0.0)), 0.0)
            mixing = decayed * cross[square, square]
            if block == 1:
                left = jnp.exp(column[square] - row[:, 0:half]) * cross[square, 0:half]
                mixing = jnp.concatenate([left, mixing], axis=1)
            high, rest = split2(mixing)
            values = x[0 : low + half, :]
            rows.append(mm(high, values) + mm(rest, values))
        parts.append(jnp.concatenate(rows, axis=0))
    first = iota((length, LANES), 1) < head_width
    out[...] = jnp.where(first, parts[0], parts[1]) + skip[0:1, :] * x[...].astype(F32)


def whole(shape):
    return pl.BlockSpec(shape, lambda *_: (0,) * len(shape))


def inside(heads, start, stop, seg_t, seg, write, read, x, skip, held=None, waits=()):
    length, width = x.shape
    column = pl.BlockSpec((length, LANES), lambda j: (0, j + start))
    share = (stop - start) / (width // LANES)
    operands = (seg_t, seg, write, read, x, skip)
    specs = [
        whole((length, LANES)), whole((LANES, length)), whole(write.shape), whole(read.shape),
        column, pl.BlockSpec((8, LANES), lambda j: (0, j + start)),
    ]
    aliases = {}
    if held is not None:
        aliases = {len(operands): 0}
        operands = operands + (held,)
        specs = specs + [WAIT]
    operands = operands + tuple(waits)
    specs = specs + [WAIT] * len(waits)
    return pl.pallas_call(
        functools.partial(inside_kernel, width // heads, start),
        name="inside",
        grid=(stop - start,),
        in_specs=specs,
        out_specs=column,
        out_shape=jax.ShapeDtypeStruct((length, width), F32),
        scratch_shapes=[pltpu.VMEM((length, length), F32)],
        input_output_aliases=aliases,
        compiler_params=params(),
        cost_estimate=cost(20e9 * share, 5e6 * share),
    )(*operands)


def gathered_total(pays, k):
    tail = pays[k][HALF : HALF + 8, :].astype(F32)
    return tail[0:1, :] + tail[1:2, :] + tail[2:3, :]


def boundary(totals, near, far, sources, position, count):
    width = totals.shape[1]
    column = jnp.zeros((count, 1), jnp.int32)
    for k in range(count):
        column = jnp.where(iota((count, 1), 0) == k, sources[k], column)
    powers = jnp.zeros((count, width), F32)
    for j in range(count):
        between = jnp.logical_and(column < sources[j], sources[j] < position)
        powers = powers + jnp.where(between, totals[j : j + 1, :], 0.0)
    weights = jnp.where(column < position, jnp.exp(powers), 0.0)
    upper = jnp.zeros((HALF, width), F32)
    lower = jnp.zeros((HALF, width), F32)
    for k in range(count):
        upper = upper + weights[k : k + 1, :] * near[k][0:HALF, :].astype(F32)
        lower = lower + weights[k : k + 1, :] * far[k][...].astype(F32)
    return upper, lower


def enter_kernel(
    count, sources, y_local, gate, grad_v, gain, read, seg_t, spread2, *rest,
):
    near, far = rest[:count], rest[count : 2 * count]
    y_out, scaled_t_out, stats_out, state_out, totals_out, state2 = rest[2 * count :]

    @pl.when(pl.program_id(0) == 0)
    def _():
        for k in range(count):
            totals_out[k : k + 1, :] = gathered_total(near, k)
        upper, lower = boundary(totals_out[...], near, far, sources, sources[count], count)
        state_out[0:HALF, :] = upper
        state_out[HALF:, :] = lower
        state2[0:LANES, :], state2[LANES:, :] = split2(state_out[...])

    from_start = spread(jnp.exp(seg_t[...]), spread2[...])
    read_part = read[...]
    carried = mm(jnp.concatenate([read_part, read_part], axis=1), state2[...])
    y = y_local[...] + from_start * carried
    y_out[...] = y
    z = gate[...].astype(F32)
    mixed = y * z / (1.0 + jnp.exp(-z))
    with_gain = mixed * gain[...]
    scaled_t_out[...] = with_gain.T
    squares = jnp.sum(mixed * mixed, axis=1, keepdims=True)
    inner = jnp.sum(grad_v[...] * with_gain, axis=1, keepdims=True)
    lane = iota((squares.shape[0], LANES), 1)
    stats = jnp.where(lane == 0, squares, jnp.where(lane == 1, inner, 0.0))
    stats_out[...] = stats.T[0:8, :]


def enter(sources, y_local, gate, grad_v, gain, read, seg_t, spread2, near, far):
    length, width = y_local.shape
    count = len(near)
    block = LANES
    token = pl.BlockSpec((block, width), lambda i, *_: (i, 0))
    narrow = pl.BlockSpec((block, LANES), lambda i, *_: (i, 0))
    shapes = (
        jax.ShapeDtypeStruct((length, width), F32),
        jax.ShapeDtypeStruct((width, length), F32),
        jax.ShapeDtypeStruct((8, length), F32),
        jax.ShapeDtypeStruct((LANES, width), F32),
        jax.ShapeDtypeStruct((count, width), F32),
    )
    return pl.pallas_call(
        functools.partial(enter_kernel, count),
        name="enter",
        grid_spec=pltpu.PrefetchScalarGridSpec(
            num_scalar_prefetch=1,
            grid=(length // block,),
            in_specs=[
                token, token, token, whole((1, width)), narrow, narrow, whole(spread2.shape),
            ] + [whole(near[0].shape)] * count + [whole(far[0].shape)] * count,
            out_specs=[
                token,
                pl.BlockSpec((width, block), lambda i, *_: (0, i)),
                pl.BlockSpec((8, block), lambda i, *_: (0, i)),
                whole((LANES, width)),
                whole((count, width)),
            ],
            scratch_shapes=[pltpu.VMEM((2 * LANES, width), BF16)],
        ),
        out_shape=shapes,
        compiler_params=params(),
        cost_estimate=cost(3e9, 15e6),
    )(sources, y_local, gate, grad_v, gain, read, seg_t, spread2, *near, *far)


def gate_kernel(
    total_width, sources, y_ref, gate, grad_v, gain, stats, x, seg_t, spread2, read_t,
    gate_out, grad_y_out, send_out, keep_out, sums, columns, cot,
):
    step = pl.program_id(0)
    row = iota((LANES, LANES), 0)
    squares, inner = stats[0:1, :], stats[1:2, :]
    scale_row = lax.rsqrt(squares * (1.0 / total_width) + EPSILON)
    back_row = scale_row * scale_row * scale_row * inner * (1.0 / total_width)
    columns[...] = jnp.where(row == 0, scale_row, jnp.where(row == 1, back_row, 0.0)).T
    scale, back = columns[:, 0:1], columns[:, 1:2]
    y = y_ref[...]
    z = gate[...].astype(F32)
    sigma = 1.0 / (1.0 + jnp.exp(-z))
    active = z * sigma
    mixed = y * active
    scaled_v = scale * grad_v[...]
    grad_mixed = scaled_v * gain[...] - mixed * back
    gate_out[...] = (grad_mixed * y * sigma * (1.0 + z * (1.0 - sigma))).astype(BF16)
    grad_y = grad_mixed * active
    grad_y_out[...] = grad_y
    gain_part = jnp.sum(scaled_v * mixed, axis=0, keepdims=True)
    skip_part = jnp.sum(grad_y * x[...].astype(F32), axis=0, keepdims=True)
    from_start = spread(jnp.exp(seg_t[...]), spread2[...])
    cot_part = mm(read_t[...], (grad_y * from_start).astype(BF16))
    wide = iota((8, grad_y.shape[1]), 0)
    sum_part = jnp.where(wide == 0, gain_part, jnp.where(wide == 1, skip_part, 0.0))

    @pl.when(step == 0)
    def _():
        cot[...] = cot_part
        sums[...] = sum_part

    @pl.when(step > 0)
    def _():
        cot[...] += cot_part
        sums[...] += sum_part

    @pl.when(step == pl.num_programs(0) - 1)
    def _():
        parity = lax.rem(sources[sources.shape[0] - 1], 2)
        keep_out[...] = cot[pl.ds(pl.multiple_of(parity * HALF, HALF), HALF), :]
        send_out[...] = cot[pl.ds(pl.multiple_of((1 - parity) * HALF, HALF), HALF), :].astype(BF16)


def gate_grads(total_width, sources, y, gate, grad_v, gain, stats, x, seg_t, spread2, read_t):
    length, width = y.shape
    block = LANES
    token = pl.BlockSpec((block, width), lambda i, *_: (i, 0))
    narrow = pl.BlockSpec((block, LANES), lambda i, *_: (i, 0))
    shapes = (
        jax.ShapeDtypeStruct((length, width), BF16),
        jax.ShapeDtypeStruct((length, width), F32),
        jax.ShapeDtypeStruct((HALF, width), BF16),
        jax.ShapeDtypeStruct((HALF, width), F32),
        jax.ShapeDtypeStruct((8, width), F32),
    )
    return pl.pallas_call(
        functools.partial(gate_kernel, total_width),
        name="gate_grads",
        grid_spec=pltpu.PrefetchScalarGridSpec(
            num_scalar_prefetch=1,
            grid=(length // block,),
            in_specs=[
                token, token, token, whole((1, width)), pl.BlockSpec((8, block), lambda i, *_: (0, i)),
                token, narrow, whole(spread2.shape), pl.BlockSpec((LANES, block), lambda i, *_: (0, i)),
            ],
            out_specs=[
                token, token, whole((HALF, width)), whole((HALF, width)), whole((8, width)),
            ],
            scratch_shapes=[pltpu.VMEM((LANES, LANES), F32), pltpu.VMEM((LANES, width), F32)],
        ),
        out_shape=shapes,
        compiler_params=params(),
        cost_estimate=cost(3e9, 15e6),
    )(sources, y, gate, grad_v, gain, stats, x, seg_t, spread2, read_t)


def inside_back_kernel(
    head_width, start, last, seg_t, seg, write, read, x, grad_y, *rest,
):
    step = pl.program_id(0) + start
    if last:
        before, out, grad_write, grad_read, cross, grad_cross = rest[-6:]
    else:
        out, sum_out, cross, grad_cross = rest[-4:]
    length = x.shape[0]
    half = length // 2

    @pl.when(pl.program_id(0) == 0)
    def _():
        cross[...] = mm_t(write[...], read[...])
        grad_cross[...] = before[...] if last else jnp.zeros_like(grad_cross)

    diagonal = iota((half, half), 0) <= iota((half, half), 1)
    first = iota((length, LANES), 1) < head_width
    grads = grad_y[...].astype(BF16)
    values = x[...]
    parts = []
    for side, column, row in pair_columns(seg_t, seg, step):
        mine = first if side == 0 else jnp.logical_not(first)
        own = jnp.where(mine, values, jnp.zeros_like(values))
        rows = []
        for block in (0, 1):
            low = block * half
            square = slice(low, low + half)
            gap = row[:, square] - column[square]
            decayed = jnp.where(diagonal, jnp.exp(jnp.minimum(gap, 0.0)), 0.0)
            mixing = decayed * cross[square, square]
            grad_cross[square, square] += mm_t(own[square], grads[square]) * decayed
            if block == 0:
                decayed = jnp.exp(row[:, half:] - column[square])
                mixing = jnp.concatenate([mixing, decayed * cross[square, half:]], axis=1)
                grad_cross[square, half:] += mm_t(own[square], grads[half:]) * decayed
            rows.append(mm(mixing.astype(BF16), grads[low:]))
        parts.append(jnp.concatenate(rows, axis=0))
    out[...] = jnp.where(first, parts[0], parts[1])

    @pl.when(pl.program_id(0) == pl.num_programs(0) - 1)
    def _():
        if last:
            high, low = split2(grad_cross[...])
            grad_write[...] = mm(high, read[...]) + mm(low, read[...])
            turned = grad_cross[...].T
            high, low = split2(turned)
            grad_read[...] = mm(high, write[...]) + mm(low, write[...])
        else:
            sum_out[...] = grad_cross[...]


def inside_back(heads, start, stop, seg_t, seg, write, read, x, grad_y, held=None, before=None):
    length, width = x.shape
    last = held is not None
    column = pl.BlockSpec((length, LANES), lambda j: (0, j + start))
    square = (length, length)
    small = (length, LANES)
    operands = (seg_t, seg, write, read, x, grad_y)
    specs = [
        whole((length, LANES)), whole((LANES, length)), whole(write.shape), whole(read.shape),
        column, column,
    ]
    share = (stop - start) / (width // LANES)
    outs = (jax.ShapeDtypeStruct((length, width), F32),)
    aliases = {}
    if last:
        operands = operands + (held, before)
        specs = specs + [WAIT, whole(square)]
        aliases = {6: 0}
        outs = outs + (jax.ShapeDtypeStruct(small, F32), jax.ShapeDtypeStruct(small, F32))
        out_specs = [column, whole(small), whole(small)]
    else:
        outs = outs + (jax.ShapeDtypeStruct(square, F32),)
        out_specs = [column, whole(square)]
    return pl.pallas_call(
        functools.partial(inside_back_kernel, width // heads, start, last),
        name="inside_back",
        grid=(stop - start,),
        in_specs=specs,
        out_specs=out_specs,
        out_shape=outs,
        scratch_shapes=[pltpu.VMEM(square, F32), pltpu.VMEM(square, F32)],
        input_output_aliases=aliases,
        compiler_params=params(),
        cost_estimate=cost(20e9 * share, 8e6 * share),
    )(*operands)


def total_of(totals, sources, count, wanted):
    found = jnp.zeros_like(totals[0:1, :])
    for k in range(count):
        found = found + jnp.where(sources[k] == wanted, totals[k : k + 1, :], 0.0)
    return found


def pair_kernel(count, sources, totals, keep, received, out):
    position = sources[count]
    odd = lax.rem(position, 2) == 1
    weight = jnp.exp(total_of(totals, sources, count, position - lax.rem(position, 2)))
    own, other = keep[...], received[...].astype(F32)
    out[...] = jnp.where(odd, other + weight * own, own + weight * other).astype(BF16)


def join_kernel(count, sources, totals, keep, received, *rest):
    shifts = count // 2 - 1
    later, (own_out, send_out) = rest[:shifts], rest[shifts:]
    position = sources[count]
    even_place = position - lax.rem(position, 2)
    odd = lax.rem(position, 2) == 1
    state = jnp.zeros_like(keep)
    power = jnp.zeros_like(totals[0:1, :])
    for shift in range(1, shifts + 1):
        state = state + jnp.exp(power) * later[shift - 1][...].astype(F32)
        if shift < shifts:
            power = power + total_of(totals, sources, count, even_place + 2 * shift)
            power = power + total_of(totals, sources, count, even_place + 2 * shift + 1)
    weight = jnp.exp(total_of(totals, sources, count, even_place + 1))
    of_odd = jnp.where(odd, keep[...], received[...].astype(F32))
    for_even = of_odd + weight * state
    own_out[...] = jnp.where(odd, state, for_even)
    send_out[...] = jnp.where(odd, for_even, state).astype(BF16)


def small_call(kernel, count, outs, sources, *arrays, waits=()):
    return pl.pallas_call(
        skipping(functools.partial(kernel, count), 1 + len(arrays), len(waits)),
        grid_spec=pltpu.PrefetchScalarGridSpec(
            num_scalar_prefetch=1,
            grid=(1,),
            in_specs=[whole(a.shape) for a in arrays] + [WAIT] * len(waits),
            out_specs=[whole(o.shape) for o in outs],
        ),
        out_shape=outs,
        compiler_params=params(),
        cost_estimate=cost(1e9, 2e6),
    )(sources, *arrays, *waits)


def pair_state(totals, sources, send, keep, size):
    partner = [(i, i ^ 1) for i in range(size)]
    received = lax.ppermute(send, "seq", partner)
    narrow = jax.ShapeDtypeStruct(send.shape, BF16)
    (pair,) = small_call(pair_kernel, size, (narrow,), sources, totals, keep, received)
    later = []
    for shift in range(1, size // 2):
        moves = [(i, i - 2 * shift) for i in range(2 * shift, size)]
        later.append(lax.ppermute(pair, "seq", moves))
    return received, later


def join_states(totals, sources, keep, received, later, size, waits):
    narrow = jax.ShapeDtypeStruct(keep.shape, BF16)
    wide = jax.ShapeDtypeStruct(keep.shape, F32)
    own, other = small_call(
        join_kernel, size, (wide, narrow), sources, totals, keep, received, *later,
        waits=waits,
    )
    return own, lax.ppermute(other, "seq", [(i, i ^ 1) for i in range(size)])


def leave_kernel(
    count, heads, sources, y_ref, x_ref, grad_y_ref, inner_ref, write, seg_t, last, spread2,
    skip, state, write_part, read_part, own, other,
    input_out, maps_out, decay_out, cot2, state16, from_head, per_head, sums, cot,
):
    step = pl.program_id(0)
    steps = pl.num_programs(0)
    block, width = y_ref.shape
    length = per_head.shape[0]

    @pl.when(step == 0)
    def _():
        parity = lax.rem(sources[count], 2)
        cot[pl.ds(pl.multiple_of(parity * HALF, HALF), HALF), :] = own[...]
        cot[pl.ds(pl.multiple_of((1 - parity) * HALF, HALF), HALF), :] = other[...].astype(F32)
        cot2[0:LANES, :], cot2[LANES:, :] = split2(cot[...])
        state16[...] = state[...].astype(BF16)
        from_head[...] = spread2[0:LANES, :].T
        ended = spread(jnp.exp(last[...]), spread2[...])
        through = jnp.sum(cot[...] * state[...], axis=0, keepdims=True) * ended[0:1, :]
        sums[...] = jnp.where(iota((8, width), 0) == 0, through, 0.0)

    seg_part = seg_t[...]
    decays = jnp.exp(seg_part)
    to_end = spread(jnp.exp(last[0:1, :] - seg_part), spread2[...])
    from_start = spread(decays, spread2[...])
    x = x_ref[...].astype(F32)
    grad_y = grad_y_ref[...]
    write_rows = write[...]
    from_later = to_end * mm(jnp.concatenate([write_rows, write_rows], axis=1), cot2[...])
    core_grad = inner_ref[...] + from_later
    skip_row = skip[0:1, :]
    input_out[...] = (skip_row * grad_y + core_grad).astype(BF16)
    leaving = jnp.sum(x * from_later, axis=0, keepdims=True)
    sums[...] += jnp.where(iota((8, width), 0) == 0, leaving, 0.0)
    terms = grad_y * (y_ref[...] - skip_row * x) - x * core_grad
    high, low = split2(terms)
    start = pl.multiple_of(step * block, block)
    per_head[pl.ds(start, block), :] = mm(high, from_head[...]) + mm(low, from_head[...])
    maps_out[0] = write_part[...] + mm_t((x * to_end).astype(BF16), cot2[0:LANES, :])
    maps_out[1] = read_part[...] + mm_t((grad_y * from_start).astype(BF16), state16[...])

    @pl.when(step == steps - 1)
    def _():
        final = sum(mm(part, from_head[...]) for part in split3(sums[...]))
        upper = (iota((length, length), 0) <= iota((length, length), 1)).astype(BF16)
        tail = sum(mm(upper, part) for part in split3(per_head[...]))
        decay_out[...] = (tail + final[0:1, :]).T[0:heads, :]


def leave(
    heads, sources, y, x, grad_y, inner, write, seg_t, spread2, skip, state,
    write_part, read_part, own, other, waits,
):
    length, width = y.shape
    count = sources.shape[0] - 1
    block = LANES
    token = pl.BlockSpec((block, width), lambda i, *_: (i, 0))
    narrow = pl.BlockSpec((block, LANES), lambda i, *_: (i, 0))
    shapes = (
        jax.ShapeDtypeStruct((length, width), BF16),
        jax.ShapeDtypeStruct((2, length, LANES), F32),
        jax.ShapeDtypeStruct((heads, length), F32),
    )
    last = jnp.broadcast_to(seg_t[length - 1 :, :], (8, LANES))
    return pl.pallas_call(
        skipping(functools.partial(leave_kernel, count, heads), 15, len(waits)),
        name="leave",
        grid_spec=pltpu.PrefetchScalarGridSpec(
            num_scalar_prefetch=1,
            grid=(length // block,),
            in_specs=[
                token, token, token, token, narrow, narrow, whole((8, LANES)),
                whole(spread2.shape), whole((8, width)), whole((LANES, width)),
                narrow, narrow, whole(own.shape), whole(other.shape),
            ] + [WAIT] * len(waits),
            out_specs=[
                token,
                pl.BlockSpec((2, block, LANES), lambda i, *_: (0, i, 0)),
                whole((heads, length)),
            ],
            scratch_shapes=[
                pltpu.VMEM((2 * LANES, width), BF16),
                pltpu.VMEM((LANES, width), BF16),
                pltpu.VMEM((width, LANES), BF16),
                pltpu.VMEM((length, LANES), F32),
                pltpu.VMEM((8, width), F32),
                pltpu.VMEM((LANES, width), F32),
            ],
        ),
        out_shape=shapes,
        compiler_params=params(),
        cost_estimate=cost(5e9, 20e6),
    )(
        sources, y, x, grad_y, inner, write, seg_t, last, spread2, skip, state,
        write_part, read_part, own, other, *waits,
    )


def product_kernel(masks, group, mine, theirs, cot_mine, cot_theirs, *outs):
    first_rows, second_rows = mine[...], theirs[...]
    for mask, out in zip(masks, outs):
        spot = jnp.bitwise_xor(group[0], mask)
        first = mm_t(cot_mine[spot], first_rows).astype(BF16).astype(F32)
        second = mm_t(cot_theirs[spot], second_rows).astype(BF16).astype(F32)
        out[...] = (first + second).astype(out.dtype)


def products(group, mine, theirs, cot_mine, cot_theirs):
    rows, length = mine.shape
    groups, columns, _ = cot_mine.shape
    masks = list(range(groups - 1, -1, -1))
    block = LANES if rows % LANES == 0 else rows
    side = pl.BlockSpec((block, length), lambda i, *_: (i, 0))
    return pl.pallas_call(
        functools.partial(product_kernel, masks),
        name="product",
        grid_spec=pltpu.PrefetchScalarGridSpec(
            num_scalar_prefetch=1,
            grid=(rows // block,),
            in_specs=[side, side, whole(cot_mine.shape), whole(cot_theirs.shape)],
            out_specs=[pl.BlockSpec((columns, block), lambda i, *_: (0, i))] * groups,
        ),
        out_shape=[
            jax.ShapeDtypeStruct((columns, rows), BF16 if mask else F32) for mask in masks
        ],
        compiler_params=params(),
        cost_estimate=cost(4.0 * rows * length * columns * groups, 5e6),
    )(group, mine, theirs, cot_mine, cot_theirs)


def finish_kernel(count, own, *rest):
    total = own[...]
    for k in range(count):
        total = total + rest[k][...].astype(F32)
    rest[-1][...] = total


def finish(part, parts, own, received, held):
    columns, rows = own.shape
    if rows % LANES:
        total = own + sum(piece.astype(F32) for piece in received)
        return total if held is None else jnp.concatenate([held, total], axis=1)
    small = pl.BlockSpec((columns, rows), lambda i: (0, 0))
    operands = [own, *received]
    specs = [small] * len(operands)
    aliases = {}
    if held is not None:
        aliases = {len(operands): 0}
        operands.append(held)
        specs = specs + [WAIT]
    return pl.pallas_call(
        functools.partial(finish_kernel, len(received)),
        name="finish",
        grid=(1,),
        in_specs=specs,
        out_specs=pl.BlockSpec((columns, rows), lambda i: (0, part)),
        out_shape=jax.ShapeDtypeStruct((columns, parts * rows), F32),
        input_output_aliases=aliases,
        compiler_params=params(),
        cost_estimate=cost(1e9, 4e6),
    )(*operands)


def ring_gather(near, far, size):
    half = size // 2
    order = [2 * q for q in range(half)] + [2 * (size - 1 - q) + 1 for q in range(half, size)]
    ahead = [(order[i], order[(i + 1) % size]) for i in range(size)]
    behind = [(b, a) for a, b in ahead]
    shifts, all_near, all_far = [0], [near], [far]
    up = down = [near, far]
    for hop in range(1, half + 1):
        last = hop == half
        up = [lax.ppermute(v, "seq", ahead) for v in (up[:1] if last else up)]
        down = [lax.ppermute(v, "seq", behind) for v in (down[1:] if last else down)]
        shifts.append(-hop)
        all_near.append(up[0])
        if last:
            all_far.append(down[0])
        else:
            all_far.append(up[1])
            shifts.append(hop)
            all_near.append(down[0])
            all_far.append(down[1])
    return all_near, all_far, shifts


def ring_sources(shifts, size):
    position = lax.axis_index("seq")
    half = size // 2
    place = jnp.where(position % 2 == 0, position // 2, size - 1 - position // 2)
    places = (place + jnp.array(shifts, jnp.int32) + size) % size
    found = jnp.where(places < half, 2 * places, 2 * (size - 1 - places) + 1)
    return jnp.concatenate([found, position[None]]).astype(jnp.int32)


def butterfly_sum(value, axis, size):
    stride = 1
    while stride < size:
        value = value + lax.ppermute(value, axis, [(i, i ^ stride) for i in range(size)])
        stride *= 2
    return value


def all_shards(value, size):
    held = [value]
    masks = [0]
    stride = size // 2
    while stride >= 1:
        moves = [(i, i ^ stride) for i in range(size)]
        held = held + [lax.ppermute(v, "tp", moves) for v in held]
        masks = masks + [m ^ stride for m in masks]
        stride //= 2
    return held, masks


def send_products(pieces, size):
    groups = size // 2
    by_mask = dict(zip(range(groups - 1, -1, -1), pieces))

    def move(value, moves):
        pairs = [(2 * a + p, 2 * b + p) for a, b in moves for p in (0, 1)]
        return lax.ppermute(value, "seq", pairs)

    if groups != 4:
        return [
            move(by_mask[mask], [(g, g ^ mask) for g in range(groups)])
            for mask in range(1, groups)
        ], []
    far = move(by_mask[3], [(0, 1), (3, 2)])
    near = [move(by_mask[3], [(1, 2), (2, 1)]), move(by_mask[1], [(g, g ^ 1) for g in range(4)])]
    merged = (by_mask[2].astype(F32) + far.astype(F32)).astype(BF16)
    return near + [move(merged, [(g, g ^ 2) for g in range(4)])], [merged]


def on_device(
    packed_input, block_exponent, gate_input, state_write, state_read, log_decay,
    skip_weight, norm_gain, out_weight, out_cotangent,
):
    heads, _ = log_decay.shape
    width = packed_input.shape[1]
    seq_size = lax.axis_size("seq")
    tp_size = lax.axis_size("tp")
    total_width = width * tp_size
    columns = out_weight.shape[1] // seq_size
    parity = lax.axis_index("seq") % 2
    partner = [(i, i ^ 1) for i in range(seq_size)]
    gain = norm_gain[None, :]

    x, near, far, seg_t, seg, spread2, skip, read_t = prepare(
        packed_input, block_exponent, log_decay, skip_weight[None, :], state_write, state_read
    )
    near, far, shifts = ring_gather(near, far, seq_size)
    sources = ring_sources(shifts, seq_size)

    other_half = pick(parity[None].astype(jnp.int32), out_cotangent, columns)
    theirs = lax.ppermute(other_half, "seq", partner)
    all_mine, masks = all_shards(out_cotangent, tp_size)
    all_theirs, _ = all_shards(theirs, tp_size)
    owners = jnp.bitwise_xor(lax.axis_index("tp"), jnp.array(masks, jnp.int32))
    owners = jnp.concatenate([owners, parity[None]]).astype(jnp.int32)

    pairs = width // LANES
    calls = min(4, pairs)
    y_local = None
    hops = seq_size // 2
    for call in range(calls):
        start, stop = call * pairs // calls, (call + 1) * pairs // calls
        waits = (*near[1:3], *far[1:3]) if call == 2 and hops > 2 else ()
        y_local = inside(
            heads, start, stop, seg_t, seg, state_write, state_read, x, skip, y_local, waits
        )
    waits = (y_local, *near[3:5], *far[3:5]) if hops > 2 else (y_local,)
    grad_v, cot_mine, cot_theirs = cotangent(
        owners, out_weight, all_mine, all_theirs, columns, waits
    )

    y, scaled_t, stats, state, totals = enter(
        sources, y_local, gate_input, grad_v, gain, state_read, seg_t, spread2, near, far
    )
    stats = butterfly_sum(stats, "tp", tp_size)
    scale = lax.rsqrt(stats[0:1, :] / total_width + EPSILON)
    part_rows = width // NORMED_PARTS
    normed, normed_theirs = [], []
    for part in range(NORMED_PARTS):
        rows = scaled_t[part * part_rows : (part + 1) * part_rows]
        normed.append((rows * scale).astype(BF16))
        normed_theirs.append(lax.ppermute(normed[part], "seq", partner))

    grad_gate, grad_y, send, keep, sums = gate_grads(
        total_width, sources, y, gate_input, grad_v, gain, stats, x, seg_t, spread2, read_t
    )
    received, later = pair_state(totals, sources, send, keep, seq_size)
    middle = pairs // 2
    operands = (seg_t, seg, state_write, state_read, x, grad_y)
    inner, grad_cross = inside_back(heads, 0, middle, *operands)
    inner, write_part, read_part = inside_back(heads, middle, pairs, *operands, inner, grad_cross)
    group = (lax.axis_index("seq") // 2)[None].astype(jnp.int32)
    arrived, own_part, merges = [], [], []
    for part in range(NORMED_PARTS):
        *pieces, last = products(group, normed[part], normed_theirs[part], cot_mine, cot_theirs)
        got, merged = send_products(pieces, seq_size)
        arrived.append(got)
        own_part.append(last)
        merges.append(merged)
    own, other = join_states(
        totals, sources, keep, received, later, seq_size, (write_part, *merges[0])
    )
    grad_input, maps, grad_decay = leave(
        heads, sources, y, x, grad_y, inner, state_write, seg_t, spread2, skip, state,
        write_part, read_part, own, other, tuple(merges[-1]),
    )
    grad_out_weight = None
    for part in range(NORMED_PARTS):
        grad_out_weight = finish(part, NORMED_PARTS, own_part[part], arrived[part], grad_out_weight)
    maps = butterfly_sum(maps, "tp", tp_size)
    sums = butterfly_sum(sums, "seq", seq_size)
    grad_skip = jnp.sum(sums[1].reshape(heads, width // heads), axis=1)
    return (
        grad_input, grad_gate, maps[0], maps[1], grad_decay, grad_skip, sums[0], grad_out_weight.T,
    )


def solution(mesh):
    placed = (
        P("seq", "tp"), P("tp", "seq"), P("seq", "tp"), P("seq", None), P("seq", None),
        P("tp", "seq"), P("tp"), P("tp"), P("tp", None), P("seq", "tp"),
    )
    return jax.shard_map(
        on_device,
        mesh=mesh,
        in_specs=placed,
        out_specs=(
            P("seq", "tp"), P("seq", "tp"), P("seq", None), P("seq", None), P("tp", "seq"),
            P("tp"), P("tp"), P("tp", "seq"),
        ),
        check_vma=False,
    )
```

```python
import functools
import jax
import jax.numpy as jnp
from jax import lax
from jax.experimental import pallas as pl
from jax.experimental.pallas import tpu as pltpu
from jax.sharding import PartitionSpec as P

F32 = jnp.float32
BF16 = jnp.bfloat16
LANES = 128
EXTRA = 16
EPSILON = 1e-05
NORMED_PARTS = 2
HALF = LANES // 2


def mm(a, b):
    return jnp.dot(a, b, preferred_element_type=F32)


def mm_t(a, b):
    return lax.dot_general(a, b, (((1,), (1,)), ((), ())), preferred_element_type=F32)


def split2(v):
    high = v.astype(BF16)
    return high, (v - high.astype(F32)).astype(BF16)


def split3(v):
    high = v.astype(BF16)
    rest = v - high.astype(F32)
    middle = rest.astype(BF16)
    return high, middle, (rest - middle.astype(F32)).astype(BF16)


def iota(shape, axis):
    return lax.broadcasted_iota(jnp.int32, shape, axis)


def spread(values, spread2):
    return mm(jnp.concatenate(split2(values), axis=1), spread2)


FULL_GRANT = 67_043_328


def params(limit=24 << 20):
    return pltpu.CompilerParams(vmem_limit_bytes=limit)


def cost(flops, nbytes, special=0):
    return pl.CostEstimate(flops=int(flops), bytes_accessed=int(nbytes), transcendentals=int(special))


def skipping(kernel, first, extra):
    return lambda *refs: kernel(*refs[:first], *refs[first + extra :])


WAIT = pl.BlockSpec(memory_space=pl.ANY)


def prepare_kernel(
    heads, packed, expo, decay, skip, write, read,
    x_out, near_out, far_out, seg_t_out, seg_out, spread_out, skip_out, read_t_out, pad, pad8,
):
    length, width = x_out.shape
    head_width = width // heads
    rows8 = packed.shape[0]
    groups = expo.shape[0]
    pad[...] = jnp.zeros_like(pad)
    pad[0:heads, :] = decay[...]
    decay_t = pad[...].T
    lower = (iota((length, length), 0) >= iota((length, length), 1)).astype(BF16)
    seg_t = sum(mm(lower, part) for part in split3(decay_t))
    seg_t_out[...] = seg_t
    seg_out[...] = seg_t.T
    of_head = (iota((LANES, width), 1) // head_width == iota((LANES, width), 0)).astype(BF16)
    spread2 = jnp.concatenate([of_head, of_head], axis=0)
    spread_out[...] = spread2
    pad8[...] = jnp.zeros_like(pad8)
    pad8[0:1, 0:heads] = skip[...]
    skip_out[...] = sum(mm(part, of_head) for part in split3(pad8[...]))
    total = seg_t[length - 1 : length, :]
    to_end = spread(jnp.exp(total - seg_t), spread2)
    pad[...] = jnp.zeros_like(pad)
    pad[0:groups, :] = jnp.left_shift(1, expo[...] + 8).astype(F32) * (2.0**-8)
    of_group = (
        iota((LANES, width), 1) // (width // groups) == iota((LANES, width), 0)
    ).astype(BF16)
    factors = mm(pad[...].T.astype(BF16), of_group)
    words = jnp.broadcast_to(packed[...][:, None, :], (rows8, 8, width))
    words = jnp.right_shift(words, 4 * iota((rows8, 8, width), 1))
    fields = (jnp.bitwise_and(words, 15) - 8).astype(F32).reshape(length, width)
    x = fields * factors
    x_out[...] = x.astype(BF16)
    states = mm(write[...].T, (x * to_end).astype(BF16)).astype(BF16)
    read_t_out[...] = read[...].T
    near_out[0:HALF, :] = states[0:HALF, :]
    far_out[...] = states[HALF:, :]
    total8 = jnp.broadcast_to(total, (8, LANES))
    high, middle, low = (mm(part, of_head) for part in split3(total8))
    row = iota((EXTRA, width), 0)
    tail = jnp.where(row == 0, high[0:1, :], jnp.where(row == 1, middle[0:1, :], low[0:1, :]))
    near_out[HALF:, :] = jnp.where(row < 3, tail, 0.0).astype(BF16)


def prepare(packed, expo, decay, skip, write, read):
    heads, length = decay.shape
    width = packed.shape[1]
    shapes = (
        jax.ShapeDtypeStruct((length, width), BF16),
        jax.ShapeDtypeStruct((HALF + EXTRA, width), BF16),
        jax.ShapeDtypeStruct((HALF, width), BF16),
        jax.ShapeDtypeStruct((length, LANES), F32),
        jax.ShapeDtypeStruct((LANES, length), F32),
        jax.ShapeDtypeStruct((2 * LANES, width), BF16),
        jax.ShapeDtypeStruct((8, width), F32),
        jax.ShapeDtypeStruct((LANES, length), BF16),
    )
    return pl.pallas_call(
        functools.partial(prepare_kernel, heads),
        name="prepare",
        out_shape=shapes,
        scratch_shapes=[pltpu.VMEM((LANES, length), F32), pltpu.VMEM((8, LANES), F32)],
        compiler_params=params(FULL_GRANT),
        cost_estimate=cost(3e9, 8e6),
    )(packed, expo, decay, skip, write, read)


def pick_kernel(per_half, columns, parity, shard, out):
    odd_wanted = parity[0] == 0
    for sub in range(per_half):
        even_part = shard[:, 2 * sub * columns : (2 * sub + 1) * columns]
        odd_part = shard[:, (2 * sub + 1) * columns : (2 * sub + 2) * columns]
        out[sub * columns : (sub + 1) * columns, :] = jnp.where(odd_wanted, odd_part, even_part).T


def pick(parity, shard, columns):
    length, shard_width = shard.shape
    out = (shard_width // 2, length)
    return pl.pallas_call(
        functools.partial(pick_kernel, shard_width // (2 * columns), columns),
        name="pick",
        grid_spec=pltpu.PrefetchScalarGridSpec(
            num_scalar_prefetch=1, grid=(1,), in_specs=[whole(shard.shape)], out_specs=whole(out)
        ),
        out_shape=jax.ShapeDtypeStruct(out, BF16),
        compiler_params=params(),
        cost_estimate=cost(1e8, 2e6),
    )(parity, shard)


def cotangent_kernel(shards, per_half, owners, weight, *rest):
    mine = rest[:shards]
    grad_v, cot_mine, full = rest[shards:]
    shard_width = mine[0].shape[1]
    columns = cot_mine.shape[1]

    @pl.when(pl.program_id(0) == 0)
    def _():
        odd = owners[shards] == 1
        for m in range(shards):
            for q in range(shards):
                @pl.when(owners[m] == q)
                def _():
                    full[:, q * shard_width : (q + 1) * shard_width] = mine[m][...]
            for sub in range(per_half):
                even_part = mine[m][:, 2 * sub * columns : (2 * sub + 1) * columns]
                odd_part = mine[m][:, (2 * sub + 1) * columns : (2 * sub + 2) * columns]
                cot_mine[owners[m] * per_half + sub] = jnp.where(odd, odd_part, even_part).T

    grad_v[...] = mm_t(full[...], weight[...])


def cotangent(owners, weight, mine, columns, waits):
    shards = len(mine)
    length, shard_width = mine[0].shape
    width, model_width = weight.shape
    per_half = shard_width // (2 * columns)
    block = 2 * LANES if width % (2 * LANES) == 0 else LANES
    stacked = (shards * per_half, columns, length)
    return pl.pallas_call(
        skipping(functools.partial(cotangent_kernel, shards, per_half), 2 + shards, len(waits)),
        name="cotangent",
        grid_spec=pltpu.PrefetchScalarGridSpec(
            num_scalar_prefetch=1,
            grid=(width // block,),
            in_specs=[pl.BlockSpec((block, model_width), lambda i, *_: (i, 0))]
            + [whole(mine[0].shape)] * shards
            + [WAIT] * len(waits),
            out_specs=[pl.BlockSpec((length, block), lambda i, *_: (0, i)), whole(stacked)],
            scratch_shapes=[pltpu.VMEM((length, model_width), BF16)],
        ),
        out_shape=(
            jax.ShapeDtypeStruct((length, width), F32),
            jax.ShapeDtypeStruct(stacked, BF16),
        ),
        compiler_params=params(),
        cost_estimate=cost(2.0 * length * width * model_width, 20e6),
    )(owners, weight, *mine, *waits)


def stack_kernel(shards, owners, *rest):
    theirs, out = rest[:shards], rest[shards]
    columns = out.shape[1]
    per_half = theirs[0].shape[0] // columns
    for m in range(shards):
        for sub in range(per_half):
            rows = slice(sub * columns, (sub + 1) * columns)
            out[owners[m] * per_half + sub] = theirs[m][rows, :]


def stack(owners, theirs, columns):
    rows, length = theirs[0].shape
    out = (len(theirs) * rows // columns, columns, length)
    return pl.pallas_call(
        functools.partial(stack_kernel, len(theirs)),
        name="stack",
        grid_spec=pltpu.PrefetchScalarGridSpec(
            num_scalar_prefetch=1,
            grid=(1,),
            in_specs=[whole(theirs[0].shape)] * len(theirs),
            out_specs=whole(out),
        ),
        out_shape=jax.ShapeDtypeStruct(out, BF16),
        compiler_params=params(),
        cost_estimate=cost(1e8, 3e6),
    )(owners, *theirs)


def pair_columns(seg_t, seg, step):
    rolled = pltpu.roll(seg_t[...], lax.rem(LANES - 2 * step, LANES), 1)
    for side in (0, 1):
        yield side, rolled[:, side : side + 1], seg[pl.ds(2 * step + side, 1), :]


def inside_kernel(head_width, start, seg_t, seg, write, read, x, skip, *rest):
    out, cross = rest[-2:]
    step = pl.program_id(0) + start
    length = x.shape[0]
    half = length // 2

    @pl.when(pl.program_id(0) == 0)
    def _():
        cross[...] = mm_t(read[...], write[...])

    diagonal = iota((half, half), 0) >= iota((half, half), 1)
    parts = []
    for side, column, row in pair_columns(seg_t, seg, step):
        rows = []
        for block in (0, 1):
            low = block * half
            square = slice(low, low + half)
            gap = column[square] - row[:, square]
            decayed = jnp.where(diagonal, jnp.exp(jnp.minimum(gap, 0.0)), 0.0)
            mixing = decayed * cross[square, square]
            if block == 1:
                left = jnp.exp(column[square] - row[:, 0:half]) * cross[square, 0:half]
                mixing = jnp.concatenate([left, mixing], axis=1)
            high, rest = split2(mixing)
            values = x[0 : low + half, :]
            rows.append(mm(high, values) + mm(rest, values))
        parts.append(jnp.concatenate(rows, axis=0))
    first = iota((length, LANES), 1) < head_width
    out[...] = jnp.where(first, parts[0], parts[1]) + skip[0:1, :] * x[...].astype(F32)


def whole(shape):
    return pl.BlockSpec(shape, lambda *_: (0,) * len(shape))


def inside(heads, start, stop, seg_t, seg, write, read, x, skip, held=None, waits=()):
    length, width = x.shape
    column = pl.BlockSpec((length, LANES), lambda j: (0, j + start))
    share = (stop - start) / (width // LANES)
    operands = (seg_t, seg, write, read, x, skip)
    specs = [
        whole((length, LANES)), whole((LANES, length)), whole(write.shape), whole(read.shape),
        column, pl.BlockSpec((8, LANES), lambda j: (0, j + start)),
    ]
    aliases = {}
    if held is not None:
        aliases = {len(operands): 0}
        operands = operands + (held,)
        specs = specs + [WAIT]
    operands = operands + tuple(waits)
    specs = specs + [WAIT] * len(waits)
    return pl.pallas_call(
        functools.partial(inside_kernel, width // heads, start),
        name="inside",
        grid=(stop - start,),
        in_specs=specs,
        out_specs=column,
        out_shape=jax.ShapeDtypeStruct((length, width), F32),
        scratch_shapes=[pltpu.VMEM((length, length), F32)],
        input_output_aliases=aliases,
        compiler_params=params(),
        cost_estimate=cost(20e9 * share, 5e6 * share),
    )(*operands)


def gathered_total(pays, k):
    tail = pays[k][HALF : HALF + 8, :].astype(F32)
    return tail[0:1, :] + tail[1:2, :] + tail[2:3, :]


def boundary(totals, near, far, sources, position, count):
    width = totals.shape[1]
    column = jnp.zeros((count, 1), jnp.int32)
    for k in range(count):
        column = jnp.where(iota((count, 1), 0) == k, sources[k], column)
    powers = jnp.zeros((count, width), F32)
    for j in range(count):
        between = jnp.logical_and(column < sources[j], sources[j] < position)
        powers = powers + jnp.where(between, totals[j : j + 1, :], 0.0)
    weights = jnp.where(column < position, jnp.exp(powers), 0.0)
    upper = jnp.zeros((HALF, width), F32)
    lower = jnp.zeros((HALF, width), F32)
    for k in range(count):
        upper = upper + weights[k : k + 1, :] * near[k][0:HALF, :].astype(F32)
        lower = lower + weights[k : k + 1, :] * far[k][...].astype(F32)
    return upper, lower


def enter_kernel(
    count, sources, y_local, gate, grad_v, gain, read, seg_t, spread2, *rest,
):
    near, far = rest[:count], rest[count : 2 * count]
    y_out, scaled_t_out, stats_out, state_out, totals_out, state2 = rest[2 * count :]

    @pl.when(pl.program_id(0) == 0)
    def _():
        for k in range(count):
            totals_out[k : k + 1, :] = gathered_total(near, k)
        upper, lower = boundary(totals_out[...], near, far, sources, sources[count], count)
        state_out[0:HALF, :] = upper
        state_out[HALF:, :] = lower
        state2[0:LANES, :], state2[LANES:, :] = split2(state_out[...])

    from_start = spread(jnp.exp(seg_t[...]), spread2[...])
    read_part = read[...]
    carried = mm(jnp.concatenate([read_part, read_part], axis=1), state2[...])
    y = y_local[...] + from_start * carried
    y_out[...] = y
    z = gate[...].astype(F32)
    mixed = y * z / (1.0 + jnp.exp(-z))
    with_gain = mixed * gain[...]
    scaled_t_out[...] = with_gain.T
    squares = jnp.sum(mixed * mixed, axis=1, keepdims=True)
    inner = jnp.sum(grad_v[...] * with_gain, axis=1, keepdims=True)
    lane = iota((squares.shape[0], LANES), 1)
    stats = jnp.where(lane == 0, squares, jnp.where(lane == 1, inner, 0.0))
    stats_out[...] = stats.T[0:8, :]


def enter(sources, y_local, gate, grad_v, gain, read, seg_t, spread2, near, far):
    length, width = y_local.shape
    count = len(near)
    block = LANES
    token = pl.BlockSpec((block, width), lambda i, *_: (i, 0))
    narrow = pl.BlockSpec((block, LANES), lambda i, *_: (i, 0))
    shapes = (
        jax.ShapeDtypeStruct((length, width), F32),
        jax.ShapeDtypeStruct((width, length), F32),
        jax.ShapeDtypeStruct((8, length), F32),
        jax.ShapeDtypeStruct((LANES, width), F32),
        jax.ShapeDtypeStruct((count, width), F32),
    )
    return pl.pallas_call(
        functools.partial(enter_kernel, count),
        name="enter",
        grid_spec=pltpu.PrefetchScalarGridSpec(
            num_scalar_prefetch=1,
            grid=(length // block,),
            in_specs=[
                token, token, token, whole((1, width)), narrow, narrow, whole(spread2.shape),
            ] + [whole(near[0].shape)] * count + [whole(far[0].shape)] * count,
            out_specs=[
                token,
                pl.BlockSpec((width, block), lambda i, *_: (0, i)),
                pl.BlockSpec((8, block), lambda i, *_: (0, i)),
                whole((LANES, width)),
                whole((count, width)),
            ],
            scratch_shapes=[pltpu.VMEM((2 * LANES, width), BF16)],
        ),
        out_shape=shapes,
        compiler_params=params(),
        cost_estimate=cost(3e9, 15e6),
    )(sources, y_local, gate, grad_v, gain, read, seg_t, spread2, *near, *far)


def gate_kernel(
    total_width, sources, y_ref, gate, grad_v, gain, stats, x, seg_t, spread2, read_t,
    gate_out, grad_y_out, send_out, keep_out, sums, columns, cot,
):
    step = pl.program_id(0)
    row = iota((LANES, LANES), 0)
    squares, inner = stats[0:1, :], stats[1:2, :]
    scale_row = lax.rsqrt(squares * (1.0 / total_width) + EPSILON)
    back_row = scale_row * scale_row * scale_row * inner * (1.0 / total_width)
    columns[...] = jnp.where(row == 0, scale_row, jnp.where(row == 1, back_row, 0.0)).T
    scale, back = columns[:, 0:1], columns[:, 1:2]
    y = y_ref[...]
    z = gate[...].astype(F32)
    sigma = 1.0 / (1.0 + jnp.exp(-z))
    active = z * sigma
    mixed = y * active
    scaled_v = scale * grad_v[...]
    grad_mixed = scaled_v * gain[...] - mixed * back
    gate_out[...] = (grad_mixed * y * sigma * (1.0 + z * (1.0 - sigma))).astype(BF16)
    grad_y = grad_mixed * active
    grad_y_out[...] = grad_y
    gain_part = jnp.sum(scaled_v * mixed, axis=0, keepdims=True)
    skip_part = jnp.sum(grad_y * x[...].astype(F32), axis=0, keepdims=True)
    from_start = spread(jnp.exp(seg_t[...]), spread2[...])
    cot_part = mm(read_t[...], (grad_y * from_start).astype(BF16))
    wide = iota((8, grad_y.shape[1]), 0)
    sum_part = jnp.where(wide == 0, gain_part, jnp.where(wide == 1, skip_part, 0.0))

    @pl.when(step == 0)
    def _():
        cot[...] = cot_part
        sums[...] = sum_part

    @pl.when(step > 0)
    def _():
        cot[...] += cot_part
        sums[...] += sum_part

    @pl.when(step == pl.num_programs(0) - 1)
    def _():
        parity = lax.rem(sources[sources.shape[0] - 1], 2)
        keep_out[...] = cot[pl.ds(pl.multiple_of(parity * HALF, HALF), HALF), :]
        send_out[...] = cot[pl.ds(pl.multiple_of((1 - parity) * HALF, HALF), HALF), :].astype(BF16)


def gate_grads(total_width, sources, y, gate, grad_v, gain, stats, x, seg_t, spread2, read_t):
    length, width = y.shape
    block = LANES
    token = pl.BlockSpec((block, width), lambda i, *_: (i, 0))
    narrow = pl.BlockSpec((block, LANES), lambda i, *_: (i, 0))
    shapes = (
        jax.ShapeDtypeStruct((length, width), BF16),
        jax.ShapeDtypeStruct((length, width), F32),
        jax.ShapeDtypeStruct((HALF, width), BF16),
        jax.ShapeDtypeStruct((HALF, width), F32),
        jax.ShapeDtypeStruct((8, width), F32),
    )
    return pl.pallas_call(
        functools.partial(gate_kernel, total_width),
        name="gate_grads",
        grid_spec=pltpu.PrefetchScalarGridSpec(
            num_scalar_prefetch=1,
            grid=(length // block,),
            in_specs=[
                token, token, token, whole((1, width)), pl.BlockSpec((8, block), lambda i, *_: (0, i)),
                token, narrow, whole(spread2.shape), pl.BlockSpec((LANES, block), lambda i, *_: (0, i)),
            ],
            out_specs=[
                token, token, whole((HALF, width)), whole((HALF, width)), whole((8, width)),
            ],
            scratch_shapes=[pltpu.VMEM((LANES, LANES), F32), pltpu.VMEM((LANES, width), F32)],
        ),
        out_shape=shapes,
        compiler_params=params(),
        cost_estimate=cost(3e9, 15e6),
    )(sources, y, gate, grad_v, gain, stats, x, seg_t, spread2, read_t)


def inside_back_kernel(
    head_width, start, last, seg_t, seg, write, read, x, grad_y, *rest,
):
    step = pl.program_id(0) + start
    if last:
        before, out, grad_write, grad_read, cross, grad_cross = rest[-6:]
    else:
        out, sum_out, cross, grad_cross = rest[-4:]
    length = x.shape[0]
    half = length // 2

    @pl.when(pl.program_id(0) == 0)
    def _():
        cross[...] = mm_t(write[...], read[...])
        grad_cross[...] = before[...] if last else jnp.zeros_like(grad_cross)

    diagonal = iota((half, half), 0) <= iota((half, half), 1)
    first = iota((length, LANES), 1) < head_width
    grads = grad_y[...].astype(BF16)
    values = x[...]
    parts = []
    for side, column, row in pair_columns(seg_t, seg, step):
        mine = first if side == 0 else jnp.logical_not(first)
        own = jnp.where(mine, values, jnp.zeros_like(values))
        rows = []
        for block in (0, 1):
            low = block * half
            square = slice(low, low + half)
            gap = row[:, square] - column[square]
            decayed = jnp.where(diagonal, jnp.exp(jnp.minimum(gap, 0.0)), 0.0)
            mixing = decayed * cross[square, square]
            grad_cross[square, square] += mm_t(own[square], grads[square]) * decayed
            if block == 0:
                decayed = jnp.exp(row[:, half:] - column[square])
                mixing = jnp.concatenate([mixing, decayed * cross[square, half:]], axis=1)
                grad_cross[square, half:] += mm_t(own[square], grads[half:]) * decayed
            rows.append(mm(mixing.astype(BF16), grads[low:]))
        parts.append(jnp.concatenate(rows, axis=0))
    out[...] = jnp.where(first, parts[0], parts[1])

    @pl.when(pl.program_id(0) == pl.num_programs(0) - 1)
    def _():
        if last:
            high, low = split2(grad_cross[...])
            grad_write[...] = mm(high, read[...]) + mm(low, read[...])
            turned = grad_cross[...].T
            high, low = split2(turned)
            grad_read[...] = mm(high, write[...]) + mm(low, write[...])
        else:
            sum_out[...] = grad_cross[...]


def inside_back(heads, start, stop, seg_t, seg, write, read, x, grad_y, held=None, before=None):
    length, width = x.shape
    last = held is not None
    column = pl.BlockSpec((length, LANES), lambda j: (0, j + start))
    square = (length, length)
    small = (length, LANES)
    operands = (seg_t, seg, write, read, x, grad_y)
    specs = [
        whole((length, LANES)), whole((LANES, length)), whole(write.shape), whole(read.shape),
        column, column,
    ]
    share = (stop - start) / (width // LANES)
    outs = (jax.ShapeDtypeStruct((length, width), F32),)
    aliases = {}
    if last:
        operands = operands + (held, before)
        specs = specs + [WAIT, whole(square)]
        aliases = {6: 0}
        outs = outs + (jax.ShapeDtypeStruct(small, F32), jax.ShapeDtypeStruct(small, F32))
        out_specs = [column, whole(small), whole(small)]
    else:
        outs = outs + (jax.ShapeDtypeStruct(square, F32),)
        out_specs = [column, whole(square)]
    return pl.pallas_call(
        functools.partial(inside_back_kernel, width // heads, start, last),
        name="inside_back",
        grid=(stop - start,),
        in_specs=specs,
        out_specs=out_specs,
        out_shape=outs,
        scratch_shapes=[pltpu.VMEM(square, F32), pltpu.VMEM(square, F32)],
        input_output_aliases=aliases,
        compiler_params=params(),
        cost_estimate=cost(20e9 * share, 8e6 * share),
    )(*operands)


def total_of(totals, sources, count, wanted):
    found = jnp.zeros_like(totals[0:1, :])
    for k in range(count):
        found = found + jnp.where(sources[k] == wanted, totals[k : k + 1, :], 0.0)
    return found


def pair_kernel(count, sources, totals, keep, received, out):
    position = sources[count]
    odd = lax.rem(position, 2) == 1
    weight = jnp.exp(total_of(totals, sources, count, position - lax.rem(position, 2)))
    own, other = keep[...], received[...].astype(F32)
    out[...] = jnp.where(odd, other + weight * own, own + weight * other).astype(BF16)


def join_kernel(count, sources, totals, keep, received, *rest):
    shifts = count // 2 - 1
    later, (own_out, send_out) = rest[:shifts], rest[shifts:]
    position = sources[count]
    even_place = position - lax.rem(position, 2)
    odd = lax.rem(position, 2) == 1
    state = jnp.zeros_like(keep)
    power = jnp.zeros_like(totals[0:1, :])
    for shift in range(1, shifts + 1):
        state = state + jnp.exp(power) * later[shift - 1][...].astype(F32)
        if shift < shifts:
            power = power + total_of(totals, sources, count, even_place + 2 * shift)
            power = power + total_of(totals, sources, count, even_place + 2 * shift + 1)
    weight = jnp.exp(total_of(totals, sources, count, even_place + 1))
    of_odd = jnp.where(odd, keep[...], received[...].astype(F32))
    for_even = of_odd + weight * state
    own_out[...] = jnp.where(odd, state, for_even)
    send_out[...] = jnp.where(odd, for_even, state).astype(BF16)


def small_call(kernel, count, outs, sources, *arrays, waits=()):
    return pl.pallas_call(
        skipping(functools.partial(kernel, count), 1 + len(arrays), len(waits)),
        grid_spec=pltpu.PrefetchScalarGridSpec(
            num_scalar_prefetch=1,
            grid=(1,),
            in_specs=[whole(a.shape) for a in arrays] + [WAIT] * len(waits),
            out_specs=[whole(o.shape) for o in outs],
        ),
        out_shape=outs,
        compiler_params=params(),
        cost_estimate=cost(1e9, 2e6),
    )(sources, *arrays, *waits)


def pair_state(totals, sources, send, keep, size):
    partner = [(i, i ^ 1) for i in range(size)]
    received = lax.ppermute(send, "seq", partner)
    narrow = jax.ShapeDtypeStruct(send.shape, BF16)
    (pair,) = small_call(pair_kernel, size, (narrow,), sources, totals, keep, received)
    later = []
    for shift in range(1, size // 2):
        moves = [(i, i - 2 * shift) for i in range(2 * shift, size)]
        later.append(lax.ppermute(pair, "seq", moves))
    return received, later


def join_states(totals, sources, keep, received, later, size, waits):
    narrow = jax.ShapeDtypeStruct(keep.shape, BF16)
    wide = jax.ShapeDtypeStruct(keep.shape, F32)
    own, other = small_call(
        join_kernel, size, (wide, narrow), sources, totals, keep, received, *later,
        waits=waits,
    )
    return own, lax.ppermute(other, "seq", [(i, i ^ 1) for i in range(size)])


def leave_kernel(
    count, heads, sources, y_ref, x_ref, grad_y_ref, inner_ref, write, seg_t, last, spread2,
    skip, state, write_part, read_part, own, other,
    input_out, maps_out, decay_out, cot2, state16, from_head, per_head, sums, cot,
):
    step = pl.program_id(0)
    steps = pl.num_programs(0)
    block, width = y_ref.shape
    length = per_head.shape[0]

    @pl.when(step == 0)
    def _():
        parity = lax.rem(sources[count], 2)
        cot[pl.ds(pl.multiple_of(parity * HALF, HALF), HALF), :] = own[...]
        cot[pl.ds(pl.multiple_of((1 - parity) * HALF, HALF), HALF), :] = other[...].astype(F32)
        cot2[0:LANES, :], cot2[LANES:, :] = split2(cot[...])
        state16[...] = state[...].astype(BF16)
        from_head[...] = spread2[0:LANES, :].T
        ended = spread(jnp.exp(last[...]), spread2[...])
        through = jnp.sum(cot[...] * state[...], axis=0, keepdims=True) * ended[0:1, :]
        sums[...] = jnp.where(iota((8, width), 0) == 0, through, 0.0)

    seg_part = seg_t[...]
    decays = jnp.exp(seg_part)
    to_end = spread(jnp.exp(last[0:1, :] - seg_part), spread2[...])
    from_start = spread(decays, spread2[...])
    x = x_ref[...].astype(F32)
    grad_y = grad_y_ref[...]
    write_rows = write[...]
    from_later = to_end * mm(jnp.concatenate([write_rows, write_rows], axis=1), cot2[...])
    core_grad = inner_ref[...] + from_later
    skip_row = skip[0:1, :]
    input_out[...] = (skip_row * grad_y + core_grad).astype(BF16)
    leaving = jnp.sum(x * from_later, axis=0, keepdims=True)
    sums[...] += jnp.where(iota((8, width), 0) == 0, leaving, 0.0)
    terms = grad_y * (y_ref[...] - skip_row * x) - x * core_grad
    high, low = split2(terms)
    start = pl.multiple_of(step * block, block)
    per_head[pl.ds(start, block), :] = mm(high, from_head[...]) + mm(low, from_head[...])
    maps_out[0] = write_part[...] + mm_t((x * to_end).astype(BF16), cot2[0:LANES, :])
    maps_out[1] = read_part[...] + mm_t((grad_y * from_start).astype(BF16), state16[...])

    @pl.when(step == steps - 1)
    def _():
        final = sum(mm(part, from_head[...]) for part in split3(sums[...]))
        upper = (iota((length, length), 0) <= iota((length, length), 1)).astype(BF16)
        tail = sum(mm(upper, part) for part in split3(per_head[...]))
        decay_out[...] = (tail + final[0:1, :]).T[0:heads, :]


def leave(
    heads, sources, y, x, grad_y, inner, write, seg_t, spread2, skip, state,
    write_part, read_part, own, other, waits,
):
    length, width = y.shape
    count = sources.shape[0] - 1
    block = LANES
    token = pl.BlockSpec((block, width), lambda i, *_: (i, 0))
    narrow = pl.BlockSpec((block, LANES), lambda i, *_: (i, 0))
    shapes = (
        jax.ShapeDtypeStruct((length, width), BF16),
        jax.ShapeDtypeStruct((2, length, LANES), F32),
        jax.ShapeDtypeStruct((heads, length), F32),
    )
    last = jnp.broadcast_to(seg_t[length - 1 :, :], (8, LANES))
    return pl.pallas_call(
        skipping(functools.partial(leave_kernel, count, heads), 15, len(waits)),
        name="leave",
        grid_spec=pltpu.PrefetchScalarGridSpec(
            num_scalar_prefetch=1,
            grid=(length // block,),
            in_specs=[
                token, token, token, token, narrow, narrow, whole((8, LANES)),
                whole(spread2.shape), whole((8, width)), whole((LANES, width)),
                narrow, narrow, whole(own.shape), whole(other.shape),
            ] + [WAIT] * len(waits),
            out_specs=[
                token,
                pl.BlockSpec((2, block, LANES), lambda i, *_: (0, i, 0)),
                whole((heads, length)),
            ],
            scratch_shapes=[
                pltpu.VMEM((2 * LANES, width), BF16),
                pltpu.VMEM((LANES, width), BF16),
                pltpu.VMEM((width, LANES), BF16),
                pltpu.VMEM((length, LANES), F32),
                pltpu.VMEM((8, width), F32),
                pltpu.VMEM((LANES, width), F32),
            ],
        ),
        out_shape=shapes,
        compiler_params=params(),
        cost_estimate=cost(5e9, 20e6),
    )(
        sources, y, x, grad_y, inner, write, seg_t, last, spread2, skip, state,
        write_part, read_part, own, other, *waits,
    )


def product_kernel(masks, group, mine, theirs, cot_mine, cot_theirs, *outs):
    first_rows, second_rows = mine[...], theirs[...]
    for mask, out in zip(masks, outs):
        spot = jnp.bitwise_xor(group[0], mask)
        first = mm_t(cot_mine[spot], first_rows).astype(BF16).astype(F32)
        second = mm_t(cot_theirs[spot], second_rows).astype(BF16).astype(F32)
        out[...] = (first + second).astype(out.dtype)


def products(group, mine, theirs, cot_mine, cot_theirs):
    rows, length = mine.shape
    groups, columns, _ = cot_mine.shape
    masks = list(range(groups - 1, -1, -1))
    block = LANES if rows % LANES == 0 else rows
    side = pl.BlockSpec((block, length), lambda i, *_: (i, 0))
    return pl.pallas_call(
        functools.partial(product_kernel, masks),
        name="product",
        grid_spec=pltpu.PrefetchScalarGridSpec(
            num_scalar_prefetch=1,
            grid=(rows // block,),
            in_specs=[side, side, whole(cot_mine.shape), whole(cot_theirs.shape)],
            out_specs=[pl.BlockSpec((columns, block), lambda i, *_: (0, i))] * groups,
        ),
        out_shape=[
            jax.ShapeDtypeStruct((columns, rows), BF16 if mask else F32) for mask in masks
        ],
        compiler_params=params(),
        cost_estimate=cost(4.0 * rows * length * columns * groups, 5e6),
    )(group, mine, theirs, cot_mine, cot_theirs)


def finish_kernel(count, own, *rest):
    total = own[...]
    for k in range(count):
        total = total + rest[k][...].astype(F32)
    rest[-1][...] = total


def finish(part, parts, own, received, held):
    columns, rows = own.shape
    if rows % LANES:
        total = own + sum(piece.astype(F32) for piece in received)
        return total if held is None else jnp.concatenate([held, total], axis=1)
    small = pl.BlockSpec((columns, rows), lambda i: (0, 0))
    operands = [own, *received]
    specs = [small] * len(operands)
    aliases = {}
    if held is not None:
        aliases = {len(operands): 0}
        operands.append(held)
        specs = specs + [WAIT]
    return pl.pallas_call(
        functools.partial(finish_kernel, len(received)),
        name="finish",
        grid=(1,),
        in_specs=specs,
        out_specs=pl.BlockSpec((columns, rows), lambda i: (0, part)),
        out_shape=jax.ShapeDtypeStruct((columns, parts * rows), F32),
        input_output_aliases=aliases,
        compiler_params=params(),
        cost_estimate=cost(1e9, 4e6),
    )(*operands)


def ring_gather(near, far, size):
    half = size // 2
    order = [2 * q for q in range(half)] + [2 * (size - 1 - q) + 1 for q in range(half, size)]
    ahead = [(order[i], order[(i + 1) % size]) for i in range(size)]
    behind = [(b, a) for a, b in ahead]
    shifts, all_near, all_far = [0], [near], [far]
    up = down = [near, far]
    for hop in range(1, half + 1):
        last = hop == half
        up = [lax.ppermute(v, "seq", ahead) for v in (up[:1] if last else up)]
        down = [lax.ppermute(v, "seq", behind) for v in (down[1:] if last else down)]
        shifts.append(-hop)
        all_near.append(up[0])
        if last:
            all_far.append(down[0])
        else:
            all_far.append(up[1])
            shifts.append(hop)
            all_near.append(down[0])
            all_far.append(down[1])
    return all_near, all_far, shifts


def ring_sources(shifts, size):
    position = lax.axis_index("seq")
    half = size // 2
    place = jnp.where(position % 2 == 0, position // 2, size - 1 - position // 2)
    places = (place + jnp.array(shifts, jnp.int32) + size) % size
    found = jnp.where(places < half, 2 * places, 2 * (size - 1 - places) + 1)
    return jnp.concatenate([found, position[None]]).astype(jnp.int32)


def butterfly_sum(value, axis, size, first=1):
    strides = [1 << k for k in range(size.bit_length() - 1)]
    for stride in [v for v in strides if v >= first] + [v for v in strides if v < first]:
        value = value + lax.ppermute(value, axis, [(i, i ^ stride) for i in range(size)])
    return value


def all_shards(value, size):
    held = [value]
    masks = [0]
    stride = size // 2
    while stride >= 1:
        moves = [(i, i ^ stride) for i in range(size)]
        held = held + [lax.ppermute(v, "tp", moves) for v in held]
        masks = masks + [m ^ stride for m in masks]
        stride //= 2
    return held, masks


def send_products(pieces, size):
    groups = size // 2
    by_mask = dict(zip(range(groups - 1, -1, -1), pieces))

    def move(value, moves):
        pairs = [(2 * a + p, 2 * b + p) for a, b in moves for p in (0, 1)]
        return lax.ppermute(value, "seq", pairs)

    if groups != 4:
        return [
            move(by_mask[mask], [(g, g ^ mask) for g in range(groups)])
            for mask in range(1, groups)
        ], []
    far = move(by_mask[3], [(0, 1), (3, 2)])
    near = [move(by_mask[3], [(1, 2), (2, 1)]), move(by_mask[1], [(g, g ^ 1) for g in range(4)])]
    merged = (by_mask[2].astype(F32) + far.astype(F32)).astype(BF16)
    return near + [move(merged, [(g, g ^ 2) for g in range(4)])], [merged]


def on_device(
    packed_input, block_exponent, gate_input, state_write, state_read, log_decay,
    skip_weight, norm_gain, out_weight, out_cotangent,
):
    heads, _ = log_decay.shape
    width = packed_input.shape[1]
    seq_size = lax.axis_size("seq")
    tp_size = lax.axis_size("tp")
    total_width = width * tp_size
    columns = out_weight.shape[1] // seq_size
    parity = lax.axis_index("seq") % 2
    partner = [(i, i ^ 1) for i in range(seq_size)]
    gain = norm_gain[None, :]

    x, near, far, seg_t, seg, spread2, skip, read_t = prepare(
        packed_input, block_exponent, log_decay, skip_weight[None, :], state_write, state_read
    )
    near, far, shifts = ring_gather(near, far, seq_size)
    sources = ring_sources(shifts, seq_size)

    other_half = pick(parity[None].astype(jnp.int32), out_cotangent, columns)
    theirs = lax.ppermute(other_half, "seq", partner)
    all_mine, masks = all_shards(out_cotangent, tp_size)
    all_theirs, _ = all_shards(theirs, tp_size)
    owners = jnp.bitwise_xor(lax.axis_index("tp"), jnp.array(masks, jnp.int32))
    owners = jnp.concatenate([owners, parity[None]]).astype(jnp.int32)

    pairs = width // LANES
    calls = min(2, pairs)
    y_local = None
    hops = seq_size // 2
    for call in range(calls):
        start, stop = call * pairs // calls, (call + 1) * pairs // calls
        waits = (*near[1:3], *far[1:3]) if call == 1 and hops > 2 else ()
        y_local = inside(
            heads, start, stop, seg_t, seg, state_write, state_read, x, skip, y_local, waits
        )
    waits = (y_local, *near[3:5], *far[3:5]) if hops > 2 else (y_local,)
    grad_v, cot_mine = cotangent(owners, out_weight, all_mine, columns, waits)
    cot_theirs = stack(owners, all_theirs, columns)

    y, scaled_t, stats, state, totals = enter(
        sources, y_local, gate_input, grad_v, gain, state_read, seg_t, spread2, near, far
    )
    stats = butterfly_sum(stats, "tp", tp_size)
    scale = lax.rsqrt(stats[0:1, :] / total_width + EPSILON)
    part_rows = width // NORMED_PARTS
    normed, normed_theirs = [], []
    for part in range(NORMED_PARTS):
        rows = scaled_t[part * part_rows : (part + 1) * part_rows]
        normed.append((rows * scale).astype(BF16))
        normed_theirs.append(lax.ppermute(normed[part], "seq", partner))

    grad_gate, grad_y, send, keep, sums = gate_grads(
        total_width, sources, y, gate_input, grad_v, gain, stats, x, seg_t, spread2, read_t
    )
    received, later = pair_state(totals, sources, send, keep, seq_size)
    middle = pairs // 2
    operands = (seg_t, seg, state_write, state_read, x, grad_y)
    inner, grad_cross = inside_back(heads, 0, middle, *operands)
    inner, write_part, read_part = inside_back(heads, middle, pairs, *operands, inner, grad_cross)
    group = (lax.axis_index("seq") // 2)[None].astype(jnp.int32)
    arrived, own_part, merges = [], [], []
    for part in range(NORMED_PARTS):
        *pieces, last = products(group, normed[part], normed_theirs[part], cot_mine, cot_theirs)
        got, merged = send_products(pieces, seq_size)
        arrived.append(got)
        own_part.append(last)
        merges.append(merged)
    own, other = join_states(
        totals, sources, keep, received, later, seq_size, (write_part, *merges[0])
    )
    grad_input, maps, grad_decay = leave(
        heads, sources, y, x, grad_y, inner, state_write, seg_t, spread2, skip, state,
        write_part, read_part, own, other, (),
    )
    grad_out_weight = None
    for part in range(NORMED_PARTS):
        grad_out_weight = finish(part, NORMED_PARTS, own_part[part], arrived[part], grad_out_weight)
    maps = butterfly_sum(maps, "tp", tp_size)
    sums = butterfly_sum(sums, "seq", seq_size, 2)
    grad_skip = jnp.sum(sums[1].reshape(heads, width // heads), axis=1)
    return (
        grad_input, grad_gate, maps[0], maps[1], grad_decay, grad_skip, sums[0], grad_out_weight.T,
    )


def solution(mesh):
    placed = (
        P("seq", "tp"), P("tp", "seq"), P("seq", "tp"), P("seq", None), P("seq", None),
        P("tp", "seq"), P("tp"), P("tp"), P("tp", None), P("seq", "tp"),
    )
    return jax.shard_map(
        on_device,
        mesh=mesh,
        in_specs=placed,
        out_specs=(
            P("seq", "tp"), P("seq", "tp"), P("seq", None), P("seq", None), P("tp", "seq"),
            P("tp"), P("tp"), P("tp", "seq"),
        ),
        check_vma=False,
    )
```

```python
import functools
import jax
import jax.numpy as jnp
from jax import lax
from jax.experimental import pallas as pl
from jax.experimental.pallas import tpu as pltpu
from jax.sharding import PartitionSpec as P

F32 = jnp.float32
BF16 = jnp.bfloat16
LANES = 128
EXTRA = 16
EPSILON = 1e-05
HALF = LANES // 2


def mm(a, b):
    return jnp.dot(a, b, preferred_element_type=F32)


def mm_t(a, b):
    return lax.dot_general(a, b, (((1,), (1,)), ((), ())), preferred_element_type=F32)


def split2(v):
    high = v.astype(BF16)
    return high, (v - high.astype(F32)).astype(BF16)


def split3(v):
    high = v.astype(BF16)
    rest = v - high.astype(F32)
    middle = rest.astype(BF16)
    return high, middle, (rest - middle.astype(F32)).astype(BF16)


def iota(shape, axis):
    return lax.broadcasted_iota(jnp.int32, shape, axis)


def spread(values, spread2):
    return mm(jnp.concatenate(split2(values), axis=1), spread2)


FULL_GRANT = 67_043_328


def params(limit=24 << 20):
    return pltpu.CompilerParams(vmem_limit_bytes=limit)


def cost(flops, nbytes, special=0):
    return pl.CostEstimate(flops=int(flops), bytes_accessed=int(nbytes), transcendentals=int(special))


def skipping(kernel, first, extra):
    return lambda *refs: kernel(*refs[:first], *refs[first + extra :])


WAIT = pl.BlockSpec(memory_space=pl.ANY)


def prepare_kernel(
    heads, packed, expo, decay, skip, write, read,
    x_out, near_out, far_out, seg_t_out, seg_out, spread_out, skip_out, read_t_out, pad, pad8,
):
    length, width = x_out.shape
    head_width = width // heads
    rows8 = packed.shape[0]
    groups = expo.shape[0]
    pad[...] = jnp.zeros_like(pad)
    pad[0:heads, :] = decay[...]
    decay_t = pad[...].T
    lower = (iota((length, length), 0) >= iota((length, length), 1)).astype(BF16)
    seg_t = sum(mm(lower, part) for part in split3(decay_t))
    seg_t_out[...] = seg_t
    seg_out[...] = seg_t.T
    of_head = (iota((LANES, width), 1) // head_width == iota((LANES, width), 0)).astype(BF16)
    spread2 = jnp.concatenate([of_head, of_head], axis=0)
    spread_out[...] = spread2
    pad8[...] = jnp.zeros_like(pad8)
    pad8[0:1, 0:heads] = skip[...]
    skip_out[...] = sum(mm(part, of_head) for part in split3(pad8[...]))
    total = seg_t[length - 1 : length, :]
    to_end = spread(jnp.exp(total - seg_t), spread2)
    pad[...] = jnp.zeros_like(pad)
    pad[0:groups, :] = jnp.left_shift(1, expo[...] + 8).astype(F32) * (2.0**-8)
    of_group = (
        iota((LANES, width), 1) // (width // groups) == iota((LANES, width), 0)
    ).astype(BF16)
    factors = mm(pad[...].T.astype(BF16), of_group)
    words = jnp.broadcast_to(packed[...][:, None, :], (rows8, 8, width))
    words = jnp.right_shift(words, 4 * iota((rows8, 8, width), 1))
    fields = (jnp.bitwise_and(words, 15) - 8).astype(F32).reshape(length, width)
    x = fields * factors
    x_out[...] = x.astype(BF16)
    states = mm(write[...].T, (x * to_end).astype(BF16)).astype(BF16)
    read_t_out[...] = read[...].T
    near_out[0:HALF, :] = states[0:HALF, :]
    far_out[...] = states[HALF:, :]
    total8 = jnp.broadcast_to(total, (8, LANES))
    high, middle, low = (mm(part, of_head) for part in split3(total8))
    row = iota((EXTRA, width), 0)
    tail = jnp.where(row == 0, high[0:1, :], jnp.where(row == 1, middle[0:1, :], low[0:1, :]))
    near_out[HALF:, :] = jnp.where(row < 3, tail, 0.0).astype(BF16)


def prepare(packed, expo, decay, skip, write, read):
    heads, length = decay.shape
    width = packed.shape[1]
    shapes = (
        jax.ShapeDtypeStruct((length, width), BF16),
        jax.ShapeDtypeStruct((HALF + EXTRA, width), BF16),
        jax.ShapeDtypeStruct((HALF, width), BF16),
        jax.ShapeDtypeStruct((length, LANES), F32),
        jax.ShapeDtypeStruct((LANES, length), F32),
        jax.ShapeDtypeStruct((2 * LANES, width), BF16),
        jax.ShapeDtypeStruct((8, width), F32),
        jax.ShapeDtypeStruct((LANES, length), BF16),
    )
    return pl.pallas_call(
        functools.partial(prepare_kernel, heads),
        name="prepare",
        out_shape=shapes,
        scratch_shapes=[pltpu.VMEM((LANES, length), F32), pltpu.VMEM((8, LANES), F32)],
        compiler_params=params(FULL_GRANT),
        cost_estimate=cost(3e9, 8e6),
    )(packed, expo, decay, skip, write, read)


def pick_kernel(per_half, columns, parity, shard, out):
    odd_wanted = parity[0] == 0
    for sub in range(per_half):
        even_part = shard[:, 2 * sub * columns : (2 * sub + 1) * columns]
        odd_part = shard[:, (2 * sub + 1) * columns : (2 * sub + 2) * columns]
        out[sub * columns : (sub + 1) * columns, :] = jnp.where(odd_wanted, odd_part, even_part).T


def pick(parity, shard, columns):
    length, shard_width = shard.shape
    out = (shard_width // 2, length)
    return pl.pallas_call(
        functools.partial(pick_kernel, shard_width // (2 * columns), columns),
        name="pick",
        grid_spec=pltpu.PrefetchScalarGridSpec(
            num_scalar_prefetch=1, grid=(1,), in_specs=[whole(shard.shape)], out_specs=whole(out)
        ),
        out_shape=jax.ShapeDtypeStruct(out, BF16),
        compiler_params=params(),
        cost_estimate=cost(1e8, 2e6),
    )(parity, shard)


def cotangent_kernel(shards, per_half, owners, weight, *rest):
    mine = rest[:shards]
    grad_v, cot_mine, full = rest[shards:]
    shard_width = mine[0].shape[1]
    columns = cot_mine.shape[1]

    @pl.when(pl.program_id(0) == 0)
    def _():
        odd = owners[shards] == 1
        for m in range(shards):
            for q in range(shards):
                @pl.when(owners[m] == q)
                def _():
                    full[:, q * shard_width : (q + 1) * shard_width] = mine[m][...]
            for sub in range(per_half):
                even_part = mine[m][:, 2 * sub * columns : (2 * sub + 1) * columns]
                odd_part = mine[m][:, (2 * sub + 1) * columns : (2 * sub + 2) * columns]
                cot_mine[owners[m] * per_half + sub] = jnp.where(odd, odd_part, even_part).T

    grad_v[...] = mm_t(full[...], weight[...])


def cotangent(owners, weight, mine, columns, waits):
    shards = len(mine)
    length, shard_width = mine[0].shape
    width, model_width = weight.shape
    per_half = shard_width // (2 * columns)
    block = 2 * LANES if width % (2 * LANES) == 0 else LANES
    stacked = (shards * per_half, columns, length)
    return pl.pallas_call(
        skipping(functools.partial(cotangent_kernel, shards, per_half), 2 + shards, len(waits)),
        name="cotangent",
        grid_spec=pltpu.PrefetchScalarGridSpec(
            num_scalar_prefetch=1,
            grid=(width // block,),
            in_specs=[pl.BlockSpec((block, model_width), lambda i, *_: (i, 0))]
            + [whole(mine[0].shape)] * shards
            + [WAIT] * len(waits),
            out_specs=[pl.BlockSpec((length, block), lambda i, *_: (0, i)), whole(stacked)],
            scratch_shapes=[pltpu.VMEM((length, model_width), BF16)],
        ),
        out_shape=(
            jax.ShapeDtypeStruct((length, width), F32),
            jax.ShapeDtypeStruct(stacked, BF16),
        ),
        compiler_params=params(),
        cost_estimate=cost(2.0 * length * width * model_width, 20e6),
    )(owners, weight, *mine, *waits)


def stack_kernel(shards, owners, *rest):
    theirs, out = rest[:shards], rest[shards]
    columns = out.shape[1]
    per_half = theirs[0].shape[0] // columns
    for m in range(shards):
        for sub in range(per_half):
            rows = slice(sub * columns, (sub + 1) * columns)
            out[owners[m] * per_half + sub] = theirs[m][rows, :]


def stack(owners, theirs, columns):
    rows, length = theirs[0].shape
    out = (len(theirs) * rows // columns, columns, length)
    return pl.pallas_call(
        functools.partial(stack_kernel, len(theirs)),
        name="stack",
        grid_spec=pltpu.PrefetchScalarGridSpec(
            num_scalar_prefetch=1,
            grid=(1,),
            in_specs=[whole(theirs[0].shape)] * len(theirs),
            out_specs=whole(out),
        ),
        out_shape=jax.ShapeDtypeStruct(out, BF16),
        compiler_params=params(),
        cost_estimate=cost(1e8, 3e6),
    )(owners, *theirs)


def pair_columns(seg_t, seg, step):
    rolled = pltpu.roll(seg_t[...], lax.rem(LANES - 2 * step, LANES), 1)
    for side in (0, 1):
        yield side, rolled[:, side : side + 1], seg[pl.ds(2 * step + side, 1), :]


def inside_kernel(head_width, start, seg_t, seg, write, read, x, skip, *rest):
    out, cross = rest[-2:]
    step = pl.program_id(0) + start
    length = x.shape[0]
    half = length // 2

    @pl.when(pl.program_id(0) == 0)
    def _():
        cross[...] = mm_t(read[...], write[...])

    diagonal = iota((half, half), 0) >= iota((half, half), 1)
    parts = []
    for side, column, row in pair_columns(seg_t, seg, step):
        rows = []
        for block in (0, 1):
            low = block * half
            square = slice(low, low + half)
            gap = column[square] - row[:, square]
            decayed = jnp.where(diagonal, jnp.exp(jnp.minimum(gap, 0.0)), 0.0)
            mixing = decayed * cross[square, square]
            if block == 1:
                left = jnp.exp(column[square] - row[:, 0:half]) * cross[square, 0:half]
                mixing = jnp.concatenate([left, mixing], axis=1)
            high, rest = split2(mixing)
            values = x[0 : low + half, :]
            rows.append(mm(high, values) + mm(rest, values))
        parts.append(jnp.concatenate(rows, axis=0))
    first = iota((length, LANES), 1) < head_width
    out[...] = jnp.where(first, parts[0], parts[1]) + skip[0:1, :] * x[...].astype(F32)


def whole(shape):
    return pl.BlockSpec(shape, lambda *_: (0,) * len(shape))


def inside(heads, start, stop, seg_t, seg, write, read, x, skip, held=None, waits=()):
    length, width = x.shape
    column = pl.BlockSpec((length, LANES), lambda j: (0, j + start))
    share = (stop - start) / (width // LANES)
    operands = (seg_t, seg, write, read, x, skip)
    if held is None:
        operands = tuple(pltpu.with_memory_space_constraint(v, pltpu.HBM) for v in operands)
    specs = [
        whole((length, LANES)), whole((LANES, length)), whole(write.shape), whole(read.shape),
        column, pl.BlockSpec((8, LANES), lambda j: (0, j + start)),
    ]
    aliases = {}
    if held is not None:
        aliases = {len(operands): 0}
        operands = operands + (held,)
        specs = specs + [WAIT]
    operands = operands + tuple(waits)
    specs = specs + [WAIT] * len(waits)
    return pl.pallas_call(
        functools.partial(inside_kernel, width // heads, start),
        name="inside",
        grid=(stop - start,),
        in_specs=specs,
        out_specs=column,
        out_shape=jax.ShapeDtypeStruct((length, width), F32),
        scratch_shapes=[pltpu.VMEM((length, length), F32)],
        input_output_aliases=aliases,
        compiler_params=params(),
        cost_estimate=cost(20e9 * share, 5e6 * share),
    )(*operands)


def gathered_total(pays, k):
    tail = pays[k][HALF : HALF + 8, :].astype(F32)
    return tail[0:1, :] + tail[1:2, :] + tail[2:3, :]


def boundary(totals, near, far, sources, position, count):
    width = totals.shape[1]
    column = jnp.zeros((count, 1), jnp.int32)
    for k in range(count):
        column = jnp.where(iota((count, 1), 0) == k, sources[k], column)
    powers = jnp.zeros((count, width), F32)
    for j in range(count):
        between = jnp.logical_and(column < sources[j], sources[j] < position)
        powers = powers + jnp.where(between, totals[j : j + 1, :], 0.0)
    weights = jnp.where(column < position, jnp.exp(powers), 0.0)
    upper = jnp.zeros((HALF, width), F32)
    lower = jnp.zeros((HALF, width), F32)
    for k in range(count):
        upper = upper + weights[k : k + 1, :] * near[k][0:HALF, :].astype(F32)
        lower = lower + weights[k : k + 1, :] * far[k][...].astype(F32)
    return upper, lower


def enter_kernel(
    count, sources, y_local, gate, grad_v, gain, read, seg_t, spread2, *rest,
):
    near, far = rest[:count], rest[count : 2 * count]
    y_out, scaled_t_out, stats_out, state_out, totals_out, state2 = rest[2 * count :]

    @pl.when(pl.program_id(0) == 0)
    def _():
        for k in range(count):
            totals_out[k : k + 1, :] = gathered_total(near, k)
        upper, lower = boundary(totals_out[...], near, far, sources, sources[count], count)
        state_out[0:HALF, :] = upper
        state_out[HALF:, :] = lower
        state2[0:LANES, :], state2[LANES:, :] = split2(state_out[...])

    from_start = spread(jnp.exp(seg_t[...]), spread2[...])
    read_part = read[...]
    carried = mm(jnp.concatenate([read_part, read_part], axis=1), state2[...])
    y = y_local[...] + from_start * carried
    y_out[...] = y
    z = gate[...].astype(F32)
    mixed = y * z / (1.0 + jnp.exp(-z))
    with_gain = mixed * gain[...]
    scaled_t_out[...] = with_gain.T
    squares = jnp.sum(mixed * mixed, axis=1, keepdims=True)
    inner = jnp.sum(grad_v[...] * with_gain, axis=1, keepdims=True)
    lane = iota((squares.shape[0], LANES), 1)
    stats = jnp.where(lane == 0, squares, jnp.where(lane == 1, inner, 0.0))
    stats_out[...] = stats.T[0:8, :]


def enter(sources, y_local, gate, grad_v, gain, read, seg_t, spread2, near, far):
    length, width = y_local.shape
    count = len(near)
    block = LANES
    token = pl.BlockSpec((block, width), lambda i, *_: (i, 0))
    narrow = pl.BlockSpec((block, LANES), lambda i, *_: (i, 0))
    shapes = (
        jax.ShapeDtypeStruct((length, width), F32),
        jax.ShapeDtypeStruct((width, length), F32),
        jax.ShapeDtypeStruct((8, length), F32),
        jax.ShapeDtypeStruct((LANES, width), F32),
        jax.ShapeDtypeStruct((count, width), F32),
    )
    return pl.pallas_call(
        functools.partial(enter_kernel, count),
        name="enter",
        grid_spec=pltpu.PrefetchScalarGridSpec(
            num_scalar_prefetch=1,
            grid=(length // block,),
            in_specs=[
                token, token, token, whole((1, width)), narrow, narrow, whole(spread2.shape),
            ] + [whole(near[0].shape)] * count + [whole(far[0].shape)] * count,
            out_specs=[
                token,
                pl.BlockSpec((width, block), lambda i, *_: (0, i)),
                pl.BlockSpec((8, block), lambda i, *_: (0, i)),
                whole((LANES, width)),
                whole((count, width)),
            ],
            scratch_shapes=[pltpu.VMEM((2 * LANES, width), BF16)],
        ),
        out_shape=shapes,
        compiler_params=params(),
        cost_estimate=cost(3e9, 15e6),
    )(sources, y_local, gate, grad_v, gain, read, seg_t, spread2, *near, *far)


def gate_kernel(
    total_width, sources, y_ref, gate, grad_v, gain, stats, x, seg_t, spread2, read_t,
    gate_out, grad_y_out, send_out, keep_out, sums, columns, cot,
):
    step = pl.program_id(0)
    row = iota((LANES, LANES), 0)
    squares, inner = stats[0:1, :], stats[1:2, :]
    scale_row = lax.rsqrt(squares * (1.0 / total_width) + EPSILON)
    back_row = scale_row * scale_row * scale_row * inner * (1.0 / total_width)
    columns[...] = jnp.where(row == 0, scale_row, jnp.where(row == 1, back_row, 0.0)).T
    scale, back = columns[:, 0:1], columns[:, 1:2]
    y = y_ref[...]
    z = gate[...].astype(F32)
    sigma = 1.0 / (1.0 + jnp.exp(-z))
    active = z * sigma
    mixed = y * active
    scaled_v = scale * grad_v[...]
    grad_mixed = scaled_v * gain[...] - mixed * back
    gate_out[...] = (grad_mixed * y * sigma * (1.0 + z * (1.0 - sigma))).astype(BF16)
    grad_y = grad_mixed * active
    grad_y_out[...] = grad_y
    gain_part = jnp.sum(scaled_v * mixed, axis=0, keepdims=True)
    skip_part = jnp.sum(grad_y * x[...].astype(F32), axis=0, keepdims=True)
    from_start = spread(jnp.exp(seg_t[...]), spread2[...])
    cot_part = mm(read_t[...], (grad_y * from_start).astype(BF16))
    wide = iota((8, grad_y.shape[1]), 0)
    sum_part = jnp.where(wide == 0, gain_part, jnp.where(wide == 1, skip_part, 0.0))

    @pl.when(step == 0)
    def _():
        cot[...] = cot_part
        sums[...] = sum_part

    @pl.when(step > 0)
    def _():
        cot[...] += cot_part
        sums[...] += sum_part

    @pl.when(step == pl.num_programs(0) - 1)
    def _():
        parity = lax.rem(sources[sources.shape[0] - 1], 2)
        keep_out[...] = cot[pl.ds(pl.multiple_of(parity * HALF, HALF), HALF), :]
        send_out[...] = cot[pl.ds(pl.multiple_of((1 - parity) * HALF, HALF), HALF), :].astype(BF16)


def gate_grads(total_width, sources, y, gate, grad_v, gain, stats, x, seg_t, spread2, read_t):
    length, width = y.shape
    block = LANES
    token = pl.BlockSpec((block, width), lambda i, *_: (i, 0))
    narrow = pl.BlockSpec((block, LANES), lambda i, *_: (i, 0))
    shapes = (
        jax.ShapeDtypeStruct((length, width), BF16),
        jax.ShapeDtypeStruct((length, width), F32),
        jax.ShapeDtypeStruct((HALF, width), BF16),
        jax.ShapeDtypeStruct((HALF, width), F32),
        jax.ShapeDtypeStruct((8, width), F32),
    )
    return pl.pallas_call(
        functools.partial(gate_kernel, total_width),
        name="gate_grads",
        grid_spec=pltpu.PrefetchScalarGridSpec(
            num_scalar_prefetch=1,
            grid=(length // block,),
            in_specs=[
                token, token, token, whole((1, width)), pl.BlockSpec((8, block), lambda i, *_: (0, i)),
                token, narrow, whole(spread2.shape), pl.BlockSpec((LANES, block), lambda i, *_: (0, i)),
            ],
            out_specs=[
                token, token, whole((HALF, width)), whole((HALF, width)), whole((8, width)),
            ],
            scratch_shapes=[pltpu.VMEM((LANES, LANES), F32), pltpu.VMEM((LANES, width), F32)],
        ),
        out_shape=shapes,
        compiler_params=params(),
        cost_estimate=cost(3e9, 15e6),
    )(sources, y, gate, grad_v, gain, stats, x, seg_t, spread2, read_t)


def inside_back_kernel(
    head_width, start, last, seg_t, seg, write, read, x, grad_y, *rest,
):
    step = pl.program_id(0) + start
    if last:
        before, out, grad_write, grad_read, cross, grad_cross = rest[-6:]
    else:
        out, sum_out, cross, grad_cross = rest[-4:]
    length = x.shape[0]
    half = length // 2

    @pl.when(pl.program_id(0) == 0)
    def _():
        cross[...] = mm_t(write[...], read[...])
        grad_cross[...] = before[...] if last else jnp.zeros_like(grad_cross)

    diagonal = iota((half, half), 0) <= iota((half, half), 1)
    first = iota((length, LANES), 1) < head_width
    grads = grad_y[...].astype(BF16)
    values = x[...]
    parts = []
    for side, column, row in pair_columns(seg_t, seg, step):
        mine = first if side == 0 else jnp.logical_not(first)
        own = jnp.where(mine, values, jnp.zeros_like(values))
        rows = []
        for block in (0, 1):
            low = block * half
            square = slice(low, low + half)
            gap = row[:, square] - column[square]
            decayed = jnp.where(diagonal, jnp.exp(jnp.minimum(gap, 0.0)), 0.0)
            mixing = decayed * cross[square, square]
            grad_cross[square, square] += mm_t(own[square], grads[square]) * decayed
            if block == 0:
                decayed = jnp.exp(row[:, half:] - column[square])
                mixing = jnp.concatenate([mixing, decayed * cross[square, half:]], axis=1)
                grad_cross[square, half:] += mm_t(own[square], grads[half:]) * decayed
            rows.append(mm(mixing.astype(BF16), grads[low:]))
        parts.append(jnp.concatenate(rows, axis=0))
    out[...] = jnp.where(first, parts[0], parts[1])

    @pl.when(pl.program_id(0) == pl.num_programs(0) - 1)
    def _():
        if last:
            high, low = split2(grad_cross[...])
            grad_write[...] = mm(high, read[...]) + mm(low, read[...])
            turned = grad_cross[...].T
            high, low = split2(turned)
            grad_read[...] = mm(high, write[...]) + mm(low, write[...])
        else:
            sum_out[...] = grad_cross[...]


def inside_back(heads, start, stop, seg_t, seg, write, read, x, grad_y, held=None, before=None):
    length, width = x.shape
    last = held is not None
    column = pl.BlockSpec((length, LANES), lambda j: (0, j + start))
    square = (length, length)
    small = (length, LANES)
    operands = (seg_t, seg, write, read, x, grad_y)
    specs = [
        whole((length, LANES)), whole((LANES, length)), whole(write.shape), whole(read.shape),
        column, column,
    ]
    share = (stop - start) / (width // LANES)
    outs = (jax.ShapeDtypeStruct((length, width), F32),)
    aliases = {}
    if last:
        operands = operands + (held, before)
        specs = specs + [WAIT, whole(square)]
        aliases = {6: 0}
        outs = outs + (jax.ShapeDtypeStruct(small, F32), jax.ShapeDtypeStruct(small, F32))
        out_specs = [column, whole(small), whole(small)]
    else:
        outs = outs + (jax.ShapeDtypeStruct(square, F32),)
        out_specs = [column, whole(square)]
    return pl.pallas_call(
        functools.partial(inside_back_kernel, width // heads, start, last),
        name="inside_back",
        grid=(stop - start,),
        in_specs=specs,
        out_specs=out_specs,
        out_shape=outs,
        scratch_shapes=[pltpu.VMEM(square, F32), pltpu.VMEM(square, F32)],
        input_output_aliases=aliases,
        compiler_params=params(),
        cost_estimate=cost(20e9 * share, 8e6 * share),
    )(*operands)


def total_of(totals, sources, count, wanted):
    found = jnp.zeros_like(totals[0:1, :])
    for k in range(count):
        found = found + jnp.where(sources[k] == wanted, totals[k : k + 1, :], 0.0)
    return found


def pair_kernel(count, sources, totals, keep, received, out):
    position = sources[count]
    odd = lax.rem(position, 2) == 1
    weight = jnp.exp(total_of(totals, sources, count, position - lax.rem(position, 2)))
    own, other = keep[...], received[...].astype(F32)
    out[...] = jnp.where(odd, other + weight * own, own + weight * other).astype(BF16)


def join_kernel(count, sources, totals, keep, received, *rest):
    shifts = count // 2 - 1
    later, (own_out, send_out) = rest[:shifts], rest[shifts:]
    position = sources[count]
    even_place = position - lax.rem(position, 2)
    odd = lax.rem(position, 2) == 1
    state = jnp.zeros_like(keep)
    power = jnp.zeros_like(totals[0:1, :])
    for shift in range(1, shifts + 1):
        state = state + jnp.exp(power) * later[shift - 1][...].astype(F32)
        if shift < shifts:
            power = power + total_of(totals, sources, count, even_place + 2 * shift)
            power = power + total_of(totals, sources, count, even_place + 2 * shift + 1)
    weight = jnp.exp(total_of(totals, sources, count, even_place + 1))
    of_odd = jnp.where(odd, keep[...], received[...].astype(F32))
    for_even = of_odd + weight * state
    own_out[...] = jnp.where(odd, state, for_even)
    send_out[...] = jnp.where(odd, for_even, state).astype(BF16)


def small_call(kernel, count, outs, sources, *arrays, waits=()):
    return pl.pallas_call(
        skipping(functools.partial(kernel, count), 1 + len(arrays), len(waits)),
        grid_spec=pltpu.PrefetchScalarGridSpec(
            num_scalar_prefetch=1,
            grid=(1,),
            in_specs=[whole(a.shape) for a in arrays] + [WAIT] * len(waits),
            out_specs=[whole(o.shape) for o in outs],
        ),
        out_shape=outs,
        compiler_params=params(),
        cost_estimate=cost(1e9, 2e6),
    )(sources, *arrays, *waits)


def pair_state(totals, sources, send, keep, size):
    partner = [(i, i ^ 1) for i in range(size)]
    received = lax.ppermute(send, "seq", partner)
    narrow = jax.ShapeDtypeStruct(send.shape, BF16)
    (pair,) = small_call(pair_kernel, size, (narrow,), sources, totals, keep, received)
    later = []
    for shift in range(1, size // 2):
        moves = [(i, i - 2 * shift) for i in range(2 * shift, size)]
        later.append(lax.ppermute(pair, "seq", moves))
    return received, later


def join_states(totals, sources, keep, received, later, size, waits):
    narrow = jax.ShapeDtypeStruct(keep.shape, BF16)
    wide = jax.ShapeDtypeStruct(keep.shape, F32)
    own, other = small_call(
        join_kernel, size, (wide, narrow), sources, totals, keep, received, *later,
        waits=waits,
    )
    return own, lax.ppermute(other, "seq", [(i, i ^ 1) for i in range(size)])


def leave_kernel(
    count, heads, sources, y_ref, x_ref, grad_y_ref, inner_ref, write, seg_t, last, spread2,
    skip, state, write_part, read_part, own, other,
    input_out, maps_out, decay_out, cot2, state16, from_head, per_head, sums, cot,
):
    step = pl.program_id(0)
    steps = pl.num_programs(0)
    block, width = y_ref.shape
    length = per_head.shape[0]

    @pl.when(step == 0)
    def _():
        parity = lax.rem(sources[count], 2)
        cot[pl.ds(pl.multiple_of(parity * HALF, HALF), HALF), :] = own[...]
        cot[pl.ds(pl.multiple_of((1 - parity) * HALF, HALF), HALF), :] = other[...].astype(F32)
        cot2[0:LANES, :], cot2[LANES:, :] = split2(cot[...])
        state16[...] = state[...].astype(BF16)
        from_head[...] = spread2[0:LANES, :].T
        ended = spread(jnp.exp(last[...]), spread2[...])
        through = jnp.sum(cot[...] * state[...], axis=0, keepdims=True) * ended[0:1, :]
        sums[...] = jnp.where(iota((8, width), 0) == 0, through, 0.0)

    seg_part = seg_t[...]
    decays = jnp.exp(seg_part)
    to_end = spread(jnp.exp(last[0:1, :] - seg_part), spread2[...])
    from_start = spread(decays, spread2[...])
    x = x_ref[...].astype(F32)
    grad_y = grad_y_ref[...]
    write_rows = write[...]
    from_later = to_end * mm(jnp.concatenate([write_rows, write_rows], axis=1), cot2[...])
    core_grad = inner_ref[...] + from_later
    skip_row = skip[0:1, :]
    input_out[...] = (skip_row * grad_y + core_grad).astype(BF16)
    leaving = jnp.sum(x * from_later, axis=0, keepdims=True)
    sums[...] += jnp.where(iota((8, width), 0) == 0, leaving, 0.0)
    terms = grad_y * (y_ref[...] - skip_row * x) - x * core_grad
    high, low = split2(terms)
    start = pl.multiple_of(step * block, block)
    per_head[pl.ds(start, block), :] = mm(high, from_head[...]) + mm(low, from_head[...])
    maps_out[0] = write_part[...] + mm_t((x * to_end).astype(BF16), cot2[0:LANES, :])
    maps_out[1] = read_part[...] + mm_t((grad_y * from_start).astype(BF16), state16[...])

    @pl.when(step == steps - 1)
    def _():
        final = sum(mm(part, from_head[...]) for part in split3(sums[...]))
        upper = (iota((length, length), 0) <= iota((length, length), 1)).astype(BF16)
        tail = sum(mm(upper, part) for part in split3(per_head[...]))
        decay_out[...] = (tail + final[0:1, :]).T[0:heads, :]


def leave(
    heads, sources, y, x, grad_y, inner, write, seg_t, spread2, skip, state,
    write_part, read_part, own, other, waits,
):
    length, width = y.shape
    count = sources.shape[0] - 1
    block = LANES
    token = pl.BlockSpec((block, width), lambda i, *_: (i, 0))
    narrow = pl.BlockSpec((block, LANES), lambda i, *_: (i, 0))
    shapes = (
        jax.ShapeDtypeStruct((length, width), BF16),
        jax.ShapeDtypeStruct((2, length, LANES), F32),
        jax.ShapeDtypeStruct((heads, length), F32),
    )
    last = jnp.broadcast_to(seg_t[length - 1 :, :], (8, LANES))
    return pl.pallas_call(
        skipping(functools.partial(leave_kernel, count, heads), 15, len(waits)),
        name="leave",
        grid_spec=pltpu.PrefetchScalarGridSpec(
            num_scalar_prefetch=1,
            grid=(length // block,),
            in_specs=[
                token, token, token, token, narrow, narrow, whole((8, LANES)),
                whole(spread2.shape), whole((8, width)), whole((LANES, width)),
                narrow, narrow, whole(own.shape), whole(other.shape),
            ] + [WAIT] * len(waits),
            out_specs=[
                token,
                pl.BlockSpec((2, block, LANES), lambda i, *_: (0, i, 0)),
                whole((heads, length)),
            ],
            scratch_shapes=[
                pltpu.VMEM((2 * LANES, width), BF16),
                pltpu.VMEM((LANES, width), BF16),
                pltpu.VMEM((width, LANES), BF16),
                pltpu.VMEM((length, LANES), F32),
                pltpu.VMEM((8, width), F32),
                pltpu.VMEM((LANES, width), F32),
            ],
        ),
        out_shape=shapes,
        compiler_params=params(),
        cost_estimate=cost(5e9, 20e6),
    )(
        sources, y, x, grad_y, inner, write, seg_t, last, spread2, skip, state,
        write_part, read_part, own, other, *waits,
    )


def product_kernel(masks, group, mine, theirs, cot_mine, cot_theirs, *outs):
    first_rows, second_rows = mine[...], theirs[...]
    for mask, out in zip(masks, outs):
        spot = jnp.bitwise_xor(group[0], mask)
        first = mm_t(cot_mine[spot], first_rows).astype(BF16).astype(F32)
        second = mm_t(cot_theirs[spot], second_rows).astype(BF16).astype(F32)
        out[...] = (first + second).astype(out.dtype)


def products(group, mine, theirs, cot_mine, cot_theirs):
    rows, length = mine.shape
    groups, columns, _ = cot_mine.shape
    masks = list(range(groups - 1, -1, -1))
    block = 2 * LANES if rows % (2 * LANES) == 0 else LANES
    side = pl.BlockSpec((block, length), lambda i, *_: (i, 0))
    return pl.pallas_call(
        functools.partial(product_kernel, masks),
        name="product",
        grid_spec=pltpu.PrefetchScalarGridSpec(
            num_scalar_prefetch=1,
            grid=(rows // block,),
            in_specs=[side, side, whole(cot_mine.shape), whole(cot_theirs.shape)],
            out_specs=[pl.BlockSpec((columns, block), lambda i, *_: (0, i))] * groups,
        ),
        out_shape=[
            jax.ShapeDtypeStruct((columns, rows), BF16 if mask else F32) for mask in masks
        ],
        compiler_params=params(),
        cost_estimate=cost(4.0 * rows * length * columns * groups, 5e6),
    )(group, mine, theirs, cot_mine, cot_theirs)


def finish_kernel(count, own, *rest):
    total = own[...]
    for k in range(count):
        total = total + rest[k][...].astype(F32)
    rest[-1][...] = total


def finish(start, width, own, received, held):
    columns, rows = own.shape
    block = 2 * LANES if rows % (2 * LANES) == 0 and start % (2 * LANES) == 0 else LANES
    small = pl.BlockSpec((columns, block), lambda i: (0, i))
    operands = [own, *received]
    specs = [small] * len(operands)
    aliases = {}
    if held is not None:
        aliases = {len(operands): 0}
        operands.append(held)
        specs = specs + [WAIT]
    return pl.pallas_call(
        functools.partial(finish_kernel, len(received)),
        name="finish",
        grid=(rows // block,),
        in_specs=specs,
        out_specs=pl.BlockSpec((columns, block), lambda i: (0, start // block + i)),
        out_shape=jax.ShapeDtypeStruct((columns, width), F32),
        input_output_aliases=aliases,
        compiler_params=params(),
        cost_estimate=cost(1e9, 4e6),
    )(*operands)


def ring_gather(near, far, size):
    half = size // 2
    order = [2 * q for q in range(half)] + [2 * (size - 1 - q) + 1 for q in range(half, size)]
    ahead = [(order[i], order[(i + 1) % size]) for i in range(size)]
    behind = [(b, a) for a, b in ahead]
    shifts, all_near, all_far = [0], [near], [far]
    up = down = [near, far]
    for hop in range(1, half + 1):
        last = hop == half

        def move(value, moves):
            return lax.ppermute(value, "seq", moves)

        up = [move(up[0], ahead)] + ([] if last else [move(up[1], ahead)])
        down = ([] if last else [move(down[0], behind)]) + [move(down[1], behind)]
        if last:
            down = [None] + down[-1:]
        shifts.append(-hop)
        all_near.append(up[0])
        if last:
            all_far.append(down[1])
        else:
            all_far.append(up[1])
            shifts.append(hop)
            all_near.append(down[0])
            all_far.append(down[1])
    return all_near, all_far, shifts


def ring_sources(shifts, size):
    position = lax.axis_index("seq")
    half = size // 2
    place = jnp.where(position % 2 == 0, position // 2, size - 1 - position // 2)
    places = (place + jnp.array(shifts, jnp.int32) + size) % size
    found = jnp.where(places < half, 2 * places, 2 * (size - 1 - places) + 1)
    return jnp.concatenate([found, position[None]]).astype(jnp.int32)


def butterfly_sum(value, axis, size, first=1):
    strides = [1 << k for k in range(size.bit_length() - 1)]
    for stride in [v for v in strides if v >= first] + [v for v in strides if v < first]:
        value = value + lax.ppermute(value, axis, [(i, i ^ stride) for i in range(size)])
    return value


def all_shards(value, size):
    held = [value]
    masks = [0]
    stride = size // 2
    while stride >= 1:
        moves = [(i, i ^ stride) for i in range(size)]
        held = held + [lax.ppermute(v, "tp", moves) for v in held]
        masks = masks + [m ^ stride for m in masks]
        stride //= 2
    return held, masks


def send_products(pieces, size):
    groups = size // 2
    by_mask = dict(zip(range(groups - 1, -1, -1), pieces))

    def move(value, moves):
        pairs = [(2 * a + p, 2 * b + p) for a, b in moves for p in (0, 1)]
        return lax.ppermute(value, "seq", pairs)

    if groups != 4:
        return [
            move(by_mask[mask], [(g, g ^ mask) for g in range(groups)])
            for mask in range(1, groups)
        ], []
    far = move(by_mask[3], [(0, 1), (3, 2)])
    near = [move(by_mask[3], [(1, 2), (2, 1)]), move(by_mask[1], [(g, g ^ 1) for g in range(4)])]
    merged = (by_mask[2].astype(F32) + far.astype(F32)).astype(BF16)
    return near + [move(merged, [(g, g ^ 2) for g in range(4)])], [merged]


def on_device(
    packed_input, block_exponent, gate_input, state_write, state_read, log_decay,
    skip_weight, norm_gain, out_weight, out_cotangent,
):
    heads, _ = log_decay.shape
    width = packed_input.shape[1]
    seq_size = lax.axis_size("seq")
    tp_size = lax.axis_size("tp")
    total_width = width * tp_size
    columns = out_weight.shape[1] // seq_size
    parity = lax.axis_index("seq") % 2
    partner = [(i, i ^ 1) for i in range(seq_size)]
    gain = norm_gain[None, :]

    x, near, far, seg_t, seg, spread2, skip, read_t = prepare(
        packed_input, block_exponent, log_decay, skip_weight[None, :], state_write, state_read
    )
    near, far, shifts = ring_gather(near, far, seq_size)
    sources = ring_sources(shifts, seq_size)

    other_half = pick(parity[None].astype(jnp.int32), out_cotangent, columns)
    theirs = lax.ppermute(other_half, "seq", partner)
    all_mine, masks = all_shards(out_cotangent, tp_size)
    all_theirs, _ = all_shards(theirs, tp_size)
    owners = jnp.bitwise_xor(lax.axis_index("tp"), jnp.array(masks, jnp.int32))
    owners = jnp.concatenate([owners, parity[None]]).astype(jnp.int32)

    pairs = width // LANES
    calls = min(2, pairs)
    y_local = None
    hops = seq_size // 2
    for call in range(calls):
        start, stop = call * pairs // calls, (call + 1) * pairs // calls
        waits = (*near[1:3], *far[1:3]) if call == 1 and hops > 2 else ()
        y_local = inside(
            heads, start, stop, seg_t, seg, state_write, state_read, x, skip, y_local, waits
        )
    waits = (y_local, *near[3:5], *far[3:5]) if hops > 2 else (y_local,)
    grad_v, cot_mine = cotangent(owners, out_weight, all_mine, columns, waits)
    cot_theirs = stack(owners, all_theirs, columns)

    y, scaled_t, stats, state, totals = enter(
        sources, y_local, gate_input, grad_v, gain, state_read, seg_t, spread2, near, far
    )
    stats = butterfly_sum(stats, "tp", tp_size)
    scale = lax.rsqrt(stats[0:1, :] / total_width + EPSILON)
    first = (2 * width // 5) // LANES * LANES
    bounds = (0, first, width)
    parts = len(bounds) - 1
    normed, normed_theirs = [], []
    for part in range(parts):
        rows = scaled_t[bounds[part] : bounds[part + 1]]
        normed.append((rows * scale).astype(BF16))
        normed_theirs.append(lax.ppermute(normed[part], "seq", partner))

    grad_gate, grad_y, send, keep, sums = gate_grads(
        total_width, sources, y, gate_input, grad_v, gain, stats, x, seg_t, spread2, read_t
    )
    received, later = pair_state(totals, sources, send, keep, seq_size)
    middle = pairs // 2
    operands = (seg_t, seg, state_write, state_read, x, grad_y)
    inner, grad_cross = inside_back(heads, 0, middle, *operands)
    inner, write_part, read_part = inside_back(heads, middle, pairs, *operands, inner, grad_cross)
    group = (lax.axis_index("seq") // 2)[None].astype(jnp.int32)
    arrived, own_part, merges = [], [], []
    for part in range(parts):
        *pieces, last = products(group, normed[part], normed_theirs[part], cot_mine, cot_theirs)
        got, merged = send_products(pieces, seq_size)
        arrived.append(got)
        own_part.append(last)
        merges.append(merged)
    own, other = join_states(
        totals, sources, keep, received, later, seq_size, (write_part, *merges[0])
    )
    grad_input, maps, grad_decay = leave(
        heads, sources, y, x, grad_y, inner, state_write, seg_t, spread2, skip, state,
        write_part, read_part, own, other, (),
    )
    grad_out_weight = None
    for part in range(parts):
        grad_out_weight = finish(
            bounds[part], width, own_part[part], arrived[part], grad_out_weight
        )
    maps = butterfly_sum(maps, "tp", tp_size)
    sums = butterfly_sum(sums, "seq", seq_size, 2)
    grad_skip = jnp.sum(sums[1].reshape(heads, width // heads), axis=1)
    return (
        grad_input, grad_gate, maps[0], maps[1], grad_decay, grad_skip, sums[0], grad_out_weight.T,
    )


def solution(mesh):
    placed = (
        P("seq", "tp"), P("tp", "seq"), P("seq", "tp"), P("seq", None), P("seq", None),
        P("tp", "seq"), P("tp"), P("tp"), P("tp", None), P("seq", "tp"),
    )
    return jax.shard_map(
        on_device,
        mesh=mesh,
        in_specs=placed,
        out_specs=(
            P("seq", "tp"), P("seq", "tp"), P("seq", None), P("seq", None), P("tp", "seq"),
            P("tp"), P("tp"), P("tp", "seq"),
        ),
        check_vma=False,
    )
```

```python
import functools
import jax
import jax.numpy as jnp
from jax import lax
from jax.experimental import pallas as pl
from jax.experimental.pallas import tpu as pltpu
from jax.sharding import PartitionSpec as P

F32 = jnp.float32
BF16 = jnp.bfloat16
LANES = 128
EXTRA = 16
EPSILON = 1e-05
HALF = LANES // 2


def mm(a, b):
    return jnp.dot(a, b, preferred_element_type=F32)


def mm_t(a, b):
    return lax.dot_general(a, b, (((1,), (1,)), ((), ())), preferred_element_type=F32)


def split2(v):
    high = v.astype(BF16)
    return high, (v - high.astype(F32)).astype(BF16)


def split3(v):
    high = v.astype(BF16)
    rest = v - high.astype(F32)
    middle = rest.astype(BF16)
    return high, middle, (rest - middle.astype(F32)).astype(BF16)


def iota(shape, axis):
    return lax.broadcasted_iota(jnp.int32, shape, axis)


def spread(values, spread2):
    return mm(jnp.concatenate(split2(values), axis=1), spread2)


FULL_GRANT = 67_043_328


def params(limit=24 << 20):
    return pltpu.CompilerParams(vmem_limit_bytes=limit)


def cost(flops, nbytes, special=0):
    return pl.CostEstimate(flops=int(flops), bytes_accessed=int(nbytes), transcendentals=int(special))


def skipping(kernel, first, extra):
    return lambda *refs: kernel(*refs[:first], *refs[first + extra :])


WAIT = pl.BlockSpec(memory_space=pl.ANY)


def prepare_kernel(
    heads, packed, expo, decay, skip, write, read,
    x_out, near_out, far_out, seg_t_out, seg_out, spread_out, skip_out, read_t_out, pad, pad8,
):
    length, width = x_out.shape
    head_width = width // heads
    rows8 = packed.shape[0]
    groups = expo.shape[0]
    pad[...] = jnp.zeros_like(pad)
    pad[0:heads, :] = decay[...]
    decay_t = pad[...].T
    lower = (iota((length, length), 0) >= iota((length, length), 1)).astype(BF16)
    seg_t = sum(mm(lower, part) for part in split3(decay_t))
    seg_t_out[...] = seg_t
    seg_out[...] = seg_t.T
    of_head = (iota((LANES, width), 1) // head_width == iota((LANES, width), 0)).astype(BF16)
    spread2 = jnp.concatenate([of_head, of_head], axis=0)
    spread_out[...] = spread2
    pad8[...] = jnp.zeros_like(pad8)
    pad8[0:1, 0:heads] = skip[...]
    skip_out[...] = sum(mm(part, of_head) for part in split3(pad8[...]))
    total = seg_t[length - 1 : length, :]
    to_end = spread(jnp.exp(total - seg_t), spread2)
    pad[...] = jnp.zeros_like(pad)
    pad[0:groups, :] = jnp.left_shift(1, expo[...] + 8).astype(F32) * (2.0**-8)
    of_group = (
        iota((LANES, width), 1) // (width // groups) == iota((LANES, width), 0)
    ).astype(BF16)
    factors = mm(pad[...].T.astype(BF16), of_group)
    words = jnp.broadcast_to(packed[...][:, None, :], (rows8, 8, width))
    words = jnp.right_shift(words, 4 * iota((rows8, 8, width), 1))
    fields = (jnp.bitwise_and(words, 15) - 8).astype(F32).reshape(length, width)
    x = fields * factors
    x_out[...] = x.astype(BF16)
    states = mm(write[...].T, (x * to_end).astype(BF16)).astype(BF16)
    read_t_out[...] = read[...].T
    near_out[0:HALF, :] = states[0:HALF, :]
    far_out[...] = states[HALF:, :]
    total8 = jnp.broadcast_to(total, (8, LANES))
    high, middle, low = (mm(part, of_head) for part in split3(total8))
    row = iota((EXTRA, width), 0)
    tail = jnp.where(row == 0, high[0:1, :], jnp.where(row == 1, middle[0:1, :], low[0:1, :]))
    near_out[HALF:, :] = jnp.where(row < 3, tail, 0.0).astype(BF16)


def prepare(packed, expo, decay, skip, write, read):
    heads, length = decay.shape
    width = packed.shape[1]
    shapes = (
        jax.ShapeDtypeStruct((length, width), BF16),
        jax.ShapeDtypeStruct((HALF + EXTRA, width), BF16),
        jax.ShapeDtypeStruct((HALF, width), BF16),
        jax.ShapeDtypeStruct((length, LANES), F32),
        jax.ShapeDtypeStruct((LANES, length), F32),
        jax.ShapeDtypeStruct((2 * LANES, width), BF16),
        jax.ShapeDtypeStruct((8, width), F32),
        jax.ShapeDtypeStruct((LANES, length), BF16),
    )
    return pl.pallas_call(
        functools.partial(prepare_kernel, heads),
        name="prepare",
        out_shape=shapes,
        scratch_shapes=[pltpu.VMEM((LANES, length), F32), pltpu.VMEM((8, LANES), F32)],
        compiler_params=params(FULL_GRANT),
        cost_estimate=cost(3e9, 8e6),
    )(packed, expo, decay, skip, write, read)


def pick_kernel(per_half, columns, parity, shard, out):
    odd_wanted = parity[0] == 0
    for sub in range(per_half):
        even_part = shard[:, 2 * sub * columns : (2 * sub + 1) * columns]
        odd_part = shard[:, (2 * sub + 1) * columns : (2 * sub + 2) * columns]
        out[sub * columns : (sub + 1) * columns, :] = jnp.where(odd_wanted, odd_part, even_part).T


def pick(parity, shard, columns):
    length, shard_width = shard.shape
    out = (shard_width // 2, length)
    return pl.pallas_call(
        functools.partial(pick_kernel, shard_width // (2 * columns), columns),
        name="pick",
        grid_spec=pltpu.PrefetchScalarGridSpec(
            num_scalar_prefetch=1, grid=(1,), in_specs=[whole(shard.shape)], out_specs=whole(out)
        ),
        out_shape=jax.ShapeDtypeStruct(out, BF16),
        compiler_params=params(),
        cost_estimate=cost(1e8, 2e6),
    )(parity, shard)


def cotangent_kernel(shards, per_half, owners, weight, *rest):
    mine = rest[:shards]
    grad_v, cot_mine, full = rest[shards:]
    shard_width = mine[0].shape[1]
    columns = cot_mine.shape[1]

    @pl.when(pl.program_id(0) == 0)
    def _():
        odd = owners[shards] == 1
        for m in range(shards):
            for q in range(shards):
                @pl.when(owners[m] == q)
                def _():
                    full[:, q * shard_width : (q + 1) * shard_width] = mine[m][...]
            for sub in range(per_half):
                even_part = mine[m][:, 2 * sub * columns : (2 * sub + 1) * columns]
                odd_part = mine[m][:, (2 * sub + 1) * columns : (2 * sub + 2) * columns]
                cot_mine[owners[m] * per_half + sub] = jnp.where(odd, odd_part, even_part).T

    grad_v[...] = mm_t(full[...], weight[...])


def cotangent(owners, weight, mine, columns, waits):
    shards = len(mine)
    length, shard_width = mine[0].shape
    width, model_width = weight.shape
    per_half = shard_width // (2 * columns)
    block = 2 * LANES if width % (2 * LANES) == 0 else LANES
    stacked = (shards * per_half, columns, length)
    return pl.pallas_call(
        skipping(functools.partial(cotangent_kernel, shards, per_half), 2 + shards, len(waits)),
        name="cotangent",
        grid_spec=pltpu.PrefetchScalarGridSpec(
            num_scalar_prefetch=1,
            grid=(width // block,),
            in_specs=[pl.BlockSpec((block, model_width), lambda i, *_: (i, 0))]
            + [whole(mine[0].shape)] * shards
            + [WAIT] * len(waits),
            out_specs=[pl.BlockSpec((length, block), lambda i, *_: (0, i)), whole(stacked)],
            scratch_shapes=[pltpu.VMEM((length, model_width), BF16)],
        ),
        out_shape=(
            jax.ShapeDtypeStruct((length, width), F32),
            jax.ShapeDtypeStruct(stacked, BF16),
        ),
        compiler_params=params(),
        cost_estimate=cost(2.0 * length * width * model_width, 20e6),
    )(owners, weight, *mine, *waits)


def stack_kernel(shards, owners, *rest):
    theirs, out = rest[:shards], rest[shards]
    columns = out.shape[1]
    per_half = theirs[0].shape[0] // columns
    for m in range(shards):
        for sub in range(per_half):
            rows = slice(sub * columns, (sub + 1) * columns)
            out[owners[m] * per_half + sub] = theirs[m][rows, :]


def stack(owners, theirs, columns):
    rows, length = theirs[0].shape
    out = (len(theirs) * rows // columns, columns, length)
    return pl.pallas_call(
        functools.partial(stack_kernel, len(theirs)),
        name="stack",
        grid_spec=pltpu.PrefetchScalarGridSpec(
            num_scalar_prefetch=1,
            grid=(1,),
            in_specs=[whole(theirs[0].shape)] * len(theirs),
            out_specs=whole(out),
        ),
        out_shape=jax.ShapeDtypeStruct(out, BF16),
        compiler_params=params(),
        cost_estimate=cost(1e8, 3e6),
    )(owners, *theirs)


def pair_columns(seg_t, seg, step):
    rolled = pltpu.roll(seg_t[...], lax.rem(LANES - 2 * step, LANES), 1)
    for side in (0, 1):
        yield side, rolled[:, side : side + 1], seg[pl.ds(2 * step + side, 1), :]


def inside_kernel(head_width, start, seg_t, seg, write, read, x, skip, *rest):
    out, cross = rest[-2:]
    step = pl.program_id(0) + start
    length = x.shape[0]
    half = length // 2

    @pl.when(pl.program_id(0) == 0)
    def _():
        cross[...] = mm_t(read[...], write[...])

    diagonal = iota((half, half), 0) >= iota((half, half), 1)
    parts = []
    for side, column, row in pair_columns(seg_t, seg, step):
        rows = []
        for block in (0, 1):
            low = block * half
            square = slice(low, low + half)
            gap = column[square] - row[:, square]
            decayed = jnp.where(diagonal, jnp.exp(jnp.minimum(gap, 0.0)), 0.0)
            mixing = decayed * cross[square, square]
            if block == 1:
                left = jnp.exp(column[square] - row[:, 0:half]) * cross[square, 0:half]
                mixing = jnp.concatenate([left, mixing], axis=1)
            high, rest = split2(mixing)
            values = x[0 : low + half, :]
            rows.append(mm(high, values) + mm(rest, values))
        parts.append(jnp.concatenate(rows, axis=0))
    first = iota((length, LANES), 1) < head_width
    out[...] = jnp.where(first, parts[0], parts[1]) + skip[0:1, :] * x[...].astype(F32)


def whole(shape):
    return pl.BlockSpec(shape, lambda *_: (0,) * len(shape))


def inside(heads, start, stop, seg_t, seg, write, read, x, skip, held=None, waits=()):
    length, width = x.shape
    column = pl.BlockSpec((length, LANES), lambda j: (0, j + start))
    share = (stop - start) / (width // LANES)
    operands = (seg_t, seg, write, read, x, skip)
    if held is None:
        operands = tuple(pltpu.with_memory_space_constraint(v, pltpu.HBM) for v in operands)
    specs = [
        whole((length, LANES)), whole((LANES, length)), whole(write.shape), whole(read.shape),
        column, pl.BlockSpec((8, LANES), lambda j: (0, j + start)),
    ]
    aliases = {}
    if held is not None:
        aliases = {len(operands): 0}
        operands = operands + (held,)
        specs = specs + [WAIT]
    operands = operands + tuple(waits)
    specs = specs + [WAIT] * len(waits)
    return pl.pallas_call(
        functools.partial(inside_kernel, width // heads, start),
        name="inside",
        grid=(stop - start,),
        in_specs=specs,
        out_specs=column,
        out_shape=jax.ShapeDtypeStruct((length, width), F32),
        scratch_shapes=[pltpu.VMEM((length, length), F32)],
        input_output_aliases=aliases,
        compiler_params=params(),
        cost_estimate=cost(20e9 * share, 5e6 * share),
    )(*operands)


def gathered_total(pays, k):
    tail = pays[k][HALF : HALF + 8, :].astype(F32)
    return tail[0:1, :] + tail[1:2, :] + tail[2:3, :]


def boundary(totals, near, far, sources, position, count):
    width = totals.shape[1]
    column = jnp.zeros((count, 1), jnp.int32)
    for k in range(count):
        column = jnp.where(iota((count, 1), 0) == k, sources[k], column)
    powers = jnp.zeros((count, width), F32)
    for j in range(count):
        between = jnp.logical_and(column < sources[j], sources[j] < position)
        powers = powers + jnp.where(between, totals[j : j + 1, :], 0.0)
    weights = jnp.where(column < position, jnp.exp(powers), 0.0)
    upper = jnp.zeros((HALF, width), F32)
    lower = jnp.zeros((HALF, width), F32)
    for k in range(count):
        upper = upper + weights[k : k + 1, :] * near[k][0:HALF, :].astype(F32)
        lower = lower + weights[k : k + 1, :] * far[k][...].astype(F32)
    return upper, lower


def enter_kernel(
    count, sources, y_local, gate, grad_v, gain, read, seg_t, spread2, *rest,
):
    near, far = rest[:count], rest[count : 2 * count]
    y_out, scaled_t_out, stats_out, state_out, totals_out, state2 = rest[2 * count :]

    @pl.when(pl.program_id(0) == 0)
    def _():
        for k in range(count):
            totals_out[k : k + 1, :] = gathered_total(near, k)
        upper, lower = boundary(totals_out[...], near, far, sources, sources[count], count)
        state_out[0:HALF, :] = upper
        state_out[HALF:, :] = lower
        state2[0:LANES, :], state2[LANES:, :] = split2(state_out[...])

    from_start = spread(jnp.exp(seg_t[...]), spread2[...])
    read_part = read[...]
    carried = mm(jnp.concatenate([read_part, read_part], axis=1), state2[...])
    y = y_local[...] + from_start * carried
    y_out[...] = y
    z = gate[...].astype(F32)
    mixed = y * z / (1.0 + jnp.exp(-z))
    with_gain = mixed * gain[...]
    scaled_t_out[...] = with_gain.T
    squares = jnp.sum(mixed * mixed, axis=1, keepdims=True)
    inner = jnp.sum(grad_v[...] * with_gain, axis=1, keepdims=True)
    lane = iota((squares.shape[0], LANES), 1)
    stats = jnp.where(lane == 0, squares, jnp.where(lane == 1, inner, 0.0))
    stats_out[...] = stats.T[0:8, :]


def enter(sources, y_local, gate, grad_v, gain, read, seg_t, spread2, near, far):
    length, width = y_local.shape
    count = len(near)
    block = LANES
    token = pl.BlockSpec((block, width), lambda i, *_: (i, 0))
    narrow = pl.BlockSpec((block, LANES), lambda i, *_: (i, 0))
    shapes = (
        jax.ShapeDtypeStruct((length, width), F32),
        jax.ShapeDtypeStruct((width, length), F32),
        jax.ShapeDtypeStruct((8, length), F32),
        jax.ShapeDtypeStruct((LANES, width), F32),
        jax.ShapeDtypeStruct((count, width), F32),
    )
    return pl.pallas_call(
        functools.partial(enter_kernel, count),
        name="enter",
        grid_spec=pltpu.PrefetchScalarGridSpec(
            num_scalar_prefetch=1,
            grid=(length // block,),
            in_specs=[
                token, token, token, whole((1, width)), narrow, narrow, whole(spread2.shape),
            ] + [whole(near[0].shape)] * count + [whole(far[0].shape)] * count,
            out_specs=[
                token,
                pl.BlockSpec((width, block), lambda i, *_: (0, i)),
                pl.BlockSpec((8, block), lambda i, *_: (0, i)),
                whole((LANES, width)),
                whole((count, width)),
            ],
            scratch_shapes=[pltpu.VMEM((2 * LANES, width), BF16)],
        ),
        out_shape=shapes,
        compiler_params=params(),
        cost_estimate=cost(3e9, 15e6),
    )(sources, y_local, gate, grad_v, gain, read, seg_t, spread2, *near, *far)


def gate_kernel(
    total_width, sources, y_ref, gate, grad_v, gain, stats, x, seg_t, spread2, read_t,
    gate_out, grad_y_out, send_out, keep_out, sums, columns, cot,
):
    step = pl.program_id(0)
    row = iota((LANES, LANES), 0)
    squares, inner = stats[0:1, :], stats[1:2, :]
    scale_row = lax.rsqrt(squares * (1.0 / total_width) + EPSILON)
    back_row = scale_row * scale_row * scale_row * inner * (1.0 / total_width)
    columns[...] = jnp.where(row == 0, scale_row, jnp.where(row == 1, back_row, 0.0)).T
    scale, back = columns[:, 0:1], columns[:, 1:2]
    y = y_ref[...]
    z = gate[...].astype(F32)
    sigma = 1.0 / (1.0 + jnp.exp(-z))
    active = z * sigma
    mixed = y * active
    scaled_v = scale * grad_v[...]
    grad_mixed = scaled_v * gain[...] - mixed * back
    gate_out[...] = (grad_mixed * y * sigma * (1.0 + z * (1.0 - sigma))).astype(BF16)
    grad_y = grad_mixed * active
    grad_y_out[...] = grad_y
    gain_part = jnp.sum(scaled_v * mixed, axis=0, keepdims=True)
    skip_part = jnp.sum(grad_y * x[...].astype(F32), axis=0, keepdims=True)
    from_start = spread(jnp.exp(seg_t[...]), spread2[...])
    cot_part = mm(read_t[...], (grad_y * from_start).astype(BF16))
    wide = iota((8, grad_y.shape[1]), 0)
    sum_part = jnp.where(wide == 0, gain_part, jnp.where(wide == 1, skip_part, 0.0))

    @pl.when(step == 0)
    def _():
        cot[...] = cot_part
        sums[...] = sum_part

    @pl.when(step > 0)
    def _():
        cot[...] += cot_part
        sums[...] += sum_part

    @pl.when(step == pl.num_programs(0) - 1)
    def _():
        parity = lax.rem(sources[sources.shape[0] - 1], 2)
        keep_out[...] = cot[pl.ds(pl.multiple_of(parity * HALF, HALF), HALF), :]
        send_out[...] = cot[pl.ds(pl.multiple_of((1 - parity) * HALF, HALF), HALF), :].astype(BF16)


def gate_grads(total_width, sources, y, gate, grad_v, gain, stats, x, seg_t, spread2, read_t):
    length, width = y.shape
    block = LANES
    token = pl.BlockSpec((block, width), lambda i, *_: (i, 0))
    narrow = pl.BlockSpec((block, LANES), lambda i, *_: (i, 0))
    shapes = (
        jax.ShapeDtypeStruct((length, width), BF16),
        jax.ShapeDtypeStruct((length, width), F32),
        jax.ShapeDtypeStruct((HALF, width), BF16),
        jax.ShapeDtypeStruct((HALF, width), F32),
        jax.ShapeDtypeStruct((8, width), F32),
    )
    return pl.pallas_call(
        functools.partial(gate_kernel, total_width),
        name="gate_grads",
        grid_spec=pltpu.PrefetchScalarGridSpec(
            num_scalar_prefetch=1,
            grid=(length // block,),
            in_specs=[
                token, token, token, whole((1, width)), pl.BlockSpec((8, block), lambda i, *_: (0, i)),
                token, narrow, whole(spread2.shape), pl.BlockSpec((LANES, block), lambda i, *_: (0, i)),
            ],
            out_specs=[
                token, token, whole((HALF, width)), whole((HALF, width)), whole((8, width)),
            ],
            scratch_shapes=[pltpu.VMEM((LANES, LANES), F32), pltpu.VMEM((LANES, width), F32)],
        ),
        out_shape=shapes,
        compiler_params=params(),
        cost_estimate=cost(3e9, 15e6),
    )(sources, y, gate, grad_v, gain, stats, x, seg_t, spread2, read_t)


def inside_back_kernel(
    head_width, start, last, seg_t, seg, write, read, x, grad_y, *rest,
):
    step = pl.program_id(0) + start
    if last:
        before, out, grad_write, grad_read, cross, grad_cross = rest[-6:]
    else:
        out, sum_out, cross, grad_cross = rest[-4:]
    length = x.shape[0]
    half = length // 2

    @pl.when(pl.program_id(0) == 0)
    def _():
        cross[...] = mm_t(write[...], read[...])
        grad_cross[...] = before[...] if last else jnp.zeros_like(grad_cross)

    diagonal = iota((half, half), 0) <= iota((half, half), 1)
    first = iota((length, LANES), 1) < head_width
    grads = grad_y[...].astype(BF16)
    values = x[...]
    parts = []
    for side, column, row in pair_columns(seg_t, seg, step):
        mine = first if side == 0 else jnp.logical_not(first)
        own = jnp.where(mine, values, jnp.zeros_like(values))
        rows = []
        for block in (0, 1):
            low = block * half
            square = slice(low, low + half)
            gap = row[:, square] - column[square]
            decayed = jnp.where(diagonal, jnp.exp(jnp.minimum(gap, 0.0)), 0.0)
            mixing = decayed * cross[square, square]
            grad_cross[square, square] += mm_t(own[square], grads[square]) * decayed
            if block == 0:
                decayed = jnp.exp(row[:, half:] - column[square])
                mixing = jnp.concatenate([mixing, decayed * cross[square, half:]], axis=1)
                grad_cross[square, half:] += mm_t(own[square], grads[half:]) * decayed
            rows.append(mm(mixing.astype(BF16), grads[low:]))
        parts.append(jnp.concatenate(rows, axis=0))
    out[...] = jnp.where(first, parts[0], parts[1])

    @pl.when(pl.program_id(0) == pl.num_programs(0) - 1)
    def _():
        if last:
            high, low = split2(grad_cross[...])
            grad_write[...] = mm(high, read[...]) + mm(low, read[...])
            turned = grad_cross[...].T
            high, low = split2(turned)
            grad_read[...] = mm(high, write[...]) + mm(low, write[...])
        else:
            sum_out[...] = grad_cross[...]


def inside_back(heads, start, stop, seg_t, seg, write, read, x, grad_y, held=None, before=None):
    length, width = x.shape
    last = held is not None
    column = pl.BlockSpec((length, LANES), lambda j: (0, j + start))
    square = (length, length)
    small = (length, LANES)
    operands = (seg_t, seg, write, read, x, grad_y)
    specs = [
        whole((length, LANES)), whole((LANES, length)), whole(write.shape), whole(read.shape),
        column, column,
    ]
    share = (stop - start) / (width // LANES)
    outs = (jax.ShapeDtypeStruct((length, width), F32),)
    aliases = {}
    if last:
        operands = operands + (held, before)
        specs = specs + [WAIT, whole(square)]
        aliases = {6: 0}
        outs = outs + (jax.ShapeDtypeStruct(small, F32), jax.ShapeDtypeStruct(small, F32))
        out_specs = [column, whole(small), whole(small)]
    else:
        outs = outs + (jax.ShapeDtypeStruct(square, F32),)
        out_specs = [column, whole(square)]
    return pl.pallas_call(
        functools.partial(inside_back_kernel, width // heads, start, last),
        name="inside_back",
        grid=(stop - start,),
        in_specs=specs,
        out_specs=out_specs,
        out_shape=outs,
        scratch_shapes=[pltpu.VMEM(square, F32), pltpu.VMEM(square, F32)],
        input_output_aliases=aliases,
        compiler_params=params(),
        cost_estimate=cost(20e9 * share, 8e6 * share),
    )(*operands)


def total_of(totals, sources, count, wanted):
    found = jnp.zeros_like(totals[0:1, :])
    for k in range(count):
        found = found + jnp.where(sources[k] == wanted, totals[k : k + 1, :], 0.0)
    return found


def pair_kernel(count, sources, totals, keep, received, out):
    position = sources[count]
    odd = lax.rem(position, 2) == 1
    weight = jnp.exp(total_of(totals, sources, count, position - lax.rem(position, 2)))
    own, other = keep[...], received[...].astype(F32)
    out[...] = jnp.where(odd, other + weight * own, own + weight * other).astype(BF16)


def join_kernel(count, sources, totals, keep, received, *rest):
    shifts = count // 2 - 1
    later, (own_out, send_out) = rest[:shifts], rest[shifts:]
    position = sources[count]
    even_place = position - lax.rem(position, 2)
    odd = lax.rem(position, 2) == 1
    state = jnp.zeros_like(keep)
    power = jnp.zeros_like(totals[0:1, :])
    for shift in range(1, shifts + 1):
        state = state + jnp.exp(power) * later[shift - 1][...].astype(F32)
        if shift < shifts:
            power = power + total_of(totals, sources, count, even_place + 2 * shift)
            power = power + total_of(totals, sources, count, even_place + 2 * shift + 1)
    weight = jnp.exp(total_of(totals, sources, count, even_place + 1))
    of_odd = jnp.where(odd, keep[...], received[...].astype(F32))
    for_even = of_odd + weight * state
    own_out[...] = jnp.where(odd, state, for_even)
    send_out[...] = jnp.where(odd, for_even, state).astype(BF16)


def small_call(kernel, count, outs, sources, *arrays, waits=()):
    return pl.pallas_call(
        skipping(functools.partial(kernel, count), 1 + len(arrays), len(waits)),
        grid_spec=pltpu.PrefetchScalarGridSpec(
            num_scalar_prefetch=1,
            grid=(1,),
            in_specs=[whole(a.shape) for a in arrays] + [WAIT] * len(waits),
            out_specs=[whole(o.shape) for o in outs],
        ),
        out_shape=outs,
        compiler_params=params(),
        cost_estimate=cost(1e9, 2e6),
    )(sources, *arrays, *waits)


def pair_state(totals, sources, send, keep, size):
    partner = [(i, i ^ 1) for i in range(size)]
    received = lax.ppermute(send, "seq", partner)
    narrow = jax.ShapeDtypeStruct(send.shape, BF16)
    (pair,) = small_call(pair_kernel, size, (narrow,), sources, totals, keep, received)
    later = []
    for shift in range(1, size // 2):
        moves = [(i, i - 2 * shift) for i in range(2 * shift, size)]
        later.append(lax.ppermute(pair, "seq", moves))
    return received, later


def join_states(totals, sources, keep, received, later, size, waits):
    narrow = jax.ShapeDtypeStruct(keep.shape, BF16)
    wide = jax.ShapeDtypeStruct(keep.shape, F32)
    own, other = small_call(
        join_kernel, size, (wide, narrow), sources, totals, keep, received, *later,
        waits=waits,
    )
    return own, lax.ppermute(other, "seq", [(i, i ^ 1) for i in range(size)])


def leave_kernel(
    count, heads, sources, y_ref, x_ref, grad_y_ref, inner_ref, write, seg_t, last, spread2,
    skip, state, write_part, read_part, own, other,
    input_out, maps_out, decay_out, cot2, state16, from_head, per_head, sums, cot,
):
    step = pl.program_id(0)
    steps = pl.num_programs(0)
    block, width = y_ref.shape
    length = per_head.shape[0]

    @pl.when(step == 0)
    def _():
        parity = lax.rem(sources[count], 2)
        cot[pl.ds(pl.multiple_of(parity * HALF, HALF), HALF), :] = own[...]
        cot[pl.ds(pl.multiple_of((1 - parity) * HALF, HALF), HALF), :] = other[...].astype(F32)
        cot2[0:LANES, :], cot2[LANES:, :] = split2(cot[...])
        state16[...] = state[...].astype(BF16)
        from_head[...] = spread2[0:LANES, :].T
        ended = spread(jnp.exp(last[...]), spread2[...])
        through = jnp.sum(cot[...] * state[...], axis=0, keepdims=True) * ended[0:1, :]
        sums[...] = jnp.where(iota((8, width), 0) == 0, through, 0.0)

    seg_part = seg_t[...]
    decays = jnp.exp(seg_part)
    to_end = spread(jnp.exp(last[0:1, :] - seg_part), spread2[...])
    from_start = spread(decays, spread2[...])
    x = x_ref[...].astype(F32)
    grad_y = grad_y_ref[...]
    write_rows = write[...]
    from_later = to_end * mm(jnp.concatenate([write_rows, write_rows], axis=1), cot2[...])
    core_grad = inner_ref[...] + from_later
    skip_row = skip[0:1, :]
    input_out[...] = (skip_row * grad_y + core_grad).astype(BF16)
    leaving = jnp.sum(x * from_later, axis=0, keepdims=True)
    sums[...] += jnp.where(iota((8, width), 0) == 0, leaving, 0.0)
    terms = grad_y * (y_ref[...] - skip_row * x) - x * core_grad
    high, low = split2(terms)
    start = pl.multiple_of(step * block, block)
    per_head[pl.ds(start, block), :] = mm(high, from_head[...]) + mm(low, from_head[...])
    maps_out[0] = write_part[...] + mm_t((x * to_end).astype(BF16), cot2[0:LANES, :])
    maps_out[1] = read_part[...] + mm_t((grad_y * from_start).astype(BF16), state16[...])

    @pl.when(step == steps - 1)
    def _():
        final = sum(mm(part, from_head[...]) for part in split3(sums[...]))
        upper = (iota((length, length), 0) <= iota((length, length), 1)).astype(BF16)
        tail = sum(mm(upper, part) for part in split3(per_head[...]))
        decay_out[...] = (tail + final[0:1, :]).T[0:heads, :]


def leave(
    heads, sources, y, x, grad_y, inner, write, seg_t, spread2, skip, state,
    write_part, read_part, own, other, waits,
):
    length, width = y.shape
    count = sources.shape[0] - 1
    block = LANES
    token = pl.BlockSpec((block, width), lambda i, *_: (i, 0))
    narrow = pl.BlockSpec((block, LANES), lambda i, *_: (i, 0))
    shapes = (
        jax.ShapeDtypeStruct((length, width), BF16),
        jax.ShapeDtypeStruct((2, length, LANES), F32),
        jax.ShapeDtypeStruct((heads, length), F32),
    )
    last = jnp.broadcast_to(seg_t[length - 1 :, :], (8, LANES))
    return pl.pallas_call(
        skipping(functools.partial(leave_kernel, count, heads), 15, len(waits)),
        name="leave",
        grid_spec=pltpu.PrefetchScalarGridSpec(
            num_scalar_prefetch=1,
            grid=(length // block,),
            in_specs=[
                token, token, token, token, narrow, narrow, whole((8, LANES)),
                whole(spread2.shape), whole((8, width)), whole((LANES, width)),
                narrow, narrow, whole(own.shape), whole(other.shape),
            ] + [WAIT] * len(waits),
            out_specs=[
                token,
                pl.BlockSpec((2, block, LANES), lambda i, *_: (0, i, 0)),
                whole((heads, length)),
            ],
            scratch_shapes=[
                pltpu.VMEM((2 * LANES, width), BF16),
                pltpu.VMEM((LANES, width), BF16),
                pltpu.VMEM((width, LANES), BF16),
                pltpu.VMEM((length, LANES), F32),
                pltpu.VMEM((8, width), F32),
                pltpu.VMEM((LANES, width), F32),
            ],
        ),
        out_shape=shapes,
        compiler_params=params(),
        cost_estimate=cost(5e9, 20e6),
    )(
        sources, y, x, grad_y, inner, write, seg_t, last, spread2, skip, state,
        write_part, read_part, own, other, *waits,
    )


def product_kernel(masks, group, mine, theirs, cot_mine, cot_theirs, *outs):
    first_rows, second_rows = mine[...], theirs[...]
    for mask, out in zip(masks, outs):
        spot = jnp.bitwise_xor(group[0], mask)
        first = mm_t(cot_mine[spot], first_rows).astype(BF16).astype(F32)
        second = mm_t(cot_theirs[spot], second_rows).astype(BF16).astype(F32)
        out[...] = (first + second).astype(out.dtype)


def products(group, mine, theirs, cot_mine, cot_theirs):
    rows, length = mine.shape
    groups, columns, _ = cot_mine.shape
    masks = list(range(groups - 1, -1, -1))
    block = 2 * LANES if rows % (2 * LANES) == 0 else LANES
    side = pl.BlockSpec((block, length), lambda i, *_: (i, 0))
    return pl.pallas_call(
        functools.partial(product_kernel, masks),
        name="product",
        grid_spec=pltpu.PrefetchScalarGridSpec(
            num_scalar_prefetch=1,
            grid=(rows // block,),
            in_specs=[side, side, whole(cot_mine.shape), whole(cot_theirs.shape)],
            out_specs=[pl.BlockSpec((columns, block), lambda i, *_: (0, i))] * groups,
        ),
        out_shape=[
            jax.ShapeDtypeStruct((columns, rows), BF16 if mask else F32) for mask in masks
        ],
        compiler_params=params(),
        cost_estimate=cost(4.0 * rows * length * columns * groups, 5e6),
    )(group, mine, theirs, cot_mine, cot_theirs)


def finish_kernel(count, own, *rest):
    total = own[...]
    for k in range(count):
        total = total + rest[k][...].astype(F32)
    rest[-1][...] = total


def finish(start, width, own, received, held, waits=()):
    columns, rows = own.shape
    block = 2 * LANES if rows % (2 * LANES) == 0 and start % (2 * LANES) == 0 else LANES
    small = pl.BlockSpec((columns, block), lambda i: (0, i))
    operands = [own, *received]
    specs = [small] * len(operands)
    aliases = {}
    if held is not None:
        aliases = {len(operands): 0}
        operands.append(held)
        specs = specs + [WAIT]
    operands += list(waits)
    specs = specs + [WAIT] * len(waits)
    return pl.pallas_call(
        functools.partial(finish_kernel, len(received)),
        name="finish",
        grid=(rows // block,),
        in_specs=specs,
        out_specs=pl.BlockSpec((columns, block), lambda i: (0, start // block + i)),
        out_shape=jax.ShapeDtypeStruct((columns, width), F32),
        input_output_aliases=aliases,
        compiler_params=params(),
        cost_estimate=cost(1e9, 4e6),
    )(*operands)


def ring_gather(near, far, size):
    half = size // 2
    order = [2 * q for q in range(half)] + [2 * (size - 1 - q) + 1 for q in range(half, size)]
    ahead = [(order[i], order[(i + 1) % size]) for i in range(size)]
    behind = [(b, a) for a, b in ahead]
    shifts, all_near, all_far = [0], [near], [far]
    up = down = [near, far]
    for hop in range(1, half + 1):
        last = hop == half

        def move(value, moves):
            return lax.ppermute(value, "seq", moves)

        up = [move(up[0], ahead)] + ([] if last else [move(up[1], ahead)])
        down = ([] if last else [move(down[0], behind)]) + [move(down[1], behind)]
        if last:
            down = [None] + down[-1:]
        shifts.append(-hop)
        all_near.append(up[0])
        if last:
            all_far.append(down[1])
        else:
            all_far.append(up[1])
            shifts.append(hop)
            all_near.append(down[0])
            all_far.append(down[1])
    return all_near, all_far, shifts


def ring_sources(shifts, size):
    position = lax.axis_index("seq")
    half = size // 2
    place = jnp.where(position % 2 == 0, position // 2, size - 1 - position // 2)
    places = (place + jnp.array(shifts, jnp.int32) + size) % size
    found = jnp.where(places < half, 2 * places, 2 * (size - 1 - places) + 1)
    return jnp.concatenate([found, position[None]]).astype(jnp.int32)


def butterfly_sum(value, axis, size, first=1):
    strides = [1 << k for k in range(size.bit_length() - 1)]
    for stride in [v for v in strides if v >= first] + [v for v in strides if v < first]:
        value = value + lax.ppermute(value, axis, [(i, i ^ stride) for i in range(size)])
    return value


def all_shards(value, size):
    held = [value]
    masks = [0]
    stride = size // 2
    while stride >= 1:
        moves = [(i, i ^ stride) for i in range(size)]
        held = held + [lax.ppermute(v, "tp", moves) for v in held]
        masks = masks + [m ^ stride for m in masks]
        stride //= 2
    return held, masks


def send_products(pieces, size):
    groups = size // 2
    by_mask = dict(zip(range(groups - 1, -1, -1), pieces))

    def move(value, moves):
        pairs = [(2 * a + p, 2 * b + p) for a, b in moves for p in (0, 1)]
        return lax.ppermute(value, "seq", pairs)

    if groups != 4:
        return [
            move(by_mask[mask], [(g, g ^ mask) for g in range(groups)])
            for mask in range(1, groups)
        ], []
    far = move(by_mask[3], [(0, 1), (3, 2)])
    near = [move(by_mask[3], [(1, 2), (2, 1)]), move(by_mask[1], [(g, g ^ 1) for g in range(4)])]
    merged = (by_mask[2].astype(F32) + far.astype(F32)).astype(BF16)
    return near + [move(merged, [(g, g ^ 2) for g in range(4)])], [merged]


def on_device(
    packed_input, block_exponent, gate_input, state_write, state_read, log_decay,
    skip_weight, norm_gain, out_weight, out_cotangent,
):
    heads, _ = log_decay.shape
    width = packed_input.shape[1]
    seq_size = lax.axis_size("seq")
    tp_size = lax.axis_size("tp")
    total_width = width * tp_size
    columns = out_weight.shape[1] // seq_size
    parity = lax.axis_index("seq") % 2
    partner = [(i, i ^ 1) for i in range(seq_size)]
    gain = norm_gain[None, :]

    x, near, far, seg_t, seg, spread2, skip, read_t = prepare(
        packed_input, block_exponent, log_decay, skip_weight[None, :], state_write, state_read
    )
    near, far, shifts = ring_gather(near, far, seq_size)
    sources = ring_sources(shifts, seq_size)

    other_half = pick(parity[None].astype(jnp.int32), out_cotangent, columns)
    theirs = lax.ppermute(other_half, "seq", partner)
    all_mine, masks = all_shards(out_cotangent, tp_size)
    all_theirs, _ = all_shards(theirs, tp_size)
    owners = jnp.bitwise_xor(lax.axis_index("tp"), jnp.array(masks, jnp.int32))
    owners = jnp.concatenate([owners, parity[None]]).astype(jnp.int32)

    pairs = width // LANES
    calls = min(2, pairs)
    y_local = None
    hops = seq_size // 2
    for call in range(calls):
        start, stop = call * pairs // calls, (call + 1) * pairs // calls
        waits = (*near[1:3], *far[1:3]) if call == 1 and hops > 2 else ()
        y_local = inside(
            heads, start, stop, seg_t, seg, state_write, state_read, x, skip, y_local, waits
        )
    waits = (y_local, *near[3:5], *far[3:5]) if hops > 2 else (y_local,)
    grad_v, cot_mine = cotangent(owners, out_weight, all_mine, columns, waits)
    cot_theirs = stack(owners, all_theirs, columns)

    y, scaled_t, stats, state, totals = enter(
        sources, y_local, gate_input, grad_v, gain, state_read, seg_t, spread2, near, far
    )
    stats = butterfly_sum(stats, "tp", tp_size)
    scale = lax.rsqrt(stats[0:1, :] / total_width + EPSILON)
    first = (2*width//5) // LANES * LANES
    bounds = (0, first, width)
    parts = len(bounds) - 1
    normed, normed_theirs = [], []
    for part in range(parts):
        rows = scaled_t[bounds[part] : bounds[part + 1]]
        normed.append((rows * scale).astype(BF16))
        normed_theirs.append(lax.ppermute(normed[part], "seq", partner))

    grad_gate, grad_y, send, keep, sums = gate_grads(
        total_width, sources, y, gate_input, grad_v, gain, stats, x, seg_t, spread2, read_t
    )
    received, later = pair_state(totals, sources, send, keep, seq_size)
    middle = pairs // 2
    operands = (seg_t, seg, state_write, state_read, x, grad_y)
    inner, grad_cross = inside_back(heads, 0, middle, *operands)
    inner, write_part, read_part = inside_back(heads, middle, pairs, *operands, inner, grad_cross)
    group = (lax.axis_index("seq") // 2)[None].astype(jnp.int32)
    arrived, own_part, merges = [], [], []
    for part in range(parts):
        *pieces, last = products(group, normed[part], normed_theirs[part], cot_mine, cot_theirs)
        got, merged = send_products(pieces, seq_size)
        arrived.append(got)
        own_part.append(last)
        merges.append(merged)
    own, other = join_states(
        totals, sources, keep, received, later, seq_size, (write_part, *merges[0])
    )
    grad_input, maps, grad_decay = leave(
        heads, sources, y, x, grad_y, inner, state_write, seg_t, spread2, skip, state,
        write_part, read_part, own, other, (),
    )
    maps = butterfly_sum(maps, "tp", tp_size)
    write_map, read_map = maps[0], maps[1]
    sums = butterfly_sum(sums, "seq", seq_size, 2)
    grad_out_weight = None
    for part in range(parts):
        grad_out_weight = finish(
            bounds[part], width, own_part[part], arrived[part], grad_out_weight,
            (write_map, read_map) if part == parts - 1 else (),
        )
    grad_skip = jnp.sum(sums[1].reshape(heads, width // heads), axis=1)
    return (
        grad_input, grad_gate, write_map, read_map, grad_decay, grad_skip, sums[0], grad_out_weight.T,
    )


def solution(mesh):
    placed = (
        P("seq", "tp"), P("tp", "seq"), P("seq", "tp"), P("seq", None), P("seq", None),
        P("tp", "seq"), P("tp"), P("tp"), P("tp", None), P("seq", "tp"),
    )
    return jax.shard_map(
        on_device,
        mesh=mesh,
        in_specs=placed,
        out_specs=(
            P("seq", "tp"), P("seq", "tp"), P("seq", None), P("seq", None), P("tp", "seq"),
            P("tp"), P("tp"), P("tp", "seq"),
        ),
        check_vma=False,
    )
```
